32 devices in a mesh: row: 4 (over y, x), col: 8 (over z, core).
Axes of the slice: x: 2, y: 2, z: 4, core: 2. Of those that a mesh axis runs over, the one named last changes fastest.
Arguments:
- hidden_in: bfloat16 [16384, 2048], P('col', 'row'), may hold values from -6 to 6
- attention_gain: bfloat16 [2048], P('row'), may hold values from 0.5 to 1.5
- query_weight: bfloat16 [2048, 2048], P('col', 'row'), may hold values from -0.125 to 0.125
- key_weight: bfloat16 [2048, 2048], P('col', 'row'), may hold values from -0.125 to 0.125
- value_weight: bfloat16 [2048, 2048], P('col', 'row'), may hold values from -0.125 to 0.125
- projection: bfloat16 [2048, 2048], P('col', 'row'), may hold values from -1 to 1
- query_gain: bfloat16 [128], replicated, may hold values from 0.5 to 1.5
- key_gain: bfloat16 [128], replicated, may hold values from 0.5 to 1.5
- feedforward_gain: bfloat16 [2048], P('row'), may hold values from 0.5 to 1.5
- router_weight: bfloat16 [2048, 64], P('col', 'row'), may hold values from -0.125 to 0.125
- gate_weight: bfloat16 [64, 2048, 1024], P(('row', 'col')), may hold values from -0.125 to 0.125
- up_weight: bfloat16 [64, 2048, 1024], P(('row', 'col')), may hold values from -0.125 to 0.125
- down_weight: bfloat16 [64, 2048, 1024], P(('row', 'col')), may hold values from -4.1875 to 4.1875
- segments: int32 [8, 2048], P('col'), may hold values from 0 to 11, never falling along the last dimension, each value on 1 to 800 neighbouring positions
- routes: int32 [16384, 8], P('col'), may hold values from 0 to 63, all different within a row
- priority: int32 [8, 2048], P('col'), may hold values from 0 to 2047, each once within a row
- cotangent: bfloat16 [16384, 2048], P('col', 'row'), may hold values from -6 to 6
Outputs:
- output: bfloat16 [16384, 2048], P('col', 'row')
- grad_input: float32 [16384, 2048], P('col', 'row')
- grad_attention_gain: float32 [2048], P('row')
- grad_query: float32 [2048, 2048], P('col', 'row')
- grad_key: float32 [2048, 2048], P('col', 'row')
- grad_value: float32 [2048, 2048], P('col', 'row')
- grad_projection: float32 [2048, 2048], P('col', 'row')
- grad_query_gain: float32 [128], replicated
- grad_key_gain: float32 [128], replicated
- grad_feedforward_gain: float32 [2048], P('row')
- grad_router: float32 [2048, 64], P('col', 'row')
- grad_gate: float32 [64, 2048, 1024], P(('row', 'col'))
- grad_up: float32 [64, 2048, 1024], P(('row', 'col'))
- grad_down: float32 [64, 2048, 1024], P(('row', 'col'))
The draws below stay inside these ranges and needn't reach their ends.
Inputs may be any that keep to these rules, and one draw needn't show every extreme that they name: `segments`: segment numbers never fall along a sequence; a document covers at most 800 positions, and each sequence has one of that length. `routes`: each token names 8 different experts. `priority`: each row is a permutation of the positions of one group's 2048 tokens.
All inputs are finite; a program needn't handle non-finite values.
Results may differ from the reference program's by a relative error of at most 0.02.
Values may be sent and summed in bfloat16 or wider, within the bound.
A program may use at most 448 MiB of HBM per device.

```python
import math
from functools import partial
import jax
import jax.numpy as jnp
import numpy as np
from jax import lax

D = 2048
NH = 16
HS = 128
E = 64
TOPK = 8
SEQ = 2048
DOC_MAX = 800
DOC_COUNT = 12
TOKC = 2048
TOKENS = 16384
NSEQ = 8
NGROUPS = 8
CAP = 256
PIECES = 1
EPIECES = 64
FEP = 1024


def levels(stream_key, extent, split, low, top_value):
    factor_of, own = 1.0, jax.random.fold_in(stream_key, 6)
    for dim, parts in split:
        draws = jnp.exp(jax.random.uniform(jax.random.fold_in(own, dim), (parts,), jnp.float32, low / len(split), top_value / len(split)))
        factor_of = factor_of * jnp.repeat(draws, extent[dim] // parts).reshape([-1 if axis == dim else 1 for axis in range(len(extent))])
    return factor_of


def picks_of(own_key, rows, count, top, lift):
    ranking = jax.random.permutation(jax.random.fold_in(own_key, 1), count)
    pull = ranking
    for power in range(3):
        pull = pull * pull // count
    pull = pull * lift // count
    chance = jax.random.randint(jax.random.fold_in(own_key, 2), (rows, count), 0, 4096) + pull
    fixed_rows = jax.random.permutation(jax.random.fold_in(own_key, 3), rows)[jnp.arange(count) % rows]
    chance = jnp.where(jnp.arange(rows)[:, None] == fixed_rows[None, :], 1 << 14, chance)
    score = chance * count + jnp.arange(count)
    return lax.top_k(score.astype(jnp.int32), top)[1].astype(jnp.int32)


def split_up(number_of, total, bound, lean):
    weights = [(1 << 20) // math.isqrt(standing ** lean) + 1 for standing in range(2, number_of + 1)]
    rest, holding = total - bound - (number_of - 1), [1] * (number_of - 1)
    while rest > 0:
        movable = [i for i in range(number_of - 1) if holding[i] < bound]
        pool, remaining = sum([weights[i] for i in movable]), rest
        for i in movable:
            extra = min(bound - holding[i], max(1, remaining * weights[i] // pool), rest)
            holding[i] = holding[i] + extra
            rest = rest - extra
    return np.array([bound] + holding)


def ragged_sizes(rng, number_of, total, limit, slope):
    if number_of == 2:
        one = jax.random.randint(rng, (), max(1, total - limit), min(limit, total - 1) + 1)
        return jnp.stack([one, total - one])
    sizes = jnp.asarray(split_up(number_of, total, limit, slope), jnp.int32)
    twos = (number_of - 1) // 2
    donor, taker = sizes[1:1 + 2 * twos:2], sizes[2:2 + 2 * twos:2]
    margin = jnp.minimum(donor - 1, limit - taker)
    moved = jax.random.randint(jax.random.fold_in(rng, 1), (twos,), 0, 1 << 20) % (margin + 1)
    sizes = sizes.at[1:1 + 2 * twos:2].set(donor - moved).at[2:2 + 2 * twos:2].set(taker + moved)
    return sizes[jax.random.permutation(jax.random.fold_in(rng, 2), number_of)]


def bell_draw(rng, extent, scale, most, pieces=(), kind=jnp.bfloat16):
    drawn = scale * jax.random.normal(rng, extent, jnp.float32)
    if pieces:
        drawn = drawn * levels(rng, extent, pieces, -0.22, 0.18)
    return jnp.clip(drawn, -most, most).astype(kind)


def setup_inputs(seed: int = 0) -> dict:
    keys = jax.random.split(jax.random.key(seed), 18)
    hidden_in = bell_draw(keys[0], (TOKENS, D), 1.0, 6.0, ((0, 8), (1, 4)))
    attention_gain = jnp.clip(1.0 + 0.1 * jax.random.normal(keys[1], (D,), jnp.float32), 0.5, 1.5).astype(jnp.bfloat16)
    query_weight = bell_draw(keys[2], (D, NH * HS), D ** -0.5, 0.125, ((0, 8), (1, 4)))
    key_weight = bell_draw(keys[3], (D, NH * HS), D ** -0.5, 0.125, ((0, 8), (1, 4)))
    value_weight = bell_draw(keys[4], (D, NH * HS), D ** -0.5, 0.125, ((0, 8), (1, 4)))
    projection = bell_draw(keys[5], (D, NH * HS), (D // 64) ** -0.5, 1.0, ((0, 8), (1, 4)))
    query_gain = jnp.clip(1.0 + 0.1 * jax.random.normal(keys[6], (HS,), jnp.float32), 0.5, 1.5).astype(jnp.bfloat16)
    key_gain = jnp.clip(1.0 + 0.1 * jax.random.normal(keys[7], (HS,), jnp.float32), 0.5, 1.5).astype(jnp.bfloat16)
    feedforward_gain = jnp.clip(1.0 + 0.1 * jax.random.normal(keys[8], (D,), jnp.float32), 0.5, 1.5).astype(jnp.bfloat16)
    router_weight = bell_draw(keys[9], (D, E), D ** -0.5, 0.125, ((0, 8), (1, 4)))
    gate_weight = bell_draw(keys[10], (EPIECES, D, FEP), D ** -0.5, 0.125, ((0, 32),))
    up_weight = bell_draw(keys[11], (EPIECES, D, FEP), D ** -0.5, 0.125, ((0, 32),))
    down_weight = bell_draw(keys[12], (EPIECES, D, FEP), 0.7, 4.1875, ((0, 32),))
    segments = jax.vmap(lambda own: jnp.searchsorted(jnp.cumsum(ragged_sizes(own, DOC_COUNT, SEQ, DOC_MAX, 2)), jnp.arange(SEQ), side="right"))(jax.random.split(keys[13], NSEQ)).reshape((NSEQ, SEQ)).astype(jnp.int32)
    routes = picks_of(keys[14], TOKENS, E, TOPK, 1024)
    priority = jax.vmap(lambda own: jax.random.permutation(own, TOKC))(jax.random.split(keys[15], NGROUPS)).reshape((NGROUPS, TOKC)).astype(jnp.int32)
    cotangent = bell_draw(keys[16], (TOKENS, D), 1.0, 6.0, ((0, 8), (1, 4)))
    return dict(hidden_in=hidden_in, attention_gain=attention_gain, query_weight=query_weight, key_weight=key_weight, value_weight=value_weight, projection=projection, query_gain=query_gain, key_gain=key_gain, feedforward_gain=feedforward_gain, router_weight=router_weight, gate_weight=gate_weight, up_weight=up_weight, down_weight=down_weight, segments=segments, routes=routes, priority=priority, cotangent=cotangent)


@jax.custom_vjp
def low(v):
    return lax.optimization_barrier(v.astype(jnp.bfloat16)).astype(jnp.float32)

@jax.custom_vjp
def low_back(v):
    return v

def low_keep(v):
    return (low(v), None)

def low_pass(kept, grad):
    return (grad,)

def back_keep(v):
    return (v, None)

def back_low(kept, grad):
    return (low(grad),)
low.defvjp(low_keep, low_pass)
low_back.defvjp(back_keep, back_low)
EPSILON = 1e-06
HIGHEST = lax.Precision.HIGHEST

def norm_factor(values):
    return lax.rsqrt(lax.optimization_barrier(jnp.mean(values * values, axis=-1, keepdims=True)) + EPSILON)

def rotary_tables():
    half_size = HS // 2
    inverse = 50000.0 ** (-(jnp.arange(half_size, dtype=jnp.float32) * 2.0) / HS)
    angles = jnp.arange(SEQ, dtype=jnp.float32)[:, None] * inverse[None, :]
    return (jnp.cos(angles), jnp.sin(angles))

def rotate(values, cosine_table, sine_table):
    half_size = HS // 2
    first_half = values[..., :half_size]
    second = values[..., half_size:]
    return jnp.concatenate([first_half * cosine_table - second * sine_table, second * cosine_table + first_half * sine_table], axis=-1)

def attend_sequence(operands):
    queries, key_heads, values, segment = operands
    scores = jnp.einsum('qhd,khd->hqk', queries, key_heads, precision=HIGHEST) * HS ** (-0.5)
    scores = low_back(scores)
    same_doc = segment[:, None] == segment[None, :]
    scores = jnp.where(same_doc[None, :, :], scores, -1e+30)
    weights = jax.nn.softmax(scores, axis=-1)
    return jnp.einsum('hqk,khd->qhd', low(weights), values, precision=HIGHEST)

def expert_piece(normed, operands):
    gate_piece, up_piece, down_piece, piece_rows, piece_fill = operands
    inputs = low_back(normed[piece_rows] * piece_fill[:, None])
    gate_values = low_back(jnp.dot(inputs, gate_piece, precision=HIGHEST))
    upward = low_back(jnp.dot(inputs, up_piece, precision=HIGHEST))
    activated = low(jax.nn.silu(gate_values) * upward)
    return low(low_back(jnp.dot(activated, down_piece.T, precision=HIGHEST)))

def slot_tables(routes, priority):
    grouped = routes.reshape(NGROUPS, TOKC, TOPK)
    member = jnp.any(grouped[:, :, :, None] == jnp.arange(E, dtype=jnp.int32)[None, None, None, :], axis=2).astype(jnp.int32)
    by_rank = jnp.argsort(priority, axis=1).astype(jnp.int32)
    ranked = jnp.take_along_axis(member, jnp.broadcast_to(by_rank[:, :, None], member.shape), axis=1)
    before = jnp.cumsum(ranked, axis=1) - ranked
    slot_index = jnp.take_along_axis(before, jnp.broadcast_to(priority[:, :, None], member.shape), axis=1)
    target = jnp.where((member == 1) & (slot_index < CAP), slot_index, CAP)
    group_id = jnp.broadcast_to(jnp.arange(NGROUPS, dtype=jnp.int32)[:, None, None], member.shape)
    token_id = jnp.broadcast_to(jnp.arange(TOKC, dtype=jnp.int32)[None, :, None], member.shape)
    expert_id = jnp.broadcast_to(jnp.arange(E, dtype=jnp.int32)[None, None, :], member.shape)
    slot_table = jnp.zeros((NGROUPS, E, CAP), jnp.int32).at[group_id, expert_id, target].set(token_id, mode='drop')
    filled = jnp.zeros((NGROUPS, E, CAP), jnp.float32).at[group_id, expert_id, target].set(1.0, mode='drop')
    global_rows = slot_table + jnp.arange(NGROUPS, dtype=jnp.int32)[:, None, None] * TOKC
    slot_rows = jnp.transpose(global_rows, (1, 0, 2)).reshape(E, NGROUPS * CAP)
    slot_fill = jnp.transpose(filled, (1, 0, 2)).reshape(E, NGROUPS * CAP)
    return (slot_rows, slot_fill)

def layer(hidden_in, attention_gain, query_weight, key_weight, value_weight, projection, query_gain, key_gain, feedforward_gain, router_weight, gate_weight, up_weight, down_weight, segments, slot_rows, slot_fill):
    normed_one = low(hidden_in * norm_factor(hidden_in) * attention_gain)
    cosine_table, sine_table = rotary_tables()

    def heads_of(values):
        return values.reshape(NSEQ, SEQ, NH, HS)

    def prepare(raw_heads, head_gain):
        normed = raw_heads * norm_factor(raw_heads) * head_gain
        return low(rotate(normed, cosine_table[:, None, :], sine_table[:, None, :]))
    query_raw = low_back(jnp.dot(normed_one, query_weight, precision=HIGHEST))
    key_raw = low_back(jnp.dot(normed_one, key_weight, precision=HIGHEST))
    value_raw = low_back(jnp.dot(normed_one, value_weight, precision=HIGHEST))
    query_heads = prepare(heads_of(query_raw), query_gain)
    key_heads = prepare(heads_of(key_raw), key_gain)
    value_heads = low(heads_of(value_raw))
    mixed_heads = lax.map(jax.checkpoint(attend_sequence), (query_heads, key_heads, value_heads, segments))
    mixed_heads = low_back(low(mixed_heads.reshape(TOKENS, NH * HS)))
    branch = low_back(jnp.dot(mixed_heads, projection.T, precision=HIGHEST))
    middle = hidden_in + branch
    normed_two = low(middle * norm_factor(middle) * feedforward_gain)
    logits = low_back(jnp.dot(normed_two, router_weight, precision=HIGHEST))
    router_probs = jax.nn.softmax(logits, axis=-1)
    piece_rows = jnp.repeat(slot_rows, PIECES, axis=0)
    piece_fill = jnp.repeat(slot_fill, PIECES, axis=0)
    produced = lax.map(jax.checkpoint(partial(expert_piece, normed_two)), (gate_weight, up_weight, down_weight, piece_rows, piece_fill))
    expert_out = lax.optimization_barrier(jnp.sum(produced.reshape(E, PIECES, NGROUPS * CAP, D), axis=1))
    slot_prob = jnp.take_along_axis(router_probs.T, slot_rows, axis=1) * slot_fill
    combined = jnp.zeros((TOKENS, D), jnp.float32).at[slot_rows.reshape(-1)].add((expert_out * slot_prob[:, :, None]).reshape(-1, D))
    return middle + combined

def reference(hidden_in, attention_gain, query_weight, key_weight, value_weight, projection, query_gain, key_gain, feedforward_gain, router_weight, gate_weight, up_weight, down_weight, segments, routes, priority, cotangent):
    slot_rows, slot_fill = slot_tables(routes, priority)
    floats = [array.astype(jnp.float32) for array in (hidden_in, attention_gain, query_weight, key_weight, value_weight, projection, query_gain, key_gain, feedforward_gain, router_weight, gate_weight, up_weight, down_weight)]

    def forward(*weights):
        return layer(*weights, segments, slot_rows, slot_fill)
    result, pullback = jax.vjp(forward, *floats)
    gradients = pullback(cotangent.astype(jnp.float32))
    return (result.astype(jnp.bfloat16), gradients[0], gradients[1], gradients[2], gradients[3], gradients[4], gradients[5], gradients[6], gradients[7], gradients[8], gradients[9], gradients[10], gradients[11], gradients[12])
```

```python
import functools

import jax
import jax.numpy as jnp
from jax import lax
from jax.experimental import pallas as pl
from jax.experimental.pallas import tpu as pltpu
from jax.sharding import Mesh, PartitionSpec as P

D = 2048
HS = 128
E = 64
TOPK = 8
SEQ = 2048
EPSILON = 1e-06
SCALE = HS ** (-0.5)
CHUNKS = 2
TOKENS_AXES = ("z", "core")
SWAP_AXES = ("row", "core")
ALL_AXES = ("row", "z", "core")
BF = jnp.bfloat16
F32 = jnp.float32
VMEM_BYTES = 60 * 1024 * 1024


def call(body, grid, in_specs, out_specs, out_shape, scratch=(), flops=0, moved=0, prefetch=0, name=None):
    return pl.pallas_call(
        body,
        out_shape=out_shape,
        grid_spec=pltpu.PrefetchScalarGridSpec(
            num_scalar_prefetch=prefetch,
            grid=grid,
            in_specs=in_specs,
            out_specs=out_specs,
            scratch_shapes=list(scratch),
        ),
        compiler_params=pltpu.CompilerParams(
            dimension_semantics=("arbitrary",) * len(grid), vmem_limit_bytes=VMEM_BYTES
        ),
        cost_estimate=pl.CostEstimate(flops=flops, bytes_accessed=moved, transcendentals=0),
        name=name,
    )


def shape(dims, dtype):
    return jax.ShapeDtypeStruct(dims, dtype)


def dot(left, right, left_dim=1, right_dim=0):
    return lax.dot_general(
        left, right, (((left_dim,), (right_dim,)), ((), ())), preferred_element_type=F32
    )


def rotary_tables():
    half_size = HS // 2
    inverse = 50000.0 ** (-(jnp.arange(half_size, dtype=F32) * 2.0) / HS)
    angles = jnp.arange(SEQ, dtype=F32)[:, None] * inverse[None, :]
    cosine, sine = jnp.cos(angles), jnp.sin(angles)
    return (
        jnp.concatenate([cosine, cosine], axis=1),
        jnp.concatenate([-sine, sine], axis=1),
    )


def project_body(x_ref, gain_ref, w_ref, cos_ref, sin_ref, hg_ref, normed_ref, heads_ref, raw_ref):
    x = x_ref[...].astype(F32)
    factor = lax.rsqrt(jnp.mean(x * x, axis=1, keepdims=True) + EPSILON)
    normed = (x * factor * gain_ref[...]).astype(BF)
    normed_ref[...] = normed
    raw = dot(normed, w_ref[...])
    turned = raw_ref.shape[1]
    raw_ref[...] = raw[:, :turned]
    cosine, sine = cos_ref[...], sin_ref[...]
    for head in range(turned // HS):
        part = raw[:, head * HS : (head + 1) * HS]
        unit = part * lax.rsqrt(jnp.mean(part * part, axis=1, keepdims=True) + EPSILON)
        scaled = unit * hg_ref[:, head * HS : (head + 1) * HS]
        heads_ref[:, head * HS : (head + 1) * HS] = (
            scaled * cosine + pltpu.roll(scaled, HS // 2, 1) * sine
        ).astype(BF)
    heads_ref[:, turned:] = raw[:, turned:].astype(BF)


def project(hidden, gain, weights, cosine, sine, head_gains):
    tokens, width = hidden.shape
    columns = weights.shape[1]
    turned = columns // 3 * 2
    tile = 256
    return call(
        project_body,
        (tokens // tile,),
        [
            pl.BlockSpec((tile, width), lambda t: (t, 0)),
            pl.BlockSpec((1, width), lambda t: (0, 0)),
            pl.BlockSpec((width, columns), lambda t: (0, 0)),
            pl.BlockSpec((tile, HS), lambda t: (t, 0)),
            pl.BlockSpec((tile, HS), lambda t: (t, 0)),
            pl.BlockSpec((1, turned), lambda t: (0, 0)),
        ],
        [
            pl.BlockSpec((tile, width), lambda t: (t, 0)),
            pl.BlockSpec((tile, columns), lambda t: (t, 0)),
            pl.BlockSpec((tile, turned), lambda t: (t, 0)),
        ],
        [shape((tokens, width), BF), shape((tokens, columns), BF), shape((tokens, turned), F32)],
        flops=2 * tokens * width * columns,
        moved=6 * tokens * width + 2 * width * columns + 6 * tokens * columns,
        name="project",
    )(hidden, gain, weights, cosine, sine, head_gains)


QUERY_TILE = 256
KEY_TILE = 256


def key_ranges(segment):
    first = segment[::QUERY_TILE]
    last = segment[QUERY_TILE - 1 :: QUERY_TILE]
    key_first = segment[::KEY_TILE]
    key_last = segment[KEY_TILE - 1 :: KEY_TILE]
    meets = (key_first[None, :] <= last[:, None]) & (key_last[None, :] >= first[:, None])
    order = jnp.arange(meets.shape[1], dtype=jnp.int32)[None, :]
    low = jnp.min(jnp.where(meets, order, meets.shape[1]), axis=1)
    high = jnp.max(jnp.where(meets, order + 1, 0), axis=1)
    return low.astype(jnp.int32), high.astype(jnp.int32)


def key_rows(step):
    return pl.ds(pl.multiple_of(step * KEY_TILE, KEY_TILE), KEY_TILE)


def attend_body(low, high, q_ref, k_ref, v_ref, qs_ref, ks_ref, out_ref, sum_ref):
    block = pl.program_id(1)
    query = q_ref[...]
    query_docs = qs_ref[...]

    def step(index, state):
        total, mixed = state
        rows = key_rows(index)
        scores = dot(query, k_ref[rows, :], 1, 1) * SCALE
        raised = jnp.where(query_docs == ks_ref[:, rows], jnp.exp(scores), 0.0)
        total = total + jnp.sum(raised, axis=1, keepdims=True)
        mixed = mixed + dot(raised.astype(BF), v_ref[rows, :])
        return total, mixed

    total, mixed = lax.fori_loop(
        low[block],
        high[block],
        step,
        (jnp.zeros((QUERY_TILE, 1), F32), jnp.zeros((QUERY_TILE, HS), F32)),
    )
    out_ref[...] = (mixed / total).astype(BF)
    sum_ref[0] = total


def attend(heads, segment, low, high):
    tokens, columns = heads.shape
    count = columns // 3 // HS
    return call(
        attend_body,
        (count, tokens // QUERY_TILE),
        [
            pl.BlockSpec((QUERY_TILE, HS), lambda h, b, lo, hi: (b, h)),
            pl.BlockSpec((tokens, HS), lambda h, b, lo, hi: (0, count + h)),
            pl.BlockSpec((tokens, HS), lambda h, b, lo, hi: (0, 2 * count + h)),
            pl.BlockSpec((QUERY_TILE, 1), lambda h, b, lo, hi: (b, 0)),
            pl.BlockSpec((1, tokens), lambda h, b, lo, hi: (0, 0)),
        ],
        [
            pl.BlockSpec((QUERY_TILE, HS), lambda h, b, lo, hi: (b, h)),
            pl.BlockSpec((1, QUERY_TILE, 1), lambda h, b, lo, hi: (h, b, 0)),
        ],
        [shape((tokens, count * HS), BF), shape((count, tokens, 1), F32)],
        flops=4 * count * tokens * tokens * HS // 2,
        moved=8 * tokens * columns,
        prefetch=2,
        name="attend",
    )(low, high, heads, heads, heads, segment[:, None], segment[None, :])


def head_back(grad, raw, gain, cosine, sine):
    turned = grad * cosine - pltpu.roll(grad, HS // 2, 1) * sine
    factor = lax.rsqrt(jnp.mean(raw * raw, axis=1, keepdims=True) + EPSILON)
    unit = raw * factor
    gain_part = jnp.sum(turned * unit, axis=0, keepdims=True)
    pulled = turned * gain
    inner = jnp.mean(pulled * unit, axis=1, keepdims=True)
    return (pulled - unit * inner) * factor, gain_part


def attend_back_body(
    low, high, q_ref, k_ref, v_ref, g_ref, o_ref, s_ref, qs_ref, ks_ref, qr_ref, kr_ref,
    cos_ref, sin_ref, hg_ref, gq_ref, gk_ref, gv_ref, gain_ref, keys_ref, values_ref,
):
    block = pl.program_id(1)

    @pl.when(block == 0)
    def _():
        keys_ref[...] = jnp.zeros_like(keys_ref)
        values_ref[...] = jnp.zeros_like(values_ref)

    @pl.when((block == 0) & (pl.program_id(0) == 0))
    def _():
        gain_ref[...] = jnp.zeros_like(gain_ref)

    query, grad = q_ref[...], g_ref[...]
    query_docs = qs_ref[...]
    scale_back = 1.0 / s_ref[0]
    inner = jnp.sum(grad.astype(F32) * o_ref[...].astype(F32), axis=1, keepdims=True)

    def step(index, grad_query):
        rows = key_rows(index)
        key = k_ref[rows, :]
        scores = dot(query, key, 1, 1) * SCALE
        weights = jnp.where(query_docs == ks_ref[:, rows], jnp.exp(scores) * scale_back, 0.0)
        grad_weights = dot(grad, v_ref[rows, :], 1, 1)
        grad_scores = (weights * (grad_weights - inner)).astype(BF)
        values_ref[rows, :] += dot(weights.astype(BF), grad, 0, 0)
        keys_ref[rows, :] += dot(grad_scores, query, 0, 0)
        return grad_query + dot(grad_scores, key)

    grad_query = lax.fori_loop(
        low[block], high[block], step, jnp.zeros((QUERY_TILE, HS), F32)
    )
    rows = pl.ds(pl.multiple_of(block * QUERY_TILE, QUERY_TILE), QUERY_TILE)
    back, part = head_back(
        grad_query * SCALE, qr_ref[...], hg_ref[0:1, :], cos_ref[rows, :], sin_ref[rows, :]
    )
    gq_ref[...] = back.astype(BF)
    gain_ref[0:1, :] += part

    @pl.when(block == pl.num_programs(1) - 1)
    def _():
        back, part = head_back(
            keys_ref[...] * SCALE, kr_ref[...], hg_ref[1:2, :], cos_ref[...], sin_ref[...]
        )
        gk_ref[...] = back.astype(BF)
        gain_ref[1:2, :] += part
        gv_ref[...] = values_ref[...].astype(BF)


def attend_back(heads, grad_mixed, mixed, sums, segment, low, high, raw, cosine, sine, gains):
    tokens, columns = heads.shape
    count = columns // 3 // HS
    whole = lambda h, b, lo, hi: (0, 0)
    tile = lambda h, b, lo, hi: (b, h)
    column = lambda h, b, lo, hi: (0, h)
    return call(
        attend_back_body,
        (count, tokens // QUERY_TILE),
        [
            pl.BlockSpec((QUERY_TILE, HS), tile),
            pl.BlockSpec((tokens, HS), lambda h, b, lo, hi: (0, count + h)),
            pl.BlockSpec((tokens, HS), lambda h, b, lo, hi: (0, 2 * count + h)),
            pl.BlockSpec((QUERY_TILE, HS), tile),
            pl.BlockSpec((QUERY_TILE, HS), tile),
            pl.BlockSpec((1, QUERY_TILE, 1), lambda h, b, lo, hi: (h, b, 0)),
            pl.BlockSpec((QUERY_TILE, 1), lambda h, b, lo, hi: (b, 0)),
            pl.BlockSpec((1, tokens), whole),
            pl.BlockSpec((QUERY_TILE, HS), tile),
            pl.BlockSpec((tokens, HS), lambda h, b, lo, hi: (0, count + h)),
            pl.BlockSpec((tokens, HS), whole),
            pl.BlockSpec((tokens, HS), whole),
            pl.BlockSpec((2, HS), whole),
        ],
        [
            pl.BlockSpec((QUERY_TILE, HS), tile),
            pl.BlockSpec((tokens, HS), column),
            pl.BlockSpec((tokens, HS), column),
            pl.BlockSpec((2, HS), whole),
        ],
        [shape((tokens, count * HS), BF)] * 3 + [shape((2, HS), F32)],
        scratch=[pltpu.VMEM((tokens, HS), F32), pltpu.VMEM((tokens, HS), F32)],
        flops=10 * count * tokens * tokens * HS // 2,
        moved=24 * tokens * columns,
        prefetch=2,
        name="attend_back",
    )(
        low, high, heads, heads, heads, grad_mixed, mixed, sums, segment[:, None],
        segment[None, :], raw, raw, cosine, sine, gains,
    )


def dispatch_body(slot_ref, x_ref, out_ref):
    local, capacity = out_ref.shape[1], out_ref.shape[3]
    tokens = x_ref.shape[1]
    rows = x_ref[0]
    order = lax.broadcasted_iota(jnp.int32, (capacity, tokens), 0)
    for index in range(local):
        hot = jnp.where(order == slot_ref[0, 0, index : index + 1, :], 1.0, 0.0).astype(BF)
        out_ref[0, index, 0] = dot(hot, rows).astype(BF)


def dispatch(slots, rows, capacity):
    groups, targets, local, tokens = slots.shape
    features = rows.shape[2]
    return call(
        dispatch_body,
        (groups, targets),
        [
            pl.BlockSpec((1, 1, local, tokens), lambda g, d: (g, d, 0, 0)),
            pl.BlockSpec((1, tokens, features), lambda g, d: (g, 0, 0)),
        ],
        pl.BlockSpec((1, local, 1, capacity, features), lambda g, d: (d, 0, g, 0, 0)),
        shape((targets, local, groups, capacity, features), BF),
        flops=2 * groups * targets * local * capacity * tokens * features,
        moved=2 * groups * features * (tokens + targets * local * capacity),
        name="dispatch",
    )(slots, rows)


def combine_body(slot_ref, rows_ref, out_ref):
    targets, local, _, capacity, features = rows_ref.shape
    tile = out_ref.shape[1]
    order = lax.broadcasted_iota(jnp.int32, (tile, capacity), 1)
    slots = slot_ref[0]
    total = jnp.zeros((tile, features), F32)
    for target in range(targets):
        hot = jnp.concatenate(
            [
                jnp.where(
                    order == slots[:, target * local + i : target * local + i + 1], 1.0, 0.0
                ).astype(BF)
                for i in range(local)
            ],
            axis=1,
        )
        total = total + dot(hot, rows_ref[target].reshape(local * capacity, features))
    out_ref[0] = total.astype(BF)


def combine(slots_by_token, rows):
    groups, tokens, experts = slots_by_token.shape
    targets, local, _, capacity, features = rows.shape
    tile = 512
    return call(
        combine_body,
        (groups, tokens // tile),
        [
            pl.BlockSpec((1, tile, experts), lambda g, t: (g, t, 0)),
            pl.BlockSpec((targets, local, 1, capacity, features), lambda g, t: (0, 0, g, 0, 0)),
        ],
        pl.BlockSpec((1, tile, features), lambda g, t: (g, t, 0)),
        shape((groups, tokens, features), BF),
        flops=2 * groups * targets * local * capacity * tokens * features,
        moved=2 * groups * features * (tokens + targets * local * capacity),
        name="combine",
    )(slots_by_token, rows)


def block_rows(ref, row=0):
    _, cores, _, groups, capacity, features = ref.shape
    return ref[row].reshape(cores * groups * capacity, features)


def gate_up_body(*refs):
    x_refs, (gate_w, up_w, gate_ref, up_ref, act_ref) = refs[:CHUNKS], refs[CHUNKS:]
    width = x_refs[0].shape[-1]
    gate = up = None
    for row in range(x_refs[0].shape[0]):
        for chunk, x_ref in enumerate(x_refs):
            x = block_rows(x_ref, row)
            features = pl.ds((row * CHUNKS + chunk) * width, width)
            gate_part = dot(x, gate_w[0, features, :])
            up_part = dot(x, up_w[0, features, :])
            gate = gate_part if gate is None else gate + gate_part
            up = up_part if up is None else up + up_part
    gate_ref[0] = gate.astype(BF)
    up_ref[0] = up.astype(BF)
    act_ref[0] = (gate / (1.0 + jnp.exp(-gate)) * up).astype(BF)


def gate_up(chunks, gate_weight, up_weight):
    rows, cores, local, groups, capacity, width = chunks[0].shape
    _, features, hidden = gate_weight.shape
    slots = groups * capacity
    tile = min(512, hidden)
    out = shape((local, cores * slots, hidden), BF)
    out_spec = pl.BlockSpec((1, slots, tile), lambda i, n, k: (i, k, n))
    w_spec = pl.BlockSpec((1, features, tile), lambda i, n, k: (i, 0, n))
    return call(
        gate_up_body,
        (local, hidden // tile, cores),
        [
            pl.BlockSpec((rows, 1, 1, groups, capacity, width), lambda i, n, k: (0, k, i, 0, 0, 0))
        ]
        * CHUNKS
        + [w_spec, w_spec],
        [out_spec] * 3,
        [out] * 3,
        flops=4 * local * cores * slots * features * hidden,
        moved=local * (8 * features * hidden + 4 * cores * slots * features),
        name="gate_up",
    )(*chunks, gate_weight, up_weight)


def produce_body(*refs):
    act_ref, w_ref, prob_ref = refs[:3]
    c_refs, out_refs, inner_ref = refs[3 : 3 + CHUNKS], refs[3 + CHUNKS : -1], refs[-1]
    width = c_refs[0].shape[-1]

    @pl.when(pl.program_id(2) == 0)
    def _():
        inner_ref[...] = jnp.zeros_like(inner_ref)

    act, prob = act_ref[0], prob_ref[0]
    inner = jnp.zeros(prob.shape, F32)
    for chunk in range(CHUNKS):
        made = dot(act, w_ref[0, pl.ds(chunk * width, width), :], 1, 1)
        inner += jnp.sum(made * block_rows(c_refs[chunk]).astype(F32), axis=1, keepdims=True)
        out_refs[chunk][...] = (made * prob).astype(BF).reshape(out_refs[chunk].shape)
    inner_ref[0] += inner


def produce(activated, down_weight, prob, cots):
    rows, cores, local, groups, capacity, width = cots[0].shape
    hidden = activated.shape[2]
    slots = groups * capacity
    row_spec = pl.BlockSpec((1, 1, 1, groups, capacity, width), lambda i, k, r: (r, k, i, 0, 0, 0))
    column = pl.BlockSpec((1, slots, 1), lambda i, k, r: (i, k, 0))
    outs = call(
        produce_body,
        (local, cores, rows),
        [
            pl.BlockSpec((1, slots, hidden), lambda i, k, r: (i, k, 0)),
            pl.BlockSpec((1, width * CHUNKS, hidden), lambda i, k, r: (i, r, 0)),
            column,
        ]
        + [row_spec] * CHUNKS,
        [row_spec] * CHUNKS + [column],
        [shape(cots[0].shape, BF)] * CHUNKS + [shape((local, cores * slots, 1), F32)],
        flops=2 * local * cores * slots * D * hidden,
        moved=local * (2 * D * hidden + 8 * cores * slots * D),
        name="produce",
    )(activated, down_weight, prob, *cots)
    return outs[:CHUNKS], outs[CHUNKS]


def act_back_body(*refs):
    c_refs = refs[:CHUNKS]
    w_ref, prob_ref, gate_ref, up_ref, gate_out, up_out = refs[CHUNKS:]
    width = c_refs[0].shape[-1]
    prob = prob_ref[0]
    grad = None
    for row in range(c_refs[0].shape[0]):
        for chunk, c_ref in enumerate(c_refs):
            c = (block_rows(c_ref, row).astype(F32) * prob).astype(BF)
            part = dot(c, w_ref[0, pl.ds((row * CHUNKS + chunk) * width, width), :])
            grad = part if grad is None else grad + part
    gate, up = gate_ref[0].astype(F32), up_ref[0].astype(F32)
    squashed = 1.0 / (1.0 + jnp.exp(-gate))
    gate_out[0] = (grad * up * squashed * (1.0 + gate * (1.0 - squashed))).astype(BF)
    up_out[0] = (grad * gate * squashed).astype(BF)


def act_back(cots, down_weight, prob, gate, up):
    rows, cores, local, groups, capacity, width = cots[0].shape
    _, features, hidden = down_weight.shape
    slots = groups * capacity
    tile = min(512, hidden)
    spec = pl.BlockSpec((1, slots, tile), lambda i, n, k: (i, k, n))
    return call(
        act_back_body,
        (local, hidden // tile, cores),
        [
            pl.BlockSpec((rows, 1, 1, groups, capacity, width), lambda i, n, k: (0, k, i, 0, 0, 0))
        ]
        * CHUNKS
        + [
            pl.BlockSpec((1, features, tile), lambda i, n, k: (i, 0, n)),
            pl.BlockSpec((1, slots, 1), lambda i, n, k: (i, k, 0)),
            spec,
            spec,
        ],
        [spec] * 2,
        [shape(gate.shape, BF)] * 2,
        flops=2 * local * cores * slots * features * hidden,
        moved=local * (2 * features * hidden + 2 * cores * slots * features),
        name="act_back",
    )(*cots, down_weight, prob, gate, up)


def down_grad_body(*refs):
    c_refs, (prob_ref, act_ref, out_ref) = refs[:CHUNKS], refs[CHUNKS:]
    width = c_refs[0].shape[-1]
    for chunk, c_ref in enumerate(c_refs):
        c = (block_rows(c_ref).astype(F32) * prob_ref[0]).astype(BF)
        out_ref[0, pl.ds(chunk * width, width), :] = dot(c, act_ref[0], 0, 0)


def down_grad(cots, prob, activated):
    rows, cores, local, groups, capacity, width = cots[0].shape
    slots, hidden = activated.shape[1:]
    return call(
        down_grad_body,
        (local, rows),
        [
            pl.BlockSpec((1, cores, 1, groups, capacity, width), lambda i, r: (r, 0, i, 0, 0, 0))
        ]
        * CHUNKS
        + [
            pl.BlockSpec((1, slots, 1), lambda i, r: (i, 0, 0)),
            pl.BlockSpec((1, slots, hidden), lambda i, r: (i, 0, 0)),
        ],
        pl.BlockSpec((1, width * CHUNKS, hidden), lambda i, r: (i, r, 0)),
        shape((local, rows * width * CHUNKS, hidden), F32),
        flops=2 * local * slots * D * hidden,
        moved=local * (4 * D * hidden + 2 * slots * D),
        name="down_grad",
    )(*cots, prob, activated)


def gate_grad_body(*refs):
    x_refs, (gate_ref, up_ref, gate_out, up_out) = refs[:CHUNKS], refs[CHUNKS:]
    width = x_refs[0].shape[-1]
    for chunk, x_ref in enumerate(x_refs):
        x = block_rows(x_ref)
        features = pl.ds(chunk * width, width)
        gate_out[0, features, :] = dot(x, gate_ref[0], 0, 0)
        up_out[0, features, :] = dot(x, up_ref[0], 0, 0)


def gate_grad(chunks, grad_gate_pre, grad_up_pre):
    rows, cores, local, groups, capacity, width = chunks[0].shape
    slots, hidden = grad_gate_pre.shape[1:]
    wide = pl.BlockSpec((1, slots, hidden), lambda i, r: (i, 0, 0))
    out = pl.BlockSpec((1, width * CHUNKS, hidden), lambda i, r: (i, r, 0))
    return call(
        gate_grad_body,
        (local, rows),
        [
            pl.BlockSpec((1, cores, 1, groups, capacity, width), lambda i, r: (r, 0, i, 0, 0, 0))
        ]
        * CHUNKS
        + [wide, wide],
        [out, out],
        [shape((local, rows * width * CHUNKS, hidden), F32)] * 2,
        flops=4 * local * slots * D * hidden,
        moved=local * (8 * D * hidden + 2 * slots * D),
        name="gate_grad",
    )(*chunks, grad_gate_pre, grad_up_pre)


def rows_back_body(gate_ref, up_ref, gate_w, up_w, out_ref):
    made = dot(gate_ref[0], gate_w[0], 1, 1) + dot(up_ref[0], up_w[0], 1, 1)
    out_ref[...] = made.astype(BF).reshape(out_ref.shape)


def rows_back(grad_gate_pre, grad_up_pre, gate_weight, up_weight, chunk, dims):
    rows, cores, local, groups, capacity, width = dims
    hidden = gate_weight.shape[2]
    slots = groups * capacity
    pre = pl.BlockSpec((1, slots, hidden), lambda i, k, r: (i, k, 0))
    weight = pl.BlockSpec((1, width, hidden), lambda i, k, r: (i, r * CHUNKS + chunk, 0))
    return call(
        rows_back_body,
        (local, cores, rows),
        [pre, pre, weight, weight],
        pl.BlockSpec((1, 1, 1, groups, capacity, width), lambda i, k, r: (r, k, i, 0, 0, 0)),
        shape(dims, BF),
        flops=4 * local * cores * slots * width * rows * hidden,
        moved=local * (4 * rows * width * hidden + 6 * cores * slots * width * rows),
        name="rows_back",
    )(grad_gate_pre, grad_up_pre, gate_weight, up_weight)


def swap(rows):
    return lax.all_to_all(rows, SWAP_AXES, split_axis=0, concat_axis=0, tiled=True)


def slot_positions(routes, ranks, capacity):
    experts = jnp.arange(E, dtype=jnp.int32)
    member = jnp.any(routes.T[:, None, :] == experts[None, :, None], axis=0)
    earlier = (ranks[:, None] < ranks[None, :]).astype(BF)
    position = jnp.dot(member.astype(BF), earlier, preferred_element_type=F32)
    return jnp.where(member & (position < capacity), position, -1.0)


def per_device(
    hidden_in,
    attention_gain,
    query_weight,
    key_weight,
    value_weight,
    projection,
    query_gain,
    key_gain,
    feedforward_gain,
    router_weight,
    gate_weight,
    up_weight,
    down_weight,
    segments,
    routes,
    priority,
    cotangent,
):
    tokens, width_here = hidden_in.shape
    row_count = lax.axis_size("row")
    z_count = lax.axis_size("z")
    core_count = lax.axis_size("core")
    local = gate_weight.shape[0]
    piece_count = row_count * z_count * core_count * local
    pieces = max(1, piece_count // E)
    capacity = tokens * TOPK // E
    width = width_here // CHUNKS
    row_index = lax.axis_index("row")
    z_index = lax.axis_index("z")
    core_index = lax.axis_index("core")
    offset = row_index * width_here
    head_columns = query_weight.shape[1]
    head_count = head_columns // HS

    hidden_full = lax.all_gather(hidden_in, "row", axis=1, tiled=True)
    gain_full = lax.all_gather(attention_gain, "row", axis=0, tiled=True)
    qkv_full = lax.all_gather(
        jnp.concatenate([query_weight, key_weight, value_weight], axis=1),
        TOKENS_AXES,
        axis=0,
        tiled=True,
    )
    projection_full = lax.all_gather(projection, TOKENS_AXES, axis=0, tiled=True)
    router_full = lax.all_gather(
        lax.all_gather(router_weight.T, TOKENS_AXES, axis=1, tiled=True), "row", axis=0, tiled=True
    )
    router_here = lax.dynamic_slice_in_dim(router_full, offset, width_here, 1)

    position = slot_positions(routes, priority[0], capacity)
    by_group = lax.all_gather(position.astype(BF), "z", axis=0)
    by_piece = jnp.repeat(by_group, pieces, axis=1).reshape(
        z_count, row_count, z_count, core_count * local, tokens
    )
    mine = lax.dynamic_index_in_dim(by_piece, z_index, 2, keepdims=False).astype(jnp.int32)
    slots = mine.reshape(z_count, row_count * core_count, local, tokens)
    slots_by_token = jnp.swapaxes(
        mine.reshape(z_count, row_count * core_count * local, tokens), 1, 2
    )
    dims = (row_count, core_count, local, z_count, capacity, width)

    def send(values):
        received = []
        for chunk in range(CHUNKS):
            part = values[:, chunk * width : (chunk + 1) * width]
            spread = lax.all_gather(part, "z", axis=0)
            received.append(swap(dispatch(slots, spread, capacity)).reshape(dims))
        return received

    def gather_back(chunks):
        parts = []
        for chunk in chunks:
            summed = combine(
                slots_by_token, swap(chunk.reshape((row_count * core_count,) + dims[2:]))
            )
            parts.append(
                lax.psum_scatter(summed, "z", scatter_dimension=0, tiled=True).reshape(
                    tokens, width
                )
            )
        return jnp.concatenate(parts, axis=1).astype(F32)

    cots = send(cotangent)

    cosine, sine = rotary_tables()
    first_gain = attention_gain.astype(F32)
    second_gain = feedforward_gain.astype(F32)
    head_gains = jnp.stack([query_gain, key_gain]).astype(F32)
    residual = hidden_in.astype(F32)
    gain_row = gain_full.astype(F32)[None, :]
    normed_one, heads, raw = project(
        hidden_full,
        gain_row,
        qkv_full,
        cosine,
        sine,
        jnp.repeat(head_gains, head_count, axis=0).reshape(1, -1),
    )
    segment = segments[0]
    low, high = key_ranges(segment)
    mixed, sums = attend(heads, segment, low, high)
    branch = lax.psum_scatter(
        dot(mixed, projection_full, 1, 1).astype(BF), "row", scatter_dimension=1, tiled=True
    )
    middle = residual + branch.astype(F32)
    second_factor = lax.rsqrt(lax.psum(jnp.sum(middle * middle, axis=1), "row") / D + EPSILON)[
        :, None
    ]
    normed_two = (middle * second_factor * second_gain).astype(BF)

    logits = jnp.sum(lax.all_gather(dot(router_here, normed_two, 1, 1), "row", axis=0), axis=0)
    raised = jnp.exp(logits)
    router_probs = raised / jnp.sum(raised, axis=0, keepdims=True)

    rows = send(normed_two)
    experts_here = E // row_count
    own_slots = lax.dynamic_slice_in_dim(position, row_index * experts_here, experts_here, 0)
    own_probs = lax.dynamic_slice_in_dim(router_probs, row_index * experts_here, experts_here, 0)
    order = jnp.arange(capacity, dtype=jnp.int32).astype(F32)
    slot_prob = jnp.sum(
        jnp.where(own_slots[:, None, :] == order[None, :, None], own_probs[:, None, :], 0.0), axis=2
    )
    prob_groups = jnp.repeat(
        lax.all_gather(slot_prob, TOKENS_AXES, axis=0), pieces, axis=1
    ).reshape(z_count, core_count, z_count, core_count, local, capacity)
    prob_here = lax.dynamic_index_in_dim(
        lax.dynamic_index_in_dim(prob_groups, z_index, 2, keepdims=False),
        core_index,
        2,
        keepdims=False,
    )
    prob = jnp.transpose(prob_here, (2, 1, 0, 3)).reshape(
        local, core_count * z_count * capacity, 1
    )
    gate, up, activated = gate_up(rows, gate_weight, up_weight)
    grad_gate_pre, grad_up_pre = act_back(cots, down_weight, prob, gate, up)
    grad_rows = [
        rows_back(grad_gate_pre, grad_up_pre, gate_weight, up_weight, chunk, dims)
        for chunk in range(CHUNKS)
    ]
    grad_normed_two = gather_back(grad_rows)
    produced, inner = produce(activated, down_weight, prob, cots)
    grad_down = down_grad(cots, prob, activated)
    grad_gate, grad_up = gate_grad(rows, grad_gate_pre, grad_up_pre)
    output = (middle + gather_back(produced)).astype(BF)

    every = lax.all_gather(
        inner.reshape(local, core_count, z_count, capacity), ALL_AXES, axis=0
    )
    of_group = lax.dynamic_index_in_dim(
        lax.dynamic_index_in_dim(every, core_index, 2, keepdims=False), z_index, 2, keepdims=False
    )
    slot_grads = jnp.sum(of_group.reshape(E, pieces, capacity), axis=1)
    grad_prob = jnp.sum(
        jnp.where(position[:, None, :] == order[None, :, None], slot_grads[:, :, None], 0.0), axis=1
    )
    grad_logits = (
        router_probs * (grad_prob - jnp.sum(router_probs * grad_prob, axis=0, keepdims=True))
    ).astype(BF)
    grad_normed_two = grad_normed_two + dot(grad_logits, router_here, 0, 0)
    router_part = dot(grad_logits, normed_two)
    router_swapped = lax.all_to_all(
        router_part.reshape(row_count, experts_here, width_here), "row", 0, 0, tiled=True
    )
    grad_router = lax.psum_scatter(
        jnp.swapaxes(router_swapped, 0, 1).reshape(experts_here, D),
        TOKENS_AXES,
        scatter_dimension=1,
        tiled=True,
    ).T

    scaled_two = grad_normed_two * second_gain
    second_inner = lax.psum(jnp.sum(scaled_two * middle, axis=1), "row")[:, None]
    grad_middle = (
        cotangent.astype(F32)
        + scaled_two * second_factor
        - middle * second_factor**3 * second_inner / D
    )
    grad_feedforward_gain = jnp.sum(grad_normed_two * middle * second_factor, axis=0)

    grad_branch = lax.all_gather(grad_middle.astype(BF), "row", axis=1, tiled=True)
    grad_mixed = dot(grad_branch, projection_full).astype(BF)
    grad_projection = dot(grad_branch, mixed, 0, 0).astype(BF)
    grad_query_raw, grad_key_raw, grad_value_raw, head_gain_grads = attend_back(
        heads, grad_mixed, mixed, sums, segment, low, high, raw, cosine, sine, head_gains
    )
    grad_raw = jnp.concatenate([grad_query_raw, grad_key_raw, grad_value_raw], axis=1)
    first_part = dot(grad_raw, qkv_full, 1, 1)
    first_inner = lax.psum(
        jnp.sum(first_part * gain_row * hidden_full.astype(F32), axis=1), "row"
    )[:, None]
    grad_first = lax.psum_scatter(
        first_part.astype(BF), "row", scatter_dimension=1, tiled=True
    ).astype(F32)
    grad_qkv = dot(normed_one, grad_raw, 0, 0).astype(BF)
    first_factor = lax.rsqrt(
        jnp.mean(jnp.square(hidden_full.astype(F32)), axis=1, keepdims=True) + EPSILON
    )
    scaled_one = grad_first * first_gain
    grad_input = (
        grad_middle + scaled_one * first_factor - residual * first_factor**3 * first_inner / D
    )
    grad_attention_gain = jnp.sum(grad_first * residual * first_factor, axis=0)

    padded_first = lax.dynamic_update_slice(jnp.zeros((D,), F32), grad_attention_gain, (offset,))
    padded_second = lax.dynamic_update_slice(jnp.zeros((D,), F32), grad_feedforward_gain, (offset,))
    totals = lax.psum((padded_first, padded_second, head_gain_grads), ALL_AXES)
    grad_projection = lax.psum_scatter(
        grad_projection, TOKENS_AXES, scatter_dimension=0, tiled=True
    ).astype(F32)
    grad_qkv = lax.psum_scatter(grad_qkv, TOKENS_AXES, scatter_dimension=0, tiled=True).astype(F32)
    return (
        output,
        grad_input,
        lax.dynamic_slice_in_dim(totals[0], offset, width_here),
        grad_qkv[:, :head_columns],
        grad_qkv[:, head_columns : 2 * head_columns],
        grad_qkv[:, 2 * head_columns :],
        grad_projection,
        totals[2][0],
        totals[2][1],
        lax.dynamic_slice_in_dim(totals[1], offset, width_here),
        grad_router,
        grad_gate,
        grad_up,
        grad_down,
    )


def solution(mesh):
    rows, columns = mesh.shape["row"], mesh.shape["col"]
    split_mesh = Mesh(
        mesh.devices.reshape(rows, columns // 2, 2), ("row", "z", "core")
    )
    both = P(TOKENS_AXES, "row")
    expert = P(ALL_AXES, None, None)
    grouped = P(TOKENS_AXES, None)
    return jax.shard_map(
        per_device,
        mesh=split_mesh,
        in_specs=(
            both, P("row"), both, both, both, both, P(), P(), P("row"), both,
            expert, expert, expert, grouped, grouped, grouped, both,
        ),
        out_specs=(
            both, both, P("row"), both, both, both, both, P(), P(), P("row"), both,
            expert, expert, expert,
        ),
        check_vma=False,
    )
```

```python
import functools

import jax
import jax.numpy as jnp
from jax import lax
from jax.experimental import pallas as pl
from jax.experimental.pallas import tpu as pltpu
from jax.sharding import Mesh, PartitionSpec as P

D = 2048
HS = 128
E = 64
TOPK = 8
SEQ = 2048
EPSILON = 1e-06
SCALE = HS ** (-0.5)
CHUNKS = 2
TOKENS_AXES = ("z", "core")
SWAP_AXES = ("row", "core")
ALL_AXES = ("row", "z", "core")
BF = jnp.bfloat16
F32 = jnp.float32
VMEM_BYTES = 60 * 1024 * 1024


def call(body, grid, in_specs, out_specs, out_shape, scratch=(), flops=0, moved=0, prefetch=0, name=None):
    return pl.pallas_call(
        body,
        out_shape=out_shape,
        grid_spec=pltpu.PrefetchScalarGridSpec(
            num_scalar_prefetch=prefetch,
            grid=grid,
            in_specs=in_specs,
            out_specs=out_specs,
            scratch_shapes=list(scratch),
        ),
        compiler_params=pltpu.CompilerParams(
            dimension_semantics=("arbitrary",) * len(grid), vmem_limit_bytes=VMEM_BYTES
        ),
        cost_estimate=pl.CostEstimate(flops=flops, bytes_accessed=moved, transcendentals=0),
        name=name,
    )


def shape(dims, dtype):
    return jax.ShapeDtypeStruct(dims, dtype)


def dot(left, right, left_dim=1, right_dim=0):
    return lax.dot_general(
        left, right, (((left_dim,), (right_dim,)), ((), ())), preferred_element_type=F32
    )


def rotary_tables():
    half_size = HS // 2
    inverse = 50000.0 ** (-(jnp.arange(half_size, dtype=F32) * 2.0) / HS)
    angles = jnp.arange(SEQ, dtype=F32)[:, None] * inverse[None, :]
    cosine, sine = jnp.cos(angles), jnp.sin(angles)
    return (
        jnp.concatenate([cosine, cosine], axis=1),
        jnp.concatenate([-sine, sine], axis=1),
    )


def project_body(starts, *refs):
    count = starts.shape[0]
    x_refs, refs = refs[:count], refs[count:]
    gain_ref, w_ref, cos_ref, sin_ref, hg_ref, normed_ref, heads_ref, raw_ref, factor_ref = refs
    width = x_refs[0].shape[1]
    square = sum(
        jnp.sum(jnp.square(x_ref[...].astype(F32)), axis=1, keepdims=True) for x_ref in x_refs
    )
    factor = lax.rsqrt(square / (width * count) + EPSILON)
    factor_ref[...] = factor
    raw = None
    for index, x_ref in enumerate(x_refs):
        features = pl.ds(pl.multiple_of(starts[index], width), width)
        normed = (x_ref[...].astype(F32) * factor * gain_ref[:, features]).astype(BF)
        normed_ref[:, features] = normed
        part = dot(normed, w_ref[features, :])
        raw = part if raw is None else raw + part
    turned = raw_ref.shape[1]
    raw_ref[...] = raw[:, :turned]
    cosine, sine = cos_ref[...], sin_ref[...]
    for head in range(turned // HS):
        part = raw[:, head * HS : (head + 1) * HS]
        unit = part * lax.rsqrt(jnp.mean(part * part, axis=1, keepdims=True) + EPSILON)
        scaled = unit * hg_ref[:, head * HS : (head + 1) * HS]
        heads_ref[:, head * HS : (head + 1) * HS] = (
            scaled * cosine + pltpu.roll(scaled, HS // 2, 1) * sine
        ).astype(BF)
    heads_ref[:, turned:] = raw[:, turned:].astype(BF)


def project(starts, pieces, gain, weights, cosine, sine, head_gains):
    tokens, piece = pieces[0].shape
    width, columns = weights.shape
    turned = columns // 3 * 2
    tile = 256
    own = lambda t, s: (t, 0)
    whole = lambda t, s: (0, 0)
    return call(
        project_body,
        (tokens // tile,),
        [pl.BlockSpec((tile, piece), own)] * len(pieces)
        + [
            pl.BlockSpec((1, width), whole),
            pl.BlockSpec((width, columns), whole),
            pl.BlockSpec((tile, HS), own),
            pl.BlockSpec((tile, HS), own),
            pl.BlockSpec((1, turned), whole),
        ],
        [
            pl.BlockSpec((tile, width), own),
            pl.BlockSpec((tile, columns), own),
            pl.BlockSpec((tile, turned), own),
            pl.BlockSpec((tile, 1), own),
        ],
        [
            shape((tokens, width), BF),
            shape((tokens, columns), BF),
            shape((tokens, turned), F32),
            shape((tokens, 1), F32),
        ],
        flops=2 * tokens * width * columns,
        moved=6 * tokens * width + 2 * width * columns + 6 * tokens * columns,
        prefetch=1,
        name="project",
    )(starts, *pieces, gain, weights, cosine, sine, head_gains)


def mix_back_body(starts, *refs):
    count = starts.shape[0]
    g_refs, (w_ref, out_ref) = refs[:count], refs[count:]
    width = g_refs[0].shape[1]
    total = None
    for index, g_ref in enumerate(g_refs):
        part = dot(g_ref[...], w_ref[pl.ds(pl.multiple_of(starts[index], width), width), :])
        total = part if total is None else total + part
    out_ref[...] = total.astype(BF)


def mix_back(starts, pieces, weights):
    tokens, piece = pieces[0].shape
    width, columns = weights.shape
    tile = 256
    return call(
        mix_back_body,
        (tokens // tile,),
        [pl.BlockSpec((tile, piece), lambda t, s: (t, 0))] * len(pieces)
        + [pl.BlockSpec((width, columns), lambda t, s: (0, 0))],
        pl.BlockSpec((tile, columns), lambda t, s: (t, 0)),
        shape((tokens, columns), BF),
        flops=2 * tokens * width * columns,
        moved=2 * tokens * width + 2 * width * columns + 2 * tokens * columns,
        prefetch=1,
        name="mix_back",
    )(starts, *pieces, weights)


def projection_grad_body(starts, *refs):
    count = starts.shape[0]
    g_refs, (mixed_ref, out_ref, total_ref) = refs[:count], refs[count:]
    width = g_refs[0].shape[1]

    @pl.when(pl.program_id(0) == 0)
    def _():
        total_ref[...] = jnp.zeros_like(total_ref)

    for index, g_ref in enumerate(g_refs):
        rows = pl.ds(pl.multiple_of(starts[index], width), width)
        total_ref[rows, :] += dot(g_ref[...], mixed_ref[...], 0, 0)

    @pl.when(pl.program_id(0) == pl.num_programs(0) - 1)
    def _():
        out_ref[...] = total_ref[...].astype(BF)


def projection_grad(starts, pieces, mixed):
    tokens, piece = pieces[0].shape
    columns = mixed.shape[1]
    width = piece * len(pieces)
    tile = 512
    return call(
        projection_grad_body,
        (tokens // tile,),
        [pl.BlockSpec((tile, piece), lambda t, s: (t, 0))] * len(pieces)
        + [pl.BlockSpec((tile, columns), lambda t, s: (t, 0))],
        pl.BlockSpec((width, columns), lambda t, s: (0, 0)),
        shape((width, columns), BF),
        scratch=[pltpu.VMEM((width, columns), F32)],
        flops=2 * tokens * width * columns,
        moved=2 * tokens * width + 2 * width * columns + 2 * tokens * columns,
        prefetch=1,
        name="projection_grad",
    )(starts, *pieces, mixed)


def permute(values, mask):
    return lax.ppermute(values, "row", [(i, i ^ mask) for i in range(4)])


def row_gather(values):
    width = values.shape[1]
    if lax.axis_size("row") != 4:
        return [lax.all_gather(values, "row", axis=1, tiled=True)], jnp.zeros((1,), jnp.int32)
    half = width // 2
    left, right = values[:, :half], values[:, half:]
    left_1, right_2 = permute(left, 1), permute(right, 2)
    left_2, right_1 = permute(left, 2), permute(right, 1)
    left_3, right_3 = permute(left_1, 2), permute(right_2, 1)
    me = lax.axis_index("row")
    starts = jnp.stack(
        [(me ^ mask) * width + side * half for mask in range(4) for side in range(2)]
    ).astype(jnp.int32)
    return [left, right, left_1, right_1, left_2, right_2, left_3, right_3], starts


def row_scatter_order(weights):
    if lax.axis_size("row") != 4:
        return weights
    width = weights.shape[0] // 4
    half = width // 2
    me = lax.axis_index("row")
    order = [(1, 0), (3, 0), (2, 1), (3, 1), (2, 0), (1, 1), (0, 0), (0, 1)]
    return jnp.concatenate(
        [
            lax.dynamic_slice_in_dim(weights, (me ^ mask) * width + side * half, half, 0)
            for mask, side in order
        ],
        axis=0,
    )


def row_scatter(left, ordered):
    if lax.axis_size("row") != 4:
        return lax.psum_scatter(
            dot(left, ordered, 1, 1).astype(BF), "row", scatter_dimension=1, tiled=True
        ).astype(F32)
    width = ordered.shape[0] // 4
    half = width // 2
    part = lambda index: dot(left, ordered[index * width : (index + 1) * width], 1, 1)
    from_x = permute(part(0).astype(BF), 1).astype(F32)
    from_y = permute(part(1).astype(BF), 2).astype(F32)
    onward, own = part(2), part(3)
    last_left = permute((onward[:, :half] + from_x[:, half:]).astype(BF), 2).astype(F32)
    last_right = permute((onward[:, half:] + from_y[:, half:]).astype(BF), 1).astype(F32)
    return jnp.concatenate(
        [
            own[:, :half] + from_x[:, :half] + last_left,
            own[:, half:] + from_y[:, :half] + last_right,
        ],
        axis=1,
    )


QUERY_TILE = 256
KEY_TILE = 256
EXP2_SCALE = SCALE * 1.4426950408889634


def key_ranges(segment):
    first = segment[::QUERY_TILE]
    last = segment[QUERY_TILE - 1 :: QUERY_TILE]
    key_first = segment[::KEY_TILE]
    key_last = segment[KEY_TILE - 1 :: KEY_TILE]
    meets = (key_first[None, :] <= last[:, None]) & (key_last[None, :] >= first[:, None])
    order = jnp.arange(meets.shape[1], dtype=jnp.int32)[None, :]
    low = jnp.min(jnp.where(meets, order, meets.shape[1]), axis=1)
    high = jnp.max(jnp.where(meets, order + 1, 0), axis=1)
    return low.astype(jnp.int32), high.astype(jnp.int32)


def key_rows(step):
    return pl.ds(pl.multiple_of(step * KEY_TILE, KEY_TILE), KEY_TILE)


def head(ref, index, rows=slice(None)):
    return ref[rows, index * HS : (index + 1) * HS]


def attend_body(low, high, q_ref, k_ref, v_ref, qs_ref, ks_ref, out_ref, sum_ref):
    block = pl.program_id(0)
    count = q_ref.shape[1] // HS
    query_docs = qs_ref[...]

    def step(index, state):
        rows = key_rows(index)
        allowed = query_docs == ks_ref[:, rows]
        scores = [dot(head(q_ref, h), head(k_ref, h, rows), 1, 1) for h in range(count)]
        raised = [jnp.where(allowed, jnp.exp2(each * EXP2_SCALE), 0.0) for each in scores]
        return tuple(
            (
                total + jnp.sum(each, axis=1, keepdims=True),
                mixed + dot(each.astype(BF), head(v_ref, h, rows)),
            )
            for h, (each, (total, mixed)) in enumerate(zip(raised, state))
        )

    state = lax.fori_loop(
        low[block],
        high[block],
        step,
        ((jnp.zeros((QUERY_TILE, 1), F32), jnp.zeros((QUERY_TILE, HS), F32)),) * count,
    )
    for h, (total, mixed) in enumerate(state):
        out_ref[:, h * HS : (h + 1) * HS] = (mixed / total).astype(BF)
        sum_ref[h] = total


def attend(heads, segment, low, high):
    tokens, columns = heads.shape
    width = columns // 3
    count = width // HS
    return call(
        attend_body,
        (tokens // QUERY_TILE,),
        [
            pl.BlockSpec((QUERY_TILE, width), lambda b, lo, hi: (b, 0)),
            pl.BlockSpec((tokens, width), lambda b, lo, hi: (0, 1)),
            pl.BlockSpec((tokens, width), lambda b, lo, hi: (0, 2)),
            pl.BlockSpec((QUERY_TILE, 1), lambda b, lo, hi: (b, 0)),
            pl.BlockSpec((1, tokens), lambda b, lo, hi: (0, 0)),
        ],
        [
            pl.BlockSpec((QUERY_TILE, width), lambda b, lo, hi: (b, 0)),
            pl.BlockSpec((count, QUERY_TILE, 1), lambda b, lo, hi: (0, b, 0)),
        ],
        [shape((tokens, width), BF), shape((count, tokens, 1), F32)],
        flops=4 * count * tokens * tokens * HS // 2,
        moved=8 * tokens * columns,
        prefetch=2,
        name="attend",
    )(low, high, heads, heads, heads, segment[:, None], segment[None, :])


def head_back(grad, raw, gain, cosine, sine):
    turned = grad * cosine - pltpu.roll(grad, HS // 2, 1) * sine
    factor = lax.rsqrt(jnp.mean(raw * raw, axis=1, keepdims=True) + EPSILON)
    unit = raw * factor
    gain_part = jnp.sum(turned * unit, axis=0, keepdims=True)
    pulled = turned * gain
    inner = jnp.mean(pulled * unit, axis=1, keepdims=True)
    return (pulled - unit * inner) * factor, gain_part


def attend_back_body(
    low, high, q_ref, k_ref, v_ref, g_ref, o_ref, s_ref, qs_ref, ks_ref, qr_ref, kr_ref,
    cos_ref, sin_ref, hg_ref, gq_ref, gk_ref, gv_ref, gain_ref, keys_ref, values_ref, inner_ref,
):
    block = pl.program_id(0)
    count = q_ref.shape[1] // HS

    @pl.when(block == 0)
    def _():
        keys_ref[...] = jnp.zeros_like(keys_ref)
        values_ref[...] = jnp.zeros_like(values_ref)
        gain_ref[...] = jnp.zeros_like(gain_ref)

    for h in range(count):
        inner_ref[h] = jnp.sum(
            head(g_ref, h).astype(F32) * head(o_ref, h).astype(F32), axis=1, keepdims=True
        )

    def step(index, state):
        rows = key_rows(index)
        allowed = qs_ref[...] == ks_ref[:, rows]
        scores = [dot(head(q_ref, h), head(k_ref, h, rows), 1, 1) for h in range(count)]
        grads = [dot(head(g_ref, h), head(v_ref, h, rows), 1, 1) for h in range(count)]
        new = []
        for h in range(count):
            columns = slice(h * HS, (h + 1) * HS)
            weights = jnp.where(
                allowed, jnp.exp2(scores[h] * EXP2_SCALE) * (1.0 / s_ref[h]), 0.0
            )
            grad_scores = (weights * (grads[h] - inner_ref[h])).astype(BF)
            values_ref[rows, columns] += dot(weights.astype(BF), head(g_ref, h), 0, 0)
            keys_ref[rows, columns] += dot(grad_scores, head(q_ref, h), 0, 0)
            new.append(state[h] + dot(grad_scores, head(k_ref, h, rows)))
        return tuple(new)

    grad_queries = lax.fori_loop(
        low[block], high[block], step, (jnp.zeros((QUERY_TILE, HS), F32),) * count
    )
    rows = pl.ds(pl.multiple_of(block * QUERY_TILE, QUERY_TILE), QUERY_TILE)
    for h, grad_query in enumerate(grad_queries):
        back, part = head_back(
            grad_query * SCALE, head(qr_ref, h), hg_ref[0:1, :], cos_ref[rows, :], sin_ref[rows, :]
        )
        gq_ref[:, h * HS : (h + 1) * HS] = back.astype(BF)
        gain_ref[0:1, :] += part

    @pl.when(block == pl.num_programs(0) - 1)
    def _():
        for h in range(count):
            back, part = head_back(
                head(keys_ref, h) * SCALE, head(kr_ref, h), hg_ref[1:2, :], cos_ref[...],
                sin_ref[...],
            )
            gk_ref[:, h * HS : (h + 1) * HS] = back.astype(BF)
            gain_ref[1:2, :] += part
        gv_ref[...] = values_ref[...].astype(BF)


def attend_back(heads, grad_mixed, mixed, sums, segment, low, high, raw, cosine, sine, gains):
    tokens, columns = heads.shape
    width = columns // 3
    count = width // HS
    whole = lambda b, lo, hi: (0, 0)
    tile = lambda b, lo, hi: (b, 0)
    return call(
        attend_back_body,
        (tokens // QUERY_TILE,),
        [
            pl.BlockSpec((QUERY_TILE, width), tile),
            pl.BlockSpec((tokens, width), lambda b, lo, hi: (0, 1)),
            pl.BlockSpec((tokens, width), lambda b, lo, hi: (0, 2)),
            pl.BlockSpec((QUERY_TILE, width), tile),
            pl.BlockSpec((QUERY_TILE, width), tile),
            pl.BlockSpec((count, QUERY_TILE, 1), lambda b, lo, hi: (0, b, 0)),
            pl.BlockSpec((QUERY_TILE, 1), tile),
            pl.BlockSpec((1, tokens), whole),
            pl.BlockSpec((QUERY_TILE, width), tile),
            pl.BlockSpec((tokens, width), lambda b, lo, hi: (0, 1)),
            pl.BlockSpec((tokens, HS), whole),
            pl.BlockSpec((tokens, HS), whole),
            pl.BlockSpec((2, HS), whole),
        ],
        [
            pl.BlockSpec((QUERY_TILE, width), tile),
            pl.BlockSpec((tokens, width), whole),
            pl.BlockSpec((tokens, width), whole),
            pl.BlockSpec((2, HS), whole),
        ],
        [shape((tokens, width), BF)] * 3 + [shape((2, HS), F32)],
        scratch=[
            pltpu.VMEM((tokens, width), F32),
            pltpu.VMEM((tokens, width), F32),
            pltpu.VMEM((count, QUERY_TILE, 1), F32),
        ],
        flops=10 * count * tokens * tokens * HS // 2,
        moved=24 * tokens * columns,
        prefetch=2,
        name="attend_back",
    )(
        low, high, heads, heads, heads, grad_mixed, mixed, sums, segment[:, None],
        segment[None, :], raw, raw, cosine, sine, gains,
    )


def dispatch_body(slot_ref, x_ref, out_ref):
    local, capacity = out_ref.shape[1], out_ref.shape[3]
    tokens = x_ref.shape[1]
    rows = x_ref[0]
    order = lax.broadcasted_iota(jnp.int32, (capacity, tokens), 0)
    for index in range(local):
        hot = jnp.where(order == slot_ref[0, 0, index : index + 1, :], 1.0, 0.0).astype(BF)
        out_ref[0, index, 0] = dot(hot, rows).astype(BF)


def dispatch(slots, rows, capacity):
    groups, targets, local, tokens = slots.shape
    features = rows.shape[2]
    return call(
        dispatch_body,
        (groups, targets),
        [
            pl.BlockSpec((1, 1, local, tokens), lambda g, d: (g, d, 0, 0)),
            pl.BlockSpec((1, tokens, features), lambda g, d: (g, 0, 0)),
        ],
        pl.BlockSpec((1, local, 1, capacity, features), lambda g, d: (d, 0, g, 0, 0)),
        shape((targets, local, groups, capacity, features), BF),
        flops=2 * groups * targets * local * capacity * tokens * features,
        moved=2 * groups * features * (tokens + targets * local * capacity),
        name="dispatch",
    )(slots, rows)


def combine_body(slot_ref, rows_ref, out_ref):
    targets, local, _, capacity, features = rows_ref.shape
    tile = out_ref.shape[1]
    order = lax.broadcasted_iota(jnp.int32, (tile, capacity), 1)
    slots = slot_ref[0]
    total = jnp.zeros((tile, features), F32)
    for target in range(targets):
        hot = jnp.concatenate(
            [
                jnp.where(
                    order == slots[:, target * local + i : target * local + i + 1], 1.0, 0.0
                ).astype(BF)
                for i in range(local)
            ],
            axis=1,
        )
        total = total + dot(hot, rows_ref[target].reshape(local * capacity, features))
    out_ref[0] = total.astype(BF)


def combine(slots_by_token, rows):
    groups, tokens, experts = slots_by_token.shape
    targets, local, _, capacity, features = rows.shape
    tile = 512
    return call(
        combine_body,
        (groups, tokens // tile),
        [
            pl.BlockSpec((1, tile, experts), lambda g, t: (g, t, 0)),
            pl.BlockSpec((targets, local, 1, capacity, features), lambda g, t: (0, 0, g, 0, 0)),
        ],
        pl.BlockSpec((1, tile, features), lambda g, t: (g, t, 0)),
        shape((groups, tokens, features), BF),
        flops=2 * groups * targets * local * capacity * tokens * features,
        moved=2 * groups * features * (tokens + targets * local * capacity),
        name="combine",
    )(slots_by_token, rows)


def block_rows(ref, row=0):
    _, cores, _, groups, capacity, features = ref.shape
    return ref[row].reshape(cores * groups * capacity, features)


def gate_up_body(*refs):
    x_refs, (gate_w, up_w, gate_ref, up_ref, act_ref) = refs[:CHUNKS], refs[CHUNKS:]
    width = x_refs[0].shape[-1]
    gate = up = None
    for row in range(x_refs[0].shape[0]):
        for chunk, x_ref in enumerate(x_refs):
            x = block_rows(x_ref, row)
            features = pl.ds((row * CHUNKS + chunk) * width, width)
            gate_part = dot(x, gate_w[0, features, :])
            up_part = dot(x, up_w[0, features, :])
            gate = gate_part if gate is None else gate + gate_part
            up = up_part if up is None else up + up_part
    gate_ref[0] = gate.astype(BF)
    up_ref[0] = up.astype(BF)
    act_ref[0] = (gate / (1.0 + jnp.exp(-gate)) * up).astype(BF)


def gate_up(chunks, gate_weight, up_weight):
    rows, cores, local, groups, capacity, width = chunks[0].shape
    _, features, hidden = gate_weight.shape
    slots = groups * capacity
    tile = min(512, hidden)
    out = shape((local, cores * slots, hidden), BF)
    out_spec = pl.BlockSpec((1, slots, tile), lambda i, n, k: (i, k, n))
    w_spec = pl.BlockSpec((1, features, tile), lambda i, n, k: (i, 0, n))
    return call(
        gate_up_body,
        (local, hidden // tile, cores),
        [
            pl.BlockSpec((rows, 1, 1, groups, capacity, width), lambda i, n, k: (0, k, i, 0, 0, 0))
        ]
        * CHUNKS
        + [w_spec, w_spec],
        [out_spec] * 3,
        [out] * 3,
        flops=4 * local * cores * slots * features * hidden,
        moved=local * (8 * features * hidden + 4 * cores * slots * features),
        name="gate_up",
    )(*chunks, gate_weight, up_weight)


def produce_body(*refs):
    act_ref, w_ref, prob_ref = refs[:3]
    c_refs, out_refs, inner_ref = refs[3 : 3 + CHUNKS], refs[3 + CHUNKS : -1], refs[-1]
    width = c_refs[0].shape[-1]

    @pl.when(pl.program_id(2) == 0)
    def _():
        inner_ref[...] = jnp.zeros_like(inner_ref)

    act, prob = act_ref[0], prob_ref[0]
    inner = jnp.zeros(prob.shape, F32)
    for chunk in range(CHUNKS):
        made = dot(act, w_ref[0, pl.ds(chunk * width, width), :], 1, 1)
        inner += jnp.sum(made * block_rows(c_refs[chunk]).astype(F32), axis=1, keepdims=True)
        out_refs[chunk][...] = (made * prob).astype(BF).reshape(out_refs[chunk].shape)
    inner_ref[0] += inner


def produce(activated, down_weight, prob, cots):
    rows, cores, local, groups, capacity, width = cots[0].shape
    hidden = activated.shape[2]
    slots = groups * capacity
    row_spec = pl.BlockSpec((1, 1, 1, groups, capacity, width), lambda i, k, r: (r, k, i, 0, 0, 0))
    column = pl.BlockSpec((1, slots, 1), lambda i, k, r: (i, k, 0))
    outs = call(
        produce_body,
        (local, cores, rows),
        [
            pl.BlockSpec((1, slots, hidden), lambda i, k, r: (i, k, 0)),
            pl.BlockSpec((1, width * CHUNKS, hidden), lambda i, k, r: (i, r, 0)),
            column,
        ]
        + [row_spec] * CHUNKS,
        [row_spec] * CHUNKS + [column],
        [shape(cots[0].shape, BF)] * CHUNKS + [shape((local, cores * slots, 1), F32)],
        flops=2 * local * cores * slots * D * hidden,
        moved=local * (2 * D * hidden + 8 * cores * slots * D),
        name="produce",
    )(activated, down_weight, prob, *cots)
    return outs[:CHUNKS], outs[CHUNKS]


def act_back_body(*refs):
    c_refs = refs[:CHUNKS]
    w_ref, prob_ref, gate_ref, up_ref, gate_out, up_out = refs[CHUNKS:]
    width = c_refs[0].shape[-1]
    prob = prob_ref[0]
    grad = None
    for row in range(c_refs[0].shape[0]):
        for chunk, c_ref in enumerate(c_refs):
            c = (block_rows(c_ref, row).astype(F32) * prob).astype(BF)
            part = dot(c, w_ref[0, pl.ds((row * CHUNKS + chunk) * width, width), :])
            grad = part if grad is None else grad + part
    gate, up = gate_ref[0].astype(F32), up_ref[0].astype(F32)
    squashed = 1.0 / (1.0 + jnp.exp(-gate))
    gate_out[0] = (grad * up * squashed * (1.0 + gate * (1.0 - squashed))).astype(BF)
    up_out[0] = (grad * gate * squashed).astype(BF)


def act_back(cots, down_weight, prob, gate, up):
    rows, cores, local, groups, capacity, width = cots[0].shape
    _, features, hidden = down_weight.shape
    slots = groups * capacity
    tile = min(512, hidden)
    spec = pl.BlockSpec((1, slots, tile), lambda i, n, k: (i, k, n))
    return call(
        act_back_body,
        (local, hidden // tile, cores),
        [
            pl.BlockSpec((rows, 1, 1, groups, capacity, width), lambda i, n, k: (0, k, i, 0, 0, 0))
        ]
        * CHUNKS
        + [
            pl.BlockSpec((1, features, tile), lambda i, n, k: (i, 0, n)),
            pl.BlockSpec((1, slots, 1), lambda i, n, k: (i, k, 0)),
            spec,
            spec,
        ],
        [spec] * 2,
        [shape(gate.shape, BF)] * 2,
        flops=2 * local * cores * slots * features * hidden,
        moved=local * (2 * features * hidden + 2 * cores * slots * features),
        name="act_back",
    )(*cots, down_weight, prob, gate, up)


def down_grad_body(*refs):
    c_refs, (prob_ref, act_ref, out_ref) = refs[:CHUNKS], refs[CHUNKS:]
    width = c_refs[0].shape[-1]
    for chunk, c_ref in enumerate(c_refs):
        c = (block_rows(c_ref).astype(F32) * prob_ref[0]).astype(BF)
        out_ref[0, pl.ds(chunk * width, width), :] = dot(c, act_ref[0], 0, 0)


def down_grad(cots, prob, activated):
    rows, cores, local, groups, capacity, width = cots[0].shape
    slots, hidden = activated.shape[1:]
    return call(
        down_grad_body,
        (local, rows),
        [
            pl.BlockSpec((1, cores, 1, groups, capacity, width), lambda i, r: (r, 0, i, 0, 0, 0))
        ]
        * CHUNKS
        + [
            pl.BlockSpec((1, slots, 1), lambda i, r: (i, 0, 0)),
            pl.BlockSpec((1, slots, hidden), lambda i, r: (i, 0, 0)),
        ],
        pl.BlockSpec((1, width * CHUNKS, hidden), lambda i, r: (i, r, 0)),
        shape((local, rows * width * CHUNKS, hidden), F32),
        flops=2 * local * slots * D * hidden,
        moved=local * (4 * D * hidden + 2 * slots * D),
        name="down_grad",
    )(*cots, prob, activated)


def gate_grad_body(*refs):
    x_refs, (gate_ref, up_ref, gate_out, up_out) = refs[:CHUNKS], refs[CHUNKS:]
    width = x_refs[0].shape[-1]
    for chunk, x_ref in enumerate(x_refs):
        x = block_rows(x_ref)
        features = pl.ds(chunk * width, width)
        gate_out[0, features, :] = dot(x, gate_ref[0], 0, 0)
        up_out[0, features, :] = dot(x, up_ref[0], 0, 0)


def gate_grad(chunks, grad_gate_pre, grad_up_pre):
    rows, cores, local, groups, capacity, width = chunks[0].shape
    slots, hidden = grad_gate_pre.shape[1:]
    wide = pl.BlockSpec((1, slots, hidden), lambda i, r: (i, 0, 0))
    out = pl.BlockSpec((1, width * CHUNKS, hidden), lambda i, r: (i, r, 0))
    return call(
        gate_grad_body,
        (local, rows),
        [
            pl.BlockSpec((1, cores, 1, groups, capacity, width), lambda i, r: (r, 0, i, 0, 0, 0))
        ]
        * CHUNKS
        + [wide, wide],
        [out, out],
        [shape((local, rows * width * CHUNKS, hidden), F32)] * 2,
        flops=4 * local * slots * D * hidden,
        moved=local * (8 * D * hidden + 2 * slots * D),
        name="gate_grad",
    )(*chunks, grad_gate_pre, grad_up_pre)


def rows_back_body(gate_ref, up_ref, gate_w, up_w, out_ref):
    made = dot(gate_ref[0], gate_w[0], 1, 1) + dot(up_ref[0], up_w[0], 1, 1)
    out_ref[...] = made.astype(BF).reshape(out_ref.shape)


def rows_back(grad_gate_pre, grad_up_pre, gate_weight, up_weight, chunk, dims):
    rows, cores, local, groups, capacity, width = dims
    hidden = gate_weight.shape[2]
    slots = groups * capacity
    pre = pl.BlockSpec((1, slots, hidden), lambda i, k, r: (i, k, 0))
    weight = pl.BlockSpec((1, width, hidden), lambda i, k, r: (i, r * CHUNKS + chunk, 0))
    return call(
        rows_back_body,
        (local, cores, rows),
        [pre, pre, weight, weight],
        pl.BlockSpec((1, 1, 1, groups, capacity, width), lambda i, k, r: (r, k, i, 0, 0, 0)),
        shape(dims, BF),
        flops=4 * local * cores * slots * width * rows * hidden,
        moved=local * (4 * rows * width * hidden + 6 * cores * slots * width * rows),
        name="rows_back",
    )(grad_gate_pre, grad_up_pre, gate_weight, up_weight)


def swap(rows):
    return lax.all_to_all(rows, SWAP_AXES, split_axis=0, concat_axis=0, tiled=True)


def slot_positions(routes, ranks, capacity):
    experts = jnp.arange(E, dtype=jnp.int32)
    member = jnp.any(routes.T[:, None, :] == experts[None, :, None], axis=0)
    earlier = (ranks[:, None] < ranks[None, :]).astype(BF)
    position = jnp.dot(member.astype(BF), earlier, preferred_element_type=F32)
    return jnp.where(member & (position < capacity), position, -1.0)


def per_device(
    hidden_in,
    attention_gain,
    query_weight,
    key_weight,
    value_weight,
    projection,
    query_gain,
    key_gain,
    feedforward_gain,
    router_weight,
    gate_weight,
    up_weight,
    down_weight,
    segments,
    routes,
    priority,
    cotangent,
):
    tokens, width_here = hidden_in.shape
    row_count = lax.axis_size("row")
    z_count = lax.axis_size("z")
    core_count = lax.axis_size("core")
    local = gate_weight.shape[0]
    piece_count = row_count * z_count * core_count * local
    pieces = max(1, piece_count // E)
    capacity = tokens * TOPK // E
    width = width_here // CHUNKS
    row_index = lax.axis_index("row")
    z_index = lax.axis_index("z")
    core_index = lax.axis_index("core")
    offset = row_index * width_here
    head_columns = query_weight.shape[1]
    head_count = head_columns // HS

    hidden_pieces, hidden_starts = row_gather(hidden_in)
    gain_full = lax.all_gather(attention_gain, "row", axis=0, tiled=True)
    qkv_full = lax.all_gather(
        jnp.concatenate([query_weight, key_weight, value_weight], axis=1),
        TOKENS_AXES,
        axis=0,
        tiled=True,
    )
    projection_full = lax.all_gather(projection, TOKENS_AXES, axis=0, tiled=True)
    router_full = lax.all_gather(
        lax.all_gather(router_weight.T, TOKENS_AXES, axis=1, tiled=True), "row", axis=0, tiled=True
    )
    router_here = lax.dynamic_slice_in_dim(router_full, offset, width_here, 1)

    position = slot_positions(routes, priority[0], capacity)
    by_group = lax.all_gather(position.astype(BF), "z", axis=0)
    by_piece = jnp.repeat(by_group, pieces, axis=1).reshape(
        z_count, row_count, z_count, core_count * local, tokens
    )
    mine = lax.dynamic_index_in_dim(by_piece, z_index, 2, keepdims=False).astype(jnp.int32)
    slots = mine.reshape(z_count, row_count * core_count, local, tokens)
    slots_by_token = jnp.swapaxes(
        mine.reshape(z_count, row_count * core_count * local, tokens), 1, 2
    )
    dims = (row_count, core_count, local, z_count, capacity, width)

    def send(values):
        received = []
        for chunk in range(CHUNKS):
            part = values[:, chunk * width : (chunk + 1) * width]
            spread = lax.all_gather(part, "z", axis=0)
            received.append(swap(dispatch(slots, spread, capacity)).reshape(dims))
        return received

    def gather_back(chunks):
        parts = []
        for chunk in chunks:
            summed = combine(
                slots_by_token, swap(chunk.reshape((row_count * core_count,) + dims[2:]))
            )
            parts.append(
                lax.psum_scatter(summed, "z", scatter_dimension=0, tiled=True).reshape(
                    tokens, width
                )
            )
        return jnp.concatenate(parts, axis=1).astype(F32)

    cots = send(cotangent)

    cosine, sine = rotary_tables()
    first_gain = attention_gain.astype(F32)
    second_gain = feedforward_gain.astype(F32)
    head_gains = jnp.stack([query_gain, key_gain]).astype(F32)
    residual = hidden_in.astype(F32)
    gain_row = gain_full.astype(F32)[None, :]
    normed_one, heads, raw, first_factor = project(
        hidden_starts,
        hidden_pieces,
        gain_row,
        qkv_full,
        cosine,
        sine,
        jnp.repeat(head_gains, head_count, axis=0).reshape(1, -1),
    )
    segment = segments[0]
    low, high = key_ranges(segment)
    mixed, sums = attend(heads, segment, low, high)
    middle = residual + row_scatter(mixed, row_scatter_order(projection_full))
    second_factor = lax.rsqrt(lax.psum(jnp.sum(middle * middle, axis=1), "row") / D + EPSILON)[
        :, None
    ]
    normed_two = (middle * second_factor * second_gain).astype(BF)

    logits = jnp.sum(lax.all_gather(dot(router_here, normed_two, 1, 1), "row", axis=0), axis=0)
    raised = jnp.exp(logits)
    router_probs = raised / jnp.sum(raised, axis=0, keepdims=True)

    rows = send(normed_two)
    experts_here = E // row_count
    own_slots = lax.dynamic_slice_in_dim(position, row_index * experts_here, experts_here, 0)
    own_probs = lax.dynamic_slice_in_dim(router_probs, row_index * experts_here, experts_here, 0)
    order = jnp.arange(capacity, dtype=jnp.int32).astype(F32)
    slot_prob = jnp.sum(
        jnp.where(own_slots[:, None, :] == order[None, :, None], own_probs[:, None, :], 0.0), axis=2
    )
    prob_groups = jnp.repeat(
        lax.all_gather(slot_prob, TOKENS_AXES, axis=0), pieces, axis=1
    ).reshape(z_count, core_count, z_count, core_count, local, capacity)
    prob_here = lax.dynamic_index_in_dim(
        lax.dynamic_index_in_dim(prob_groups, z_index, 2, keepdims=False),
        core_index,
        2,
        keepdims=False,
    )
    prob = jnp.transpose(prob_here, (2, 1, 0, 3)).reshape(
        local, core_count * z_count * capacity, 1
    )
    gate, up, activated = gate_up(rows, gate_weight, up_weight)
    grad_gate_pre, grad_up_pre = act_back(cots, down_weight, prob, gate, up)
    grad_rows = [
        rows_back(grad_gate_pre, grad_up_pre, gate_weight, up_weight, chunk, dims)
        for chunk in range(CHUNKS)
    ]
    grad_normed_two = gather_back(grad_rows)
    produced, inner = produce(activated, down_weight, prob, cots)
    grad_down = down_grad(cots, prob, activated)
    grad_gate, grad_up = gate_grad(rows, grad_gate_pre, grad_up_pre)
    output = (middle + gather_back(produced)).astype(BF)

    every = lax.all_gather(
        inner.reshape(local, core_count, z_count, capacity), ALL_AXES, axis=0
    )
    of_group = lax.dynamic_index_in_dim(
        lax.dynamic_index_in_dim(every, core_index, 2, keepdims=False), z_index, 2, keepdims=False
    )
    slot_grads = jnp.sum(of_group.reshape(E, pieces, capacity), axis=1)
    grad_prob = jnp.sum(
        jnp.where(position[:, None, :] == order[None, :, None], slot_grads[:, :, None], 0.0), axis=1
    )
    grad_logits = (
        router_probs * (grad_prob - jnp.sum(router_probs * grad_prob, axis=0, keepdims=True))
    ).astype(BF)
    grad_normed_two = grad_normed_two + dot(grad_logits, router_here, 0, 0)
    router_part = dot(grad_logits, normed_two)
    router_swapped = lax.all_to_all(
        router_part.reshape(row_count, experts_here, width_here), "row", 0, 0, tiled=True
    )
    grad_router = lax.psum_scatter(
        jnp.swapaxes(router_swapped, 0, 1).reshape(experts_here, D),
        TOKENS_AXES,
        scatter_dimension=1,
        tiled=True,
    ).T

    scaled_two = grad_normed_two * second_gain
    second_inner = lax.psum(jnp.sum(scaled_two * middle, axis=1), "row")[:, None]
    grad_middle = (
        cotangent.astype(F32)
        + scaled_two * second_factor
        - middle * second_factor**3 * second_inner / D
    )
    grad_feedforward_gain = jnp.sum(grad_normed_two * middle * second_factor, axis=0)

    branch_pieces, branch_starts = row_gather(grad_middle.astype(BF))
    grad_mixed = mix_back(branch_starts, branch_pieces, projection_full)
    grad_projection = projection_grad(branch_starts, branch_pieces, mixed)
    grad_query_raw, grad_key_raw, grad_value_raw, head_gain_grads = attend_back(
        heads, grad_mixed, mixed, sums, segment, low, high, raw, cosine, sine, head_gains
    )
    grad_raw = jnp.concatenate([grad_query_raw, grad_key_raw, grad_value_raw], axis=1)
    grad_first = row_scatter(grad_raw, row_scatter_order(qkv_full))
    first_inner = lax.psum(
        jnp.sum(grad_first * first_gain * residual, axis=1), "row"
    )[:, None]
    grad_qkv = dot(normed_one, grad_raw, 0, 0).astype(BF)
    scaled_one = grad_first * first_gain
    grad_input = (
        grad_middle + scaled_one * first_factor - residual * first_factor**3 * first_inner / D
    )
    grad_attention_gain = jnp.sum(grad_first * residual * first_factor, axis=0)

    padded_first = lax.dynamic_update_slice(jnp.zeros((D,), F32), grad_attention_gain, (offset,))
    padded_second = lax.dynamic_update_slice(jnp.zeros((D,), F32), grad_feedforward_gain, (offset,))
    totals = lax.psum((padded_first, padded_second, head_gain_grads), ALL_AXES)
    grad_projection = lax.psum_scatter(
        grad_projection, TOKENS_AXES, scatter_dimension=0, tiled=True
    ).astype(F32)
    grad_qkv = lax.psum_scatter(grad_qkv, TOKENS_AXES, scatter_dimension=0, tiled=True).astype(F32)
    return (
        output,
        grad_input,
        lax.dynamic_slice_in_dim(totals[0], offset, width_here),
        grad_qkv[:, :head_columns],
        grad_qkv[:, head_columns : 2 * head_columns],
        grad_qkv[:, 2 * head_columns :],
        grad_projection,
        totals[2][0],
        totals[2][1],
        lax.dynamic_slice_in_dim(totals[1], offset, width_here),
        grad_router,
        grad_gate,
        grad_up,
        grad_down,
    )


def solution(mesh):
    rows, columns = mesh.shape["row"], mesh.shape["col"]
    split_mesh = Mesh(
        mesh.devices.reshape(rows, columns // 2, 2), ("row", "z", "core")
    )
    both = P(TOKENS_AXES, "row")
    expert = P(ALL_AXES, None, None)
    grouped = P(TOKENS_AXES, None)
    return jax.shard_map(
        per_device,
        mesh=split_mesh,
        in_specs=(
            both, P("row"), both, both, both, both, P(), P(), P("row"), both,
            expert, expert, expert, grouped, grouped, grouped, both,
        ),
        out_specs=(
            both, both, P("row"), both, both, both, both, P(), P(), P("row"), both,
            expert, expert, expert,
        ),
        check_vma=False,
    )
```

```python
import functools

import jax
import jax.numpy as jnp
from jax import lax
from jax.experimental import pallas as pl
from jax.experimental.pallas import tpu as pltpu
from jax.sharding import Mesh, PartitionSpec as P

D = 2048
HS = 128
E = 64
TOPK = 8
SEQ = 2048
EPSILON = 1e-06
SCALE = HS ** (-0.5)
CHUNKS = 2
GAIN_ROWS = 16
TOKENS_AXES = ("z", "core")
SWAP_AXES = ("row", "core")
ALL_AXES = ("row", "z", "core")
BF = jnp.bfloat16
F32 = jnp.float32
VMEM_BYTES = 60 * 1024 * 1024


def call(body, grid, in_specs, out_specs, out_shape, scratch=(), prefetch=0, name=None, deps=(), flops=0):
    deps = tuple(deps)

    def without_deps(*refs):
        body(*refs[:prefetch], *refs[prefetch + len(deps) :])

    kernel = pl.pallas_call(
        without_deps,
        out_shape=out_shape,
        grid_spec=pltpu.PrefetchScalarGridSpec(
            num_scalar_prefetch=prefetch,
            grid=grid,
            in_specs=[pl.BlockSpec(memory_space=pl.ANY)] * len(deps) + list(in_specs),
            out_specs=out_specs,
            scratch_shapes=list(scratch),
        ),
        compiler_params=pltpu.CompilerParams(
            dimension_semantics=("arbitrary",) * len(grid), vmem_limit_bytes=VMEM_BYTES
        ),
        cost_estimate=pl.CostEstimate(flops=flops, bytes_accessed=0, transcendentals=0),
        name=name,
    )
    return lambda *args: kernel(*args[:prefetch], *deps, *args[prefetch:])


def shape(dims, dtype):
    return jax.ShapeDtypeStruct(dims, dtype)


def dot(left, right, left_dim=1, right_dim=0):
    return lax.dot_general(
        left, right, (((left_dim,), (right_dim,)), ((), ())), preferred_element_type=F32
    )


def rotary_tables():
    half_size = HS // 2
    inverse = 50000.0 ** (-(jnp.arange(half_size, dtype=F32) * 2.0) / HS)
    angles = jnp.arange(SEQ, dtype=F32)[:, None] * inverse[None, :]
    cosine, sine = jnp.cos(angles), jnp.sin(angles)
    return (
        jnp.concatenate([cosine, cosine], axis=1),
        jnp.concatenate([-sine, sine], axis=1),
    )


def project_body(starts, *refs):
    count = starts.shape[0]
    x_refs, gain_refs, refs = refs[:count], refs[count : 2 * count], refs[2 * count :]
    w_ref, cos_ref, sin_ref, hg_ref, normed_ref, heads_ref, raw_ref, factor_ref = refs
    width = x_refs[0].shape[1]
    square = sum(
        jnp.sum(jnp.square(x_ref[...].astype(F32)), axis=1, keepdims=True) for x_ref in x_refs
    )
    factor = lax.rsqrt(square / (width * count) + EPSILON)
    factor_ref[...] = factor
    raw = None
    for index, x_ref in enumerate(x_refs):
        features = pl.ds(pl.multiple_of(starts[index], width), width)
        gain = gain_refs[index][0:1, :].astype(F32)
        normed = (x_ref[...].astype(F32) * factor * gain).astype(BF)
        normed_ref[:, features] = normed
        part = dot(normed, w_ref[features, :])
        raw = part if raw is None else raw + part
    turned = raw_ref.shape[1]
    raw_ref[...] = raw[:, :turned]
    cosine, sine = cos_ref[...], sin_ref[...]
    for head in range(turned // HS):
        part = raw[:, head * HS : (head + 1) * HS]
        unit = part * lax.rsqrt(jnp.mean(part * part, axis=1, keepdims=True) + EPSILON)
        scaled = unit * hg_ref[:, head * HS : (head + 1) * HS]
        heads_ref[:, head * HS : (head + 1) * HS] = (
            scaled * cosine + pltpu.roll(scaled, HS // 2, 1) * sine
        ).astype(BF)
    heads_ref[:, turned:] = raw[:, turned:].astype(BF)


def project(starts, pieces, weights, cosine, sine, head_gains, deps=()):
    tokens, piece = cosine.shape[0], pieces[0].shape[1]
    width, columns = weights.shape
    turned = columns // 3 * 2
    tile = 256
    own = lambda t, s: (t, 0)
    whole = lambda t, s: (0, 0)
    return call(
        project_body,
        (tokens // tile,),
        [pl.BlockSpec((tile, piece), own)] * len(pieces)
        + [pl.BlockSpec((GAIN_ROWS, piece), lambda t, s: (tokens // GAIN_ROWS, 0))] * len(pieces)
        + [
            pl.BlockSpec((width, columns), whole),
            pl.BlockSpec((tile, HS), own),
            pl.BlockSpec((tile, HS), own),
            pl.BlockSpec((1, turned), whole),
        ],
        [
            pl.BlockSpec((tile, width), own),
            pl.BlockSpec((tile, columns), own),
            pl.BlockSpec((tile, turned), own),
            pl.BlockSpec((tile, 1), own),
        ],
        [
            shape((tokens, width), BF),
            shape((tokens, columns), BF),
            shape((tokens, turned), F32),
            shape((tokens, 1), F32),
        ],
        prefetch=1,
        name="project",
        deps=deps,
    )(starts, *pieces, *pieces, weights, cosine, sine, head_gains)


def mix_back_body(starts, *refs):
    count = starts.shape[0]
    g_refs, (w_ref, out_ref) = refs[:count], refs[count:]
    width = g_refs[0].shape[1]
    total = None
    for index, g_ref in enumerate(g_refs):
        part = dot(g_ref[...], w_ref[pl.ds(pl.multiple_of(starts[index], width), width), :])
        total = part if total is None else total + part
    out_ref[...] = total.astype(BF)


def mix_back(starts, pieces, weights, deps=()):
    tokens, piece = pieces[0].shape
    width, columns = weights.shape
    tile = 256
    return call(
        mix_back_body,
        (tokens // tile,),
        [pl.BlockSpec((tile, piece), lambda t, s: (t, 0))] * len(pieces)
        + [pl.BlockSpec((width, columns), lambda t, s: (0, 0))],
        pl.BlockSpec((tile, columns), lambda t, s: (t, 0)),
        shape((tokens, columns), BF),
        prefetch=1,
        name="mix_back",
        deps=deps,
    )(starts, *pieces, weights)


def projection_grad_body(starts, *refs):
    count = starts.shape[0]
    g_refs, (mixed_ref, out_ref, total_ref) = refs[:count], refs[count:]
    width = g_refs[0].shape[1]

    @pl.when(pl.program_id(0) == 0)
    def _():
        total_ref[...] = jnp.zeros_like(total_ref)

    for index, g_ref in enumerate(g_refs):
        rows = pl.ds(pl.multiple_of(starts[index], width), width)
        total_ref[rows, :] += dot(g_ref[...], mixed_ref[...], 0, 0)

    @pl.when(pl.program_id(0) == pl.num_programs(0) - 1)
    def _():
        out_ref[...] = total_ref[...].astype(BF)


def projection_grad(starts, pieces, mixed, deps=()):
    tokens, piece = pieces[0].shape
    columns = mixed.shape[1]
    width = piece * len(pieces)
    tile = 512
    return call(
        projection_grad_body,
        (tokens // tile,),
        [pl.BlockSpec((tile, piece), lambda t, s: (t, 0))] * len(pieces)
        + [pl.BlockSpec((tile, columns), lambda t, s: (t, 0))],
        pl.BlockSpec((width, columns), lambda t, s: (0, 0)),
        shape((width, columns), BF),
        scratch=[pltpu.VMEM((width, columns), F32)],
        prefetch=1,
        name="projection_grad",
        deps=deps,
    )(starts, *pieces, mixed)


def permute(values, mask):
    return lax.ppermute(values, "row", [(i, i ^ mask) for i in range(4)])


def row_gather(values):
    width = values.shape[1]
    if lax.axis_size("row") != 4:
        return [lax.all_gather(values, "row", axis=1, tiled=True)], jnp.zeros((1,), jnp.int32)
    half = width // 2
    left, right = values[:, :half], values[:, half:]
    left_1, right_2 = permute(left, 1), permute(right, 2)
    left_2, right_1 = permute(left, 2), permute(right, 1)
    left_3, right_3 = permute(left_1, 2), permute(right_2, 1)
    me = lax.axis_index("row")
    starts = jnp.stack(
        [(me ^ mask) * width + side * half for mask in range(4) for side in range(2)]
    ).astype(jnp.int32)
    return [left, right, left_1, right_1, left_2, right_2, left_3, right_3], starts


def small_row_gather(values):
    if lax.axis_size("row") != 4:
        return lax.all_gather(values, "row", axis=0)
    stacked = jnp.stack([values] + [permute(values, mask) for mask in (1, 2, 3)])
    return jnp.take(stacked, lax.axis_index("row") ^ jnp.arange(4), axis=0)


def small_row_swap(blocks):
    if lax.axis_size("row") != 4:
        return lax.all_to_all(blocks, "row", 0, 0, tiled=True)
    me = lax.axis_index("row")
    near = jnp.take(blocks, me ^ jnp.arange(4), axis=0)
    stacked = jnp.stack([near[0]] + [permute(near[mask], mask) for mask in (1, 2, 3)])
    return jnp.take(stacked, me ^ jnp.arange(4), axis=0)


def token_scatter(values):
    z_count, core_count = lax.axis_size("z"), lax.axis_size("core")
    rows, columns = values.shape
    blocks = values.reshape(z_count, core_count, rows // (z_count * core_count), columns)
    core = lax.axis_index("core")
    keep = lax.dynamic_index_in_dim(blocks, core, 1, keepdims=False)
    give = lax.dynamic_index_in_dim(blocks, 1 - core, 1, keepdims=False)
    got = lax.ppermute(give, "core", [(0, 1), (1, 0)])
    summed = (keep.astype(F32) + got.astype(F32)).astype(values.dtype)
    return lax.psum_scatter(summed.reshape(-1, columns), "z", scatter_dimension=0, tiled=True)


def after(value, *others):
    others = [other for other in others if other is not None]
    return pl.pallas_call(
        lambda *refs: None,
        out_shape=shape(value.shape, value.dtype),
        in_specs=[pl.BlockSpec(memory_space=pl.ANY)] * (1 + len(others)),
        out_specs=pl.BlockSpec(memory_space=pl.ANY),
        input_output_aliases={0: 0},
        cost_estimate=pl.CostEstimate(flops=0, bytes_accessed=0, transcendentals=0),
        name="after",
    )(value, *others)


def row_scatter_order(weights):
    if lax.axis_size("row") != 4:
        return weights
    width = weights.shape[0] // 4
    half = width // 2
    me = lax.axis_index("row")
    order = [(1, 0), (3, 0), (2, 1), (3, 1), (2, 0), (1, 1), (0, 0), (0, 1)]
    return jnp.concatenate(
        [
            lax.dynamic_slice_in_dim(weights, (me ^ mask) * width + side * half, half, 0)
            for mask, side in order
        ],
        axis=0,
    )


def row_scatter(left, ordered):
    if lax.axis_size("row") != 4:
        return lax.psum_scatter(
            dot(left, ordered, 1, 1).astype(BF), "row", scatter_dimension=1, tiled=True
        ).astype(F32), ()
    width = ordered.shape[0] // 4
    half = width // 2
    part = lambda index: dot(left, ordered[index * width : (index + 1) * width], 1, 1)
    sent = [part(0).astype(BF), part(1).astype(BF)]
    from_x = permute(sent[0], 1).astype(F32)
    from_y = permute(sent[1], 2).astype(F32)
    onward, own = part(2), part(3)
    last_left = permute((onward[:, :half] + from_x[:, half:]).astype(BF), 2).astype(F32)
    last_right = permute((onward[:, half:] + from_y[:, half:]).astype(BF), 1).astype(F32)
    total = jnp.concatenate(
        [
            own[:, :half] + from_x[:, :half] + last_left,
            own[:, half:] + from_y[:, :half] + last_right,
        ],
        axis=1,
    )
    return total, sent


QUERY_TILE = 256
KEY_TILE = 256
EXP2_SCALE = SCALE * 1.4426950408889634


def key_ranges(segment):
    first = segment[::QUERY_TILE]
    last = segment[QUERY_TILE - 1 :: QUERY_TILE]
    key_first = segment[::KEY_TILE]
    key_last = segment[KEY_TILE - 1 :: KEY_TILE]
    meets = (key_first[None, :] <= last[:, None]) & (key_last[None, :] >= first[:, None])
    order = jnp.arange(meets.shape[1], dtype=jnp.int32)[None, :]
    low = jnp.min(jnp.where(meets, order, meets.shape[1]), axis=1)
    high = jnp.max(jnp.where(meets, order + 1, 0), axis=1)
    return low.astype(jnp.int32), high.astype(jnp.int32)


def key_rows(step):
    return pl.ds(pl.multiple_of(step * KEY_TILE, KEY_TILE), KEY_TILE)


def head(ref, index, rows=slice(None)):
    return ref[rows, index * HS : (index + 1) * HS]


def attend_body(low, high, q_ref, k_ref, v_ref, qs_ref, ks_ref, out_ref, sum_ref):
    block = pl.program_id(0)
    count = q_ref.shape[1] // HS
    query_docs = qs_ref[...]

    def step(index, state):
        rows = key_rows(index)
        allowed = query_docs == ks_ref[:, rows]
        scores = [dot(head(q_ref, h), head(k_ref, h, rows), 1, 1) for h in range(count)]
        raised = [jnp.where(allowed, jnp.exp2(each * EXP2_SCALE), 0.0) for each in scores]
        return tuple(
            (
                total + jnp.sum(each, axis=1, keepdims=True),
                mixed + dot(each.astype(BF), head(v_ref, h, rows)),
            )
            for h, (each, (total, mixed)) in enumerate(zip(raised, state))
        )

    state = lax.fori_loop(
        low[block],
        high[block],
        step,
        ((jnp.zeros((QUERY_TILE, 1), F32), jnp.zeros((QUERY_TILE, HS), F32)),) * count,
    )
    for h, (total, mixed) in enumerate(state):
        out_ref[:, h * HS : (h + 1) * HS] = (mixed / total).astype(BF)
        sum_ref[h] = total


def attend(heads, segment, low, high):
    tokens, columns = heads.shape
    width = columns // 3
    count = width // HS
    return call(
        attend_body,
        (tokens // QUERY_TILE,),
        [
            pl.BlockSpec((QUERY_TILE, width), lambda b, lo, hi: (b, 0)),
            pl.BlockSpec((tokens, width), lambda b, lo, hi: (0, 1)),
            pl.BlockSpec((tokens, width), lambda b, lo, hi: (0, 2)),
            pl.BlockSpec((QUERY_TILE, 1), lambda b, lo, hi: (b, 0)),
            pl.BlockSpec((1, tokens), lambda b, lo, hi: (0, 0)),
        ],
        [
            pl.BlockSpec((QUERY_TILE, width), lambda b, lo, hi: (b, 0)),
            pl.BlockSpec((count, QUERY_TILE, 1), lambda b, lo, hi: (0, b, 0)),
        ],
        [shape((tokens, width), BF), shape((count, tokens, 1), F32)],
        prefetch=2,
        name="attend",
    )(low, high, heads, heads, heads, segment[:, None], segment[None, :])


def head_back(grad, raw, gain, cosine, sine):
    turned = grad * cosine - pltpu.roll(grad, HS // 2, 1) * sine
    factor = lax.rsqrt(jnp.mean(raw * raw, axis=1, keepdims=True) + EPSILON)
    unit = raw * factor
    gain_part = jnp.sum(turned * unit, axis=0, keepdims=True)
    pulled = turned * gain
    inner = jnp.mean(pulled * unit, axis=1, keepdims=True)
    return (pulled - unit * inner) * factor, gain_part


def attend_back_body(
    low, high, q_ref, k_ref, v_ref, g_ref, o_ref, s_ref, qs_ref, ks_ref, qr_ref, kr_ref,
    cos_ref, sin_ref, hg_ref, grad_ref, gain_ref, along_ref, keys_ref, values_ref,
    inner_ref,
):
    block = pl.program_id(0)
    count = q_ref.shape[1] // HS

    @pl.when(block == 0)
    def _():
        keys_ref[...] = jnp.zeros_like(keys_ref)
        values_ref[...] = jnp.zeros_like(values_ref)
        gain_ref[...] = jnp.zeros_like(gain_ref)

    for h in range(count):
        inner_ref[h] = jnp.sum(
            head(g_ref, h).astype(F32) * head(o_ref, h).astype(F32), axis=1, keepdims=True
        )

    def step(index, state):
        rows = key_rows(index)
        allowed = qs_ref[...] == ks_ref[:, rows]
        scores = [dot(head(q_ref, h), head(k_ref, h, rows), 1, 1) for h in range(count)]
        grads = [dot(head(g_ref, h), head(v_ref, h, rows), 1, 1) for h in range(count)]
        new = []
        for h in range(count):
            columns = slice(h * HS, (h + 1) * HS)
            weights = jnp.where(
                allowed, jnp.exp2(scores[h] * EXP2_SCALE) * (1.0 / s_ref[h]), 0.0
            )
            grad_scores = (weights * (grads[h] - inner_ref[h])).astype(BF)
            values_ref[rows, columns] += dot(weights.astype(BF), head(g_ref, h), 0, 0)
            keys_ref[rows, columns] += dot(grad_scores, head(q_ref, h), 0, 0)
            new.append(state[h] + dot(grad_scores, head(k_ref, h, rows)))
        return tuple(new)

    grad_queries = lax.fori_loop(
        low[block], high[block], step, (jnp.zeros((QUERY_TILE, HS), F32),) * count
    )
    rows = pl.ds(pl.multiple_of(block * QUERY_TILE, QUERY_TILE), QUERY_TILE)
    along = jnp.zeros((QUERY_TILE, 1), F32)
    for h, grad_query in enumerate(grad_queries):
        back, part = head_back(
            grad_query * SCALE, head(qr_ref, h), hg_ref[0:1, :], cos_ref[rows, :], sin_ref[rows, :]
        )
        grad_ref[rows, h * HS : (h + 1) * HS] = back.astype(BF)
        gain_ref[0:1, :] += part
        along += jnp.sum(back * head(qr_ref, h), axis=1, keepdims=True)
    along_ref[rows, :] = along

    @pl.when(block == pl.num_programs(0) - 1)
    def _():
        along_ref[...] += jnp.sum(values_ref[...] * v_ref[...].astype(F32), axis=1, keepdims=True)
        for h in range(count):
            back, part = head_back(
                head(keys_ref, h) * SCALE, head(kr_ref, h), hg_ref[1:2, :], cos_ref[...],
                sin_ref[...],
            )
            grad_ref[:, (count + h) * HS : (count + h + 1) * HS] = back.astype(BF)
            gain_ref[1:2, :] += part
            along_ref[...] += jnp.sum(back * head(kr_ref, h), axis=1, keepdims=True)
        grad_ref[:, 2 * count * HS :] = values_ref[...].astype(BF)


def attend_back(
    heads, grad_mixed, mixed, sums, segment, low, high, raw, cosine, sine, gains, deps=()
):
    tokens, columns = heads.shape
    width = columns // 3
    count = width // HS
    whole = lambda b, lo, hi: (0, 0)
    tile = lambda b, lo, hi: (b, 0)
    return call(
        attend_back_body,
        (tokens // QUERY_TILE,),
        [
            pl.BlockSpec((QUERY_TILE, width), tile),
            pl.BlockSpec((tokens, width), lambda b, lo, hi: (0, 1)),
            pl.BlockSpec((tokens, width), lambda b, lo, hi: (0, 2)),
            pl.BlockSpec((QUERY_TILE, width), tile),
            pl.BlockSpec((QUERY_TILE, width), tile),
            pl.BlockSpec((count, QUERY_TILE, 1), lambda b, lo, hi: (0, b, 0)),
            pl.BlockSpec((QUERY_TILE, 1), tile),
            pl.BlockSpec((1, tokens), whole),
            pl.BlockSpec((QUERY_TILE, width), tile),
            pl.BlockSpec((tokens, width), lambda b, lo, hi: (0, 1)),
            pl.BlockSpec((tokens, HS), whole),
            pl.BlockSpec((tokens, HS), whole),
            pl.BlockSpec((2, HS), whole),
        ],
        [
            pl.BlockSpec((tokens, columns), whole),
            pl.BlockSpec((2, HS), whole),
            pl.BlockSpec((tokens, 1), whole),
        ],
        [shape((tokens, columns), BF), shape((2, HS), F32), shape((tokens, 1), F32)],
        scratch=[
            pltpu.VMEM((tokens, width), F32),
            pltpu.VMEM((tokens, width), F32),
            pltpu.VMEM((count, QUERY_TILE, 1), F32),
        ],
        prefetch=2,
        name="attend_back",
        deps=deps,
    )(
        low, high, heads, heads, heads, grad_mixed, mixed, sums, segment[:, None],
        segment[None, :], raw, raw, cosine, sine, gains,
    )


def dispatch_body(slot_ref, x_ref, out_ref):
    local, capacity = out_ref.shape[1], out_ref.shape[3]
    tokens = x_ref.shape[1]
    rows = x_ref[0]
    order = lax.broadcasted_iota(jnp.int32, (capacity, tokens), 0)
    for index in range(local):
        hot = jnp.where(order == slot_ref[0, 0, index : index + 1, :], 1.0, 0.0).astype(BF)
        out_ref[0, index, 0] = dot(hot, rows).astype(BF)


def dispatch(slots, rows, capacity, deps=()):
    groups, targets, local, tokens = slots.shape
    features = rows.shape[2]
    return call(
        dispatch_body,
        (groups, targets),
        [
            pl.BlockSpec((1, 1, local, tokens), lambda g, d: (g, d, 0, 0)),
            pl.BlockSpec((1, tokens, features), lambda g, d: (g, 0, 0)),
        ],
        pl.BlockSpec((1, local, 1, capacity, features), lambda g, d: (d, 0, g, 0, 0)),
        shape((targets, local, groups, capacity, features), BF),
        name="dispatch",
        deps=deps,
    )(slots, rows)


def combine_body(*refs):
    slot_ref, rows_refs, out_ref = refs[0], refs[1:-1], refs[-1]
    targets, local, _, capacity, features = rows_refs[0].shape
    total_local = local * len(rows_refs)
    tile = out_ref.shape[1]
    order = lax.broadcasted_iota(jnp.int32, (tile, capacity), 1)
    slots = slot_ref[0]
    total = jnp.zeros((tile, features), F32)
    for target in range(targets):
        for part, rows_ref in enumerate(rows_refs):
            first = target * total_local + part * local
            hot = jnp.concatenate(
                [
                    jnp.where(order == slots[:, first + i : first + i + 1], 1.0, 0.0).astype(BF)
                    for i in range(local)
                ],
                axis=1,
            )
            total = total + dot(hot, rows_ref[target].reshape(local * capacity, features))
    out_ref[0] = total.astype(BF)


def combine(slots_by_token, parts, chunk, features, deps=()):
    groups, tokens, experts = slots_by_token.shape
    targets, local, _, capacity, _ = parts[0].shape
    tile = 512
    return call(
        combine_body,
        (groups, tokens // tile),
        [pl.BlockSpec((1, tile, experts), lambda g, t: (g, t, 0))]
        + [
            pl.BlockSpec(
                (targets, local, 1, capacity, features), lambda g, t: (0, 0, g, 0, chunk)
            )
        ]
        * len(parts),
        pl.BlockSpec((1, tile, features), lambda g, t: (g, t, 0)),
        shape((groups, tokens, features), BF),
        name="combine",
        flops=2 * groups * experts * capacity * tokens * features,
        deps=deps,
    )(slots_by_token, *parts)


def block_rows(ref, row=0):
    _, cores, _, groups, capacity, features = ref.shape
    return ref[row].reshape(cores * groups * capacity, features)


def expert_body(x_ref, c_ref, gate_w, up_w, down_w, prob_ref, act_ref, gate_out, up_out):
    rows, width = x_ref.shape[0], x_ref.shape[-1]
    prob = prob_ref[0]
    gate = up = grad = None
    for row in range(rows):
        features = pl.ds(row * width, width)
        x = block_rows(x_ref, row)
        c = (block_rows(c_ref, row).astype(F32) * prob).astype(BF)
        gate_part = dot(x, gate_w[0, features, :])
        up_part = dot(x, up_w[0, features, :])
        grad_part = dot(c, down_w[0, features, :])
        gate = gate_part if gate is None else gate + gate_part
        up = up_part if up is None else up + up_part
        grad = grad_part if grad is None else grad + grad_part
    squashed = 1.0 / (1.0 + jnp.exp(-gate))
    act_ref[...] = (gate * squashed * up).astype(BF)
    gate_out[...] = (grad * up * squashed * (1.0 + gate * (1.0 - squashed))).astype(BF)
    up_out[...] = (grad * gate * squashed).astype(BF)


def expert(index, rows, cots, gate_weight, up_weight, down_weight, prob):
    row_count, cores, _, groups, capacity, width = rows.shape
    _, features, hidden = gate_weight.shape
    slots = groups * capacity
    tile = min(512, hidden, 512 * 1024 // slots)
    block = (row_count, 1, 1, groups, capacity, width)
    row_spec = pl.BlockSpec(block, lambda n, k: (0, k, 0, 0, 0, 0))
    w_spec = pl.BlockSpec((1, features, tile), lambda n, k: (index, 0, n))
    out_spec = pl.BlockSpec((slots, tile), lambda n, k: (k, n))
    return call(
        expert_body,
        (hidden // tile, cores),
        [row_spec, row_spec, w_spec, w_spec, w_spec]
        + [pl.BlockSpec((1, slots, 1), lambda n, k: (index, k, 0))],
        [out_spec] * 3,
        [shape((cores * slots, hidden), BF)] * 3,
        name="expert",
    )(rows, cots, gate_weight, up_weight, down_weight, prob)


def produce_body(act_ref, w_ref, prob_ref, c_ref, *refs):
    out_refs, inner_ref = refs[-CHUNKS - 1 : -1], refs[-1]
    width = out_refs[0].shape[-1]

    @pl.when(pl.program_id(1) == 0)
    def _():
        inner_ref[...] = jnp.zeros_like(inner_ref)

    made = dot(act_ref[...], w_ref[0], 1, 1)
    inner_ref[...] += jnp.sum(made * block_rows(c_ref).astype(F32), axis=1, keepdims=True)
    weighted = (made * prob_ref[0]).astype(BF)
    for chunk, out_ref in enumerate(out_refs):
        out_ref[...] = weighted[:, chunk * width : (chunk + 1) * width].reshape(out_ref.shape)


def produce(index, activated, down_weight, prob, cots, dims, buffers):
    rows, cores, local, groups, capacity, width = dims
    hidden = activated.shape[1]
    slots = groups * capacity
    given = () if buffers is None else tuple(buffers)
    outs = pl.pallas_call(
        produce_body,
        out_shape=[shape(dims, BF)] * CHUNKS + [shape((cores * slots, 1), F32)],
        grid=(cores, rows),
        in_specs=[
            pl.BlockSpec((slots, hidden), lambda k, r: (k, 0)),
            pl.BlockSpec((1, width * CHUNKS, hidden), lambda k, r: (index, r, 0)),
            pl.BlockSpec((1, slots, 1), lambda k, r: (index, k, 0)),
            pl.BlockSpec(
                (1, 1, 1, groups, capacity, width * CHUNKS), lambda k, r: (r, k, 0, 0, 0, 0)
            ),
        ]
        + [pl.BlockSpec(memory_space=pl.ANY)] * len(given),
        out_specs=[
            pl.BlockSpec(
                (1, 1, 1, groups, capacity, width), lambda k, r: (r, k, index, 0, 0, 0)
            )
        ]
        * CHUNKS
        + [pl.BlockSpec((slots, 1), lambda k, r: (k, 0))],
        input_output_aliases={4 + chunk: chunk for chunk in range(len(given))},
        compiler_params=pltpu.CompilerParams(
            dimension_semantics=("arbitrary",) * 2, vmem_limit_bytes=VMEM_BYTES
        ),
        cost_estimate=pl.CostEstimate(
            flops=2 * cores * slots * D * hidden,
            bytes_accessed=2 * D * hidden + 8 * cores * slots * D,
            transcendentals=0,
        ),
        name="produce",
    )(activated, down_weight, prob, cots, *given)
    return outs[:CHUNKS], outs[CHUNKS]


def held_while(expert_index, last):
    return lambda i, r: jnp.where(i == expert_index, r, jnp.where(i < expert_index, 0, last))


def down_grad_body(*refs):
    prob_ref, refs = refs[0], refs[1:]
    local = len(refs) // 2
    c_refs, act_refs, out_ref = refs[:local], refs[local:-1], refs[-1]
    for index in range(local):

        @pl.when(pl.program_id(0) == index)
        def _():
            c = (block_rows(c_refs[index]).astype(F32) * prob_ref[0]).astype(BF)
            out_ref[0] = dot(c, act_refs[index][...], 0, 0)


def row_specs(local, shape_of):
    rows, cores, _, groups, capacity, width = shape_of

    def spec(index):
        where = held_while(index, rows - 1)
        return pl.BlockSpec(
            (1, cores, 1, groups, capacity, width), lambda i, r: (where(i, r), 0, 0, 0, 0, 0)
        )

    return [spec(index) for index in range(local)]


def down_grad(cots, prob, activated, deps=()):
    rows, cores, _, groups, capacity, width = cots[0].shape
    slots, hidden = activated[0].shape
    local = len(cots)
    return call(
        down_grad_body,
        (local, rows),
        [pl.BlockSpec((1, slots, 1), lambda i, r: (i, 0, 0))]
        + row_specs(local, cots[0].shape)
        + [pl.BlockSpec((slots, hidden), lambda i, r: (0, 0))] * local,
        pl.BlockSpec((1, width, hidden), lambda i, r: (i, r, 0)),
        shape((local, rows * width, hidden), F32),
        name="down_grad",
        flops=2 * local * slots * D * hidden,
        deps=deps,
    )(prob, *cots, *activated)


def gate_grad_body(*refs):
    local = (len(refs) - 2) // 3
    x_refs, gate_refs, up_refs = refs[:local], refs[local : 2 * local], refs[2 * local : -2]
    gate_out, up_out = refs[-2:]
    for index in range(local):

        @pl.when(pl.program_id(0) == index)
        def _():
            x = block_rows(x_refs[index])
            gate_out[0] = dot(x, gate_refs[index][...], 0, 0)
            up_out[0] = dot(x, up_refs[index][...], 0, 0)


def gate_grad(parts, grad_gate_pre, grad_up_pre, deps=()):
    rows, cores, _, groups, capacity, width = parts[0].shape
    slots, hidden = grad_gate_pre[0].shape
    local = len(parts)
    wide = pl.BlockSpec((slots, hidden), lambda i, r: (0, 0))
    out = pl.BlockSpec((1, width, hidden), lambda i, r: (i, r, 0))
    return call(
        gate_grad_body,
        (local, rows),
        row_specs(local, parts[0].shape) + [wide] * (2 * local),
        [out, out],
        [shape((local, rows * width, hidden), F32)] * 2,
        name="gate_grad",
        deps=deps,
    )(*parts, *grad_gate_pre, *grad_up_pre)


def rows_back_body(gate_ref, up_ref, gate_w, up_w, *refs):
    out_ref = refs[-1]
    made = dot(gate_ref[...], gate_w[0], 1, 1) + dot(up_ref[...], up_w[0], 1, 1)
    out_ref[...] = made.astype(BF).reshape(out_ref.shape)


def rows_back(
    index, grad_gate_pre, grad_up_pre, gate_weight, up_weight, chunk, dims, buffer, deps=()
):
    rows, cores, local, groups, capacity, width = dims
    hidden = gate_weight.shape[2]
    slots = groups * capacity
    pre = pl.BlockSpec((slots, hidden), lambda k, r: (k, 0))
    weight = pl.BlockSpec((1, width, hidden), lambda k, r: (index, r * CHUNKS + chunk, 0))
    given = () if buffer is None else (buffer,)
    return pl.pallas_call(
        rows_back_body,
        out_shape=shape(dims, BF),
        grid=(cores, rows),
        in_specs=[pre, pre, weight, weight]
        + [pl.BlockSpec(memory_space=pl.ANY)] * len(given + tuple(deps)),
        out_specs=pl.BlockSpec(
            (1, 1, 1, groups, capacity, width), lambda k, r: (r, k, index, 0, 0, 0)
        ),
        input_output_aliases={4: 0} if given else {},
        compiler_params=pltpu.CompilerParams(
            dimension_semantics=("arbitrary",) * 2, vmem_limit_bytes=VMEM_BYTES
        ),
        cost_estimate=pl.CostEstimate(
            flops=4 * cores * slots * width * rows * hidden,
            bytes_accessed=4 * rows * width * hidden + 6 * cores * slots * width * rows,
            transcendentals=0,
        ),
        name="rows_back",
    )(grad_gate_pre, grad_up_pre, gate_weight, up_weight, *given, *deps)


def swap(rows):
    return lax.all_to_all(rows, SWAP_AXES, split_axis=0, concat_axis=0, tiled=True)


def slot_positions(routes, ranks, capacity):
    experts = jnp.arange(E, dtype=jnp.int32)
    member = jnp.any(routes.T[:, None, :] == experts[None, :, None], axis=0)
    earlier = (ranks[:, None] < ranks[None, :]).astype(BF)
    position = jnp.dot(member.astype(BF), earlier, preferred_element_type=F32)
    return jnp.where(member & (position < capacity), position, -1.0)


def per_device(
    hidden_in,
    attention_gain,
    query_weight,
    key_weight,
    value_weight,
    projection,
    query_gain,
    key_gain,
    feedforward_gain,
    router_weight,
    gate_weight,
    up_weight,
    down_weight,
    segments,
    routes,
    priority,
    cotangent,
):
    tokens, width_here = hidden_in.shape
    row_count = lax.axis_size("row")
    z_count = lax.axis_size("z")
    core_count = lax.axis_size("core")
    local = gate_weight.shape[0]
    piece_count = row_count * z_count * core_count * local
    pieces = max(1, piece_count // E)
    capacity = tokens * TOPK // E
    width = width_here // CHUNKS
    row_index = lax.axis_index("row")
    z_index = lax.axis_index("z")
    core_index = lax.axis_index("core")
    head_columns = query_weight.shape[1]
    experts_here = E // row_count
    head_count = head_columns // HS

    hidden_pieces, hidden_starts = row_gather(
        jnp.concatenate(
            [hidden_in, jnp.broadcast_to(attention_gain[None, :], (GAIN_ROWS, width_here))], axis=0
        )
    )
    qkv_full = lax.all_gather(
        jnp.concatenate([query_weight, key_weight, value_weight], axis=1),
        TOKENS_AXES,
        axis=0,
        tiled=True,
    )
    with_router = lax.all_gather(
        jnp.concatenate([projection, router_weight], axis=1),
        TOKENS_AXES,
        axis=0,
        tiled=True,
    )
    projection_full = with_router[:, :head_columns]
    router_rows = with_router[:, head_columns:].reshape(row_count, width_here, -1)
    router_here = jnp.swapaxes(small_row_swap(router_rows), 1, 2).reshape(E, width_here)

    position = slot_positions(routes, priority[0], capacity)
    by_piece = jnp.repeat(position.astype(BF), pieces, axis=0).reshape(
        row_count, z_count, core_count * local, tokens
    )
    mine = lax.all_to_all(jnp.swapaxes(by_piece, 0, 1), "z", 0, 0, tiled=True).astype(jnp.int32)
    slots = mine.reshape(z_count, row_count * core_count, local, tokens)
    slots_by_token = jnp.swapaxes(
        mine.reshape(z_count, row_count * core_count * local, tokens), 1, 2
    )
    dims = (row_count, core_count, local, z_count, capacity, width)

    expert_dims = (row_count, core_count, 1, z_count, capacity, width_here)
    def scatter_back(summed):
        return lax.psum_scatter(summed, "z", scatter_dimension=0, tiled=True).reshape(
            tokens, width
        )

    spread_cots = lax.all_gather(after(cotangent, *hidden_pieces[2:6]), "z", axis=0)

    cosine, sine = rotary_tables()
    first_gain = attention_gain.astype(F32)
    second_gain = feedforward_gain.astype(F32)
    head_gains = jnp.stack([query_gain, key_gain]).astype(F32)
    residual = hidden_in.astype(F32)
    normed_one, heads, raw, first_factor = project(
        hidden_starts,
        hidden_pieces,
        qkv_full,
        cosine,
        sine,
        jnp.repeat(head_gains, head_count, axis=0).reshape(1, -1),
        (mine, router_here),
    )
    segment = segments[0]
    low, high = key_ranges(segment)
    mixed, sums = attend(heads, segment, low, high)
    middle = residual + row_scatter(mixed, row_scatter_order(projection_full))[0]
    second_factor = lax.rsqrt(lax.psum(jnp.sum(middle * middle, axis=1), "row") / D + EPSILON)[
        :, None
    ]
    normed_two = (middle * second_factor * second_gain).astype(BF)

    logits = jnp.sum(small_row_gather(dot(router_here, normed_two, 1, 1)), axis=0)
    raised = jnp.exp(logits)
    router_probs = raised / jnp.sum(raised, axis=0, keepdims=True)

    def send(spread, index, earlier, *before):
        picked = dispatch(slots[:, :, index : index + 1], spread, capacity, before)
        return swap(after(picked, *earlier) if earlier else picked).reshape(expert_dims)

    cots, rows = [], []
    for index in range(local):
        cots.append(send(spread_cots, index, cots[-1:] or [logits], normed_two))
    spread_rows = lax.all_gather(normed_two, "z", axis=0)
    for index in range(local):
        rows.append(send(spread_rows, index, [cots[-1]] + rows[-1:], cots[0]))
    own_slots = lax.dynamic_slice_in_dim(position, row_index * experts_here, experts_here, 0)
    own_probs = lax.dynamic_slice_in_dim(router_probs, row_index * experts_here, experts_here, 0)
    order = jnp.arange(capacity, dtype=jnp.int32).astype(F32)
    slot_prob = jnp.sum(
        jnp.where(own_slots[:, None, :] == order[None, :, None], own_probs[:, None, :], 0.0), axis=2
    )
    prob_groups = jnp.repeat(
        lax.all_gather(slot_prob, TOKENS_AXES, axis=0), pieces, axis=1
    ).reshape(z_count, core_count, z_count, core_count, local, capacity)
    prob_here = lax.dynamic_index_in_dim(
        lax.dynamic_index_in_dim(prob_groups, z_index, 2, keepdims=False),
        core_index,
        2,
        keepdims=False,
    )
    prob = jnp.transpose(prob_here, (2, 1, 0, 3)).reshape(
        local, core_count * z_count * capacity, 1
    )
    swapped_dims = (row_count * core_count,) + dims[2:]
    activated, grad_gate_pre, grad_up_pre = [], [], []
    buffers = [None] * CHUNKS
    for index in range(local):
        rows_here = rows[index]
        act, gate_pre, up_pre = expert(
            index, rows_here, cots[index], gate_weight, up_weight, down_weight, prob
        )
        activated.append(act)
        grad_gate_pre.append(gate_pre)
        grad_up_pre.append(up_pre)
        for chunk in range(CHUNKS):
            buffers[chunk] = rows_back(
                index, gate_pre, up_pre, gate_weight, up_weight, chunk, dims, buffers[chunk],
                buffers[:chunk] if index == local - 1 else (),
            )
    inners, made_buffers = [], None
    for index in range(local):
        made_buffers, inner = produce(
            index, activated[index], down_weight, prob, cots[index], dims, made_buffers
        )
        inners.append(inner)

    inner = jnp.stack(inners).reshape(local, core_count, z_count, capacity)
    to_groups = jnp.transpose(inner, (2, 1, 0, 3)).reshape(
        z_count * core_count, local * capacity
    )
    back_rows = [swap(buffers[0].reshape(swapped_dims))]
    of_group = lax.all_to_all(
        after(to_groups, back_rows[0]), TOKENS_AXES, 0, 0, tiled=True
    ).reshape(-1, capacity)
    slot_grads = jnp.sum(small_row_gather(of_group).reshape(E, pieces, capacity), axis=1)
    grad_down = down_grad(cots, prob, activated, inners)
    ready = after(buffers[1], grad_down)
    back_rows.append(swap(ready.reshape(swapped_dims)))
    grad_prob = jnp.sum(
        jnp.where(position[:, None, :] == order[None, :, None], slot_grads[:, :, None], 0.0), axis=1
    )
    grad_logits = (
        router_probs * (grad_prob - jnp.sum(router_probs * grad_prob, axis=0, keepdims=True))
    ).astype(BF)
    from_router = dot(grad_logits, router_here, 0, 0)
    first_sum = combine(slots_by_token, [back_rows[0]], 0, width, [ready])
    grad_gate, grad_up = gate_grad(rows, grad_gate_pre, grad_up_pre, [first_sum])
    first_sum = scatter_back(first_sum)
    second_sum = scatter_back(
        combine(slots_by_token, [back_rows[1]], 0, width, [grad_gate, first_sum])
    )
    grad_normed_two = from_router + jnp.concatenate(
        [first_sum, second_sum], axis=1
    ).astype(F32)
    router_part = dot(grad_logits, normed_two)
    router_swapped = lax.all_to_all(
        router_part.reshape(row_count, experts_here, width_here), "row", 0, 0, tiled=True
    )
    grad_router = lax.psum_scatter(
        jnp.swapaxes(router_swapped, 0, 1).reshape(experts_here, D),
        TOKENS_AXES,
        scatter_dimension=1,
        tiled=True,
    ).T

    scaled_two = grad_normed_two * second_gain
    second_inner = lax.psum(jnp.sum(scaled_two * middle, axis=1), "row")[:, None]
    grad_middle = (
        cotangent.astype(F32)
        + scaled_two * second_factor
        - middle * second_factor**3 * second_inner / D
    )
    grad_feedforward_gain = jnp.sum(grad_normed_two * middle * second_factor, axis=0)

    grad_branch = grad_middle.astype(BF)
    made_rows = [swap(after(made_buffers[0], back_rows[1], slot_grads).reshape(swapped_dims))]
    branch_pieces, branch_starts = row_gather(after(grad_branch, made_rows[0]))
    made_rows.append(swap(after(made_buffers[1], *branch_pieces).reshape(swapped_dims)))
    made_sums = [combine(slots_by_token, [made_rows[0]], 0, width, [grad_branch])]
    grad_mixed = mix_back(
        branch_starts, branch_pieces, projection_full, made_sums + [router_swapped]
    )
    grad_projection = projection_grad(branch_starts, branch_pieces, mixed, [grad_mixed])
    grad_raw, head_gain_grads, along = attend_back(
        heads, grad_mixed, mixed, sums, segment, low, high, raw, cosine, sine, head_gains,
        [grad_projection],
    )
    from_experts = [scatter_back(made_sums[0])]
    grad_raw = after(grad_raw, made_rows[1], from_experts[0])
    grad_first, sent = row_scatter(grad_raw, row_scatter_order(qkv_full))
    from_experts.append(
        scatter_back(combine(slots_by_token, [made_rows[1]], 0, width, sent))
    )
    small = jnp.concatenate([along.reshape(-1, HS), head_gain_grads], axis=0)
    small = jnp.sum(small_row_gather(small), axis=0)
    first_inner = small[:-2].reshape(-1, 1) / first_factor
    head_gain_grads = small[-2:]
    grad_qkv = dot(after(normed_one, *sent), grad_raw, 0, 0).astype(BF)
    scaled_one = grad_first * first_gain
    grad_input = (
        grad_middle + scaled_one * first_factor - residual * first_factor**3 * first_inner / D
    )
    grad_attention_gain = jnp.sum(grad_first * residual * first_factor, axis=0)

    grad_attention_gain, grad_feedforward_gain, head_gain_grads = lax.psum(
        (grad_attention_gain, grad_feedforward_gain, head_gain_grads), TOKENS_AXES
    )
    grad_projection = token_scatter(grad_projection).astype(F32)
    grad_qkv = token_scatter(grad_qkv).astype(F32)
    from_experts = jnp.concatenate(from_experts, axis=1).astype(F32)
    output = (after(middle, grad_first) + from_experts).astype(BF)
    return (
        output,
        grad_input,
        grad_attention_gain,
        grad_qkv[:, :head_columns],
        grad_qkv[:, head_columns : 2 * head_columns],
        grad_qkv[:, 2 * head_columns :],
        grad_projection,
        head_gain_grads[0],
        head_gain_grads[1],
        grad_feedforward_gain,
        grad_router,
        grad_gate,
        grad_up,
        grad_down,
    )


def solution(mesh):
    rows, columns = mesh.shape["row"], mesh.shape["col"]
    split_mesh = Mesh(
        mesh.devices.reshape(rows, columns // 2, 2), ("row", "z", "core")
    )
    both = P(TOKENS_AXES, "row")
    expert = P(ALL_AXES, None, None)
    grouped = P(TOKENS_AXES, None)
    return jax.shard_map(
        per_device,
        mesh=split_mesh,
        in_specs=(
            both, P("row"), both, both, both, both, P(), P(), P("row"), both,
            expert, expert, expert, grouped, grouped, grouped, both,
        ),
        out_specs=(
            both, both, P("row"), both, both, both, both, P(), P(), P("row"), both,
            expert, expert, expert,
        ),
        check_vma=False,
    )
```

```python
import functools

import jax
import jax.numpy as jnp
from jax import lax
from jax.experimental import pallas as pl
from jax.experimental.pallas import tpu as pltpu
from jax.sharding import Mesh, PartitionSpec as P

D = 2048
HS = 128
E = 64
TOPK = 8
SEQ = 2048
EPSILON = 1e-06
SCALE = HS ** (-0.5)
CHUNKS = 2
GAIN_ROWS = 16
TOKENS_AXES = ("z", "core")
SWAP_AXES = ("row", "core")
ALL_AXES = ("row", "z", "core")
BF = jnp.bfloat16
F32 = jnp.float32
VMEM_BYTES = 60 * 1024 * 1024


def call(body, grid, in_specs, out_specs, out_shape, scratch=(), prefetch=0, name=None, deps=(), flops=0):
    deps = tuple(deps)

    def without_deps(*refs):
        body(*refs[:prefetch], *refs[prefetch + len(deps) :])

    kernel = pl.pallas_call(
        without_deps,
        out_shape=out_shape,
        grid_spec=pltpu.PrefetchScalarGridSpec(
            num_scalar_prefetch=prefetch,
            grid=grid,
            in_specs=[pl.BlockSpec(memory_space=pl.ANY)] * len(deps) + list(in_specs),
            out_specs=out_specs,
            scratch_shapes=list(scratch),
        ),
        compiler_params=pltpu.CompilerParams(
            dimension_semantics=("arbitrary",) * len(grid), vmem_limit_bytes=VMEM_BYTES
        ),
        cost_estimate=pl.CostEstimate(flops=flops, bytes_accessed=0, transcendentals=0),
        name=name,
    )
    return lambda *args: kernel(*args[:prefetch], *deps, *args[prefetch:])


def shape(dims, dtype):
    return jax.ShapeDtypeStruct(dims, dtype)


def dot(left, right, left_dim=1, right_dim=0):
    return lax.dot_general(
        left, right, (((left_dim,), (right_dim,)), ((), ())), preferred_element_type=F32
    )


def rotary_tables():
    half_size = HS // 2
    inverse = 50000.0 ** (-(jnp.arange(half_size, dtype=F32) * 2.0) / HS)
    angles = jnp.arange(SEQ, dtype=F32)[:, None] * inverse[None, :]
    cosine, sine = jnp.cos(angles), jnp.sin(angles)
    return (
        jnp.concatenate([cosine, cosine], axis=1),
        jnp.concatenate([-sine, sine], axis=1),
    )


def project_body(starts, *refs):
    count = starts.shape[0]
    x_refs, gain_refs, refs = refs[:count], refs[count : 2 * count], refs[2 * count :]
    w_ref, cos_ref, sin_ref, hg_ref, normed_ref, heads_ref, raw_ref, factor_ref = refs
    width = x_refs[0].shape[1]
    square = sum(
        jnp.sum(jnp.square(x_ref[...].astype(F32)), axis=1, keepdims=True) for x_ref in x_refs
    )
    factor = lax.rsqrt(square / (width * count) + EPSILON)
    factor_ref[...] = factor
    raw = None
    for index, x_ref in enumerate(x_refs):
        features = pl.ds(pl.multiple_of(starts[index], width), width)
        gain = gain_refs[index][0:1, :].astype(F32)
        normed = (x_ref[...].astype(F32) * factor * gain).astype(BF)
        normed_ref[:, features] = normed
        part = dot(normed, w_ref[features, :])
        raw = part if raw is None else raw + part
    turned = raw_ref.shape[1]
    raw_ref[...] = raw[:, :turned]
    cosine, sine = cos_ref[...], sin_ref[...]
    for head in range(turned // HS):
        part = raw[:, head * HS : (head + 1) * HS]
        unit = part * lax.rsqrt(jnp.mean(part * part, axis=1, keepdims=True) + EPSILON)
        scaled = unit * hg_ref[:, head * HS : (head + 1) * HS]
        heads_ref[:, head * HS : (head + 1) * HS] = (
            scaled * cosine + pltpu.roll(scaled, HS // 2, 1) * sine
        ).astype(BF)
    heads_ref[:, turned:] = raw[:, turned:].astype(BF)


def project(starts, pieces, weights, cosine, sine, head_gains, deps=()):
    tokens, piece = cosine.shape[0], pieces[0].shape[1]
    width, columns = weights.shape
    turned = columns // 3 * 2
    tile = 256
    own = lambda t, s: (t, 0)
    whole = lambda t, s: (0, 0)
    return call(
        project_body,
        (tokens // tile,),
        [pl.BlockSpec((tile, piece), own)] * len(pieces)
        + [pl.BlockSpec((GAIN_ROWS, piece), lambda t, s: (tokens // GAIN_ROWS, 0))] * len(pieces)
        + [
            pl.BlockSpec((width, columns), whole),
            pl.BlockSpec((tile, HS), own),
            pl.BlockSpec((tile, HS), own),
            pl.BlockSpec((1, turned), whole),
        ],
        [
            pl.BlockSpec((tile, width), own),
            pl.BlockSpec((tile, columns), own),
            pl.BlockSpec((tile, turned), own),
            pl.BlockSpec((tile, 1), own),
        ],
        [
            shape((tokens, width), BF),
            shape((tokens, columns), BF),
            shape((tokens, turned), F32),
            shape((tokens, 1), F32),
        ],
        prefetch=1,
        name="project",
        deps=deps,
    )(starts, *pieces, *pieces, weights, cosine, sine, head_gains)


def mix_back_body(starts, *refs):
    count = starts.shape[0]
    g_refs, (w_ref, out_ref) = refs[:count], refs[count:]
    width = g_refs[0].shape[1]
    total = None
    for index, g_ref in enumerate(g_refs):
        part = dot(g_ref[...], w_ref[pl.ds(pl.multiple_of(starts[index], width), width), :])
        total = part if total is None else total + part
    out_ref[...] = total.astype(BF)


def mix_back(starts, pieces, weights, deps=()):
    tokens, piece = pieces[0].shape
    width, columns = weights.shape
    tile = 256
    return call(
        mix_back_body,
        (tokens // tile,),
        [pl.BlockSpec((tile, piece), lambda t, s: (t, 0))] * len(pieces)
        + [pl.BlockSpec((width, columns), lambda t, s: (0, 0))],
        pl.BlockSpec((tile, columns), lambda t, s: (t, 0)),
        shape((tokens, columns), BF),
        prefetch=1,
        name="mix_back",
        deps=deps,
    )(starts, *pieces, weights)


def projection_grad_body(starts, *refs):
    count = starts.shape[0]
    g_refs, (mixed_ref, out_ref, total_ref) = refs[:count], refs[count:]
    width = g_refs[0].shape[1]

    @pl.when(pl.program_id(0) == 0)
    def _():
        total_ref[...] = jnp.zeros_like(total_ref)

    for index, g_ref in enumerate(g_refs):
        rows = pl.ds(pl.multiple_of(starts[index], width), width)
        total_ref[rows, :] += dot(g_ref[...], mixed_ref[...], 0, 0)

    @pl.when(pl.program_id(0) == pl.num_programs(0) - 1)
    def _():
        out_ref[...] = total_ref[...].astype(BF)


def projection_grad(starts, pieces, mixed, deps=()):
    tokens, piece = pieces[0].shape
    columns = mixed.shape[1]
    width = piece * len(pieces)
    tile = 512
    return call(
        projection_grad_body,
        (tokens // tile,),
        [pl.BlockSpec((tile, piece), lambda t, s: (t, 0))] * len(pieces)
        + [pl.BlockSpec((tile, columns), lambda t, s: (t, 0))],
        pl.BlockSpec((width, columns), lambda t, s: (0, 0)),
        shape((width, columns), BF),
        scratch=[pltpu.VMEM((width, columns), F32)],
        prefetch=1,
        name="projection_grad",
        deps=deps,
    )(starts, *pieces, mixed)


def permute(values, mask):
    return lax.ppermute(values, "row", [(i, i ^ mask) for i in range(4)])


def row_gather(values):
    width = values.shape[1]
    if lax.axis_size("row") != 4:
        return [lax.all_gather(values, "row", axis=1, tiled=True)], jnp.zeros((1,), jnp.int32)
    half = width // 2
    left, right = values[:, :half], values[:, half:]
    left_1, right_2 = permute(left, 1), permute(right, 2)
    left_2, right_1 = permute(left, 2), permute(right, 1)
    left_3, right_3 = permute(left_1, 2), permute(right_2, 1)
    me = lax.axis_index("row")
    starts = jnp.stack(
        [(me ^ mask) * width + side * half for mask in range(4) for side in range(2)]
    ).astype(jnp.int32)
    return [left, right, left_1, right_1, left_2, right_2, left_3, right_3], starts


def small_row_gather(values):
    if lax.axis_size("row") != 4:
        return lax.all_gather(values, "row", axis=0)
    stacked = jnp.stack([values] + [permute(values, mask) for mask in (1, 2, 3)])
    return jnp.take(stacked, lax.axis_index("row") ^ jnp.arange(4), axis=0)


def small_row_swap(blocks):
    if lax.axis_size("row") != 4:
        return lax.all_to_all(blocks, "row", 0, 0, tiled=True)
    me = lax.axis_index("row")
    near = jnp.take(blocks, me ^ jnp.arange(4), axis=0)
    stacked = jnp.stack([near[0]] + [permute(near[mask], mask) for mask in (1, 2, 3)])
    return jnp.take(stacked, me ^ jnp.arange(4), axis=0)


def core_sum(values):
    z_count, core_count = lax.axis_size("z"), lax.axis_size("core")
    rows, columns = values.shape
    blocks = values.reshape(z_count, core_count, rows // (z_count * core_count), columns)
    core = lax.axis_index("core")
    keep = lax.dynamic_index_in_dim(blocks, core, 1, keepdims=False)
    give = lax.dynamic_index_in_dim(blocks, 1 - core, 1, keepdims=False)
    got = lax.ppermute(give, "core", [(0, 1), (1, 0)])
    return (keep.astype(F32) + got.astype(F32)).astype(values.dtype).reshape(-1, columns)


def z_scatter(values):
    return lax.psum_scatter(values, "z", scatter_dimension=0, tiled=True)


def row_sum(values):
    if lax.axis_size("row") != 4:
        return jnp.sum(lax.all_gather(values, "row", axis=0), axis=0)
    half = values.shape[1] // 2
    left, right = values[:, :half], values[:, half:]
    left, right = left + permute(left, 1), right + permute(right, 2)
    return jnp.concatenate([left + permute(left, 2), right + permute(right, 1)], axis=1)


def after(value, *others):
    others = [other for other in others if other is not None]
    return pl.pallas_call(
        lambda *refs: None,
        out_shape=shape(value.shape, value.dtype),
        in_specs=[pl.BlockSpec(memory_space=pl.ANY)] * (1 + len(others)),
        out_specs=pl.BlockSpec(memory_space=pl.ANY),
        input_output_aliases={0: 0},
        cost_estimate=pl.CostEstimate(flops=0, bytes_accessed=0, transcendentals=0),
        name="after",
    )(value, *others)


def row_scatter_order(weights):
    if lax.axis_size("row") != 4:
        return weights
    width = weights.shape[0] // 4
    half = width // 2
    me = lax.axis_index("row")
    order = [(1, 0), (3, 0), (2, 1), (3, 1), (2, 0), (1, 1), (0, 0), (0, 1)]
    return jnp.concatenate(
        [
            lax.dynamic_slice_in_dim(weights, (me ^ mask) * width + side * half, half, 0)
            for mask, side in order
        ],
        axis=0,
    )


def row_scatter(left, ordered, *meanwhile):
    if lax.axis_size("row") != 4:
        return lax.psum_scatter(
            dot(left, ordered, 1, 1).astype(BF), "row", scatter_dimension=1, tiled=True
        ).astype(F32), (), ()
    width = ordered.shape[0] // 4
    half = width // 2
    part = lambda index: dot(left, ordered[index * width : (index + 1) * width], 1, 1)
    sent = [part(0).astype(BF), part(1).astype(BF)]
    received = [permute(sent[0], 1), permute(sent[1], 2)]
    from_x, from_y = received[0].astype(F32), received[1].astype(F32)
    onward, own = part(2), part(3)
    onward_left = (onward[:, :half] + from_x[:, half:]).astype(BF)
    onward_right = (onward[:, half:] + from_y[:, half:]).astype(BF)
    if meanwhile:
        onward_left = after(onward_left, *meanwhile)
        onward_right = after(onward_right, *meanwhile)
    last_left = permute(onward_left, 2).astype(F32)
    last_right = permute(onward_right, 1).astype(F32)
    total = jnp.concatenate(
        [
            own[:, :half] + from_x[:, :half] + last_left,
            own[:, half:] + from_y[:, :half] + last_right,
        ],
        axis=1,
    )
    return total, sent, received


QUERY_TILE = 256
KEY_TILE = 256
EXP2_SCALE = SCALE * 1.4426950408889634


def key_ranges(segment):
    first = segment[::QUERY_TILE]
    last = segment[QUERY_TILE - 1 :: QUERY_TILE]
    key_first = segment[::KEY_TILE]
    key_last = segment[KEY_TILE - 1 :: KEY_TILE]
    meets = (key_first[None, :] <= last[:, None]) & (key_last[None, :] >= first[:, None])
    order = jnp.arange(meets.shape[1], dtype=jnp.int32)[None, :]
    low = jnp.min(jnp.where(meets, order, meets.shape[1]), axis=1)
    high = jnp.max(jnp.where(meets, order + 1, 0), axis=1)
    return low.astype(jnp.int32), high.astype(jnp.int32)


def key_rows(step):
    return pl.ds(pl.multiple_of(step * KEY_TILE, KEY_TILE), KEY_TILE)


def head(ref, index, rows=slice(None)):
    return ref[rows, index * HS : (index + 1) * HS]


def attend_body(low, high, q_ref, k_ref, v_ref, qs_ref, ks_ref, out_ref, sum_ref):
    block = pl.program_id(0)
    count = q_ref.shape[1] // HS
    query_docs = qs_ref[...]

    def step(index, state):
        rows = key_rows(index)
        allowed = query_docs == ks_ref[:, rows]
        scores = [dot(head(q_ref, h), head(k_ref, h, rows), 1, 1) for h in range(count)]
        raised = [jnp.where(allowed, jnp.exp2(each * EXP2_SCALE), 0.0) for each in scores]
        return tuple(
            (
                total + jnp.sum(each, axis=1, keepdims=True),
                mixed + dot(each.astype(BF), head(v_ref, h, rows)),
            )
            for h, (each, (total, mixed)) in enumerate(zip(raised, state))
        )

    state = lax.fori_loop(
        low[block],
        high[block],
        step,
        ((jnp.zeros((QUERY_TILE, 1), F32), jnp.zeros((QUERY_TILE, HS), F32)),) * count,
    )
    for h, (total, mixed) in enumerate(state):
        out_ref[:, h * HS : (h + 1) * HS] = (mixed / total).astype(BF)
        sum_ref[h] = total


def attend(heads, segment, low, high):
    tokens, columns = heads.shape
    width = columns // 3
    count = width // HS
    return call(
        attend_body,
        (tokens // QUERY_TILE,),
        [
            pl.BlockSpec((QUERY_TILE, width), lambda b, lo, hi: (b, 0)),
            pl.BlockSpec((tokens, width), lambda b, lo, hi: (0, 1)),
            pl.BlockSpec((tokens, width), lambda b, lo, hi: (0, 2)),
            pl.BlockSpec((QUERY_TILE, 1), lambda b, lo, hi: (b, 0)),
            pl.BlockSpec((1, tokens), lambda b, lo, hi: (0, 0)),
        ],
        [
            pl.BlockSpec((QUERY_TILE, width), lambda b, lo, hi: (b, 0)),
            pl.BlockSpec((count, QUERY_TILE, 1), lambda b, lo, hi: (0, b, 0)),
        ],
        [shape((tokens, width), BF), shape((count, tokens, 1), F32)],
        prefetch=2,
        name="attend",
    )(low, high, heads, heads, heads, segment[:, None], segment[None, :])


def head_back(grad, raw, gain, cosine, sine):
    turned = grad * cosine - pltpu.roll(grad, HS // 2, 1) * sine
    factor = lax.rsqrt(jnp.mean(raw * raw, axis=1, keepdims=True) + EPSILON)
    unit = raw * factor
    gain_part = jnp.sum(turned * unit, axis=0, keepdims=True)
    pulled = turned * gain
    inner = jnp.mean(pulled * unit, axis=1, keepdims=True)
    return (pulled - unit * inner) * factor, gain_part


def attend_back_body(
    low, high, q_ref, k_ref, v_ref, g_ref, o_ref, s_ref, qs_ref, ks_ref, qr_ref, kr_ref,
    cos_ref, sin_ref, hg_ref, grad_ref, gain_ref, along_ref, keys_ref, values_ref,
    inner_ref,
):
    block = pl.program_id(0)
    count = q_ref.shape[1] // HS

    @pl.when(block == 0)
    def _():
        keys_ref[...] = jnp.zeros_like(keys_ref)
        values_ref[...] = jnp.zeros_like(values_ref)
        gain_ref[...] = jnp.zeros_like(gain_ref)

    for h in range(count):
        inner_ref[h] = jnp.sum(
            head(g_ref, h).astype(F32) * head(o_ref, h).astype(F32), axis=1, keepdims=True
        )

    def step(index, state):
        rows = key_rows(index)
        allowed = qs_ref[...] == ks_ref[:, rows]
        scores = [dot(head(q_ref, h), head(k_ref, h, rows), 1, 1) for h in range(count)]
        grads = [dot(head(g_ref, h), head(v_ref, h, rows), 1, 1) for h in range(count)]
        new = []
        for h in range(count):
            columns = slice(h * HS, (h + 1) * HS)
            weights = jnp.where(
                allowed, jnp.exp2(scores[h] * EXP2_SCALE) * (1.0 / s_ref[h]), 0.0
            )
            grad_scores = (weights * (grads[h] - inner_ref[h])).astype(BF)
            values_ref[rows, columns] += dot(weights.astype(BF), head(g_ref, h), 0, 0)
            keys_ref[rows, columns] += dot(grad_scores, head(q_ref, h), 0, 0)
            new.append(state[h] + dot(grad_scores, head(k_ref, h, rows)))
        return tuple(new)

    grad_queries = lax.fori_loop(
        low[block], high[block], step, (jnp.zeros((QUERY_TILE, HS), F32),) * count
    )
    rows = pl.ds(pl.multiple_of(block * QUERY_TILE, QUERY_TILE), QUERY_TILE)
    along = jnp.zeros((QUERY_TILE, 1), F32)
    for h, grad_query in enumerate(grad_queries):
        back, part = head_back(
            grad_query * SCALE, head(qr_ref, h), hg_ref[0:1, :], cos_ref[rows, :], sin_ref[rows, :]
        )
        grad_ref[rows, h * HS : (h + 1) * HS] = back.astype(BF)
        gain_ref[0:1, :] += part
        along += jnp.sum(back * head(qr_ref, h), axis=1, keepdims=True)
    along_ref[rows, :] = along

    @pl.when(block == pl.num_programs(0) - 1)
    def _():
        along_ref[...] += jnp.sum(values_ref[...] * v_ref[...].astype(F32), axis=1, keepdims=True)
        for h in range(count):
            back, part = head_back(
                head(keys_ref, h) * SCALE, head(kr_ref, h), hg_ref[1:2, :], cos_ref[...],
                sin_ref[...],
            )
            grad_ref[:, (count + h) * HS : (count + h + 1) * HS] = back.astype(BF)
            gain_ref[1:2, :] += part
            along_ref[...] += jnp.sum(back * head(kr_ref, h), axis=1, keepdims=True)
        grad_ref[:, 2 * count * HS :] = values_ref[...].astype(BF)


def attend_back(
    heads, grad_mixed, mixed, sums, segment, low, high, raw, cosine, sine, gains, deps=()
):
    tokens, columns = heads.shape
    width = columns // 3
    count = width // HS
    whole = lambda b, lo, hi: (0, 0)
    tile = lambda b, lo, hi: (b, 0)
    return call(
        attend_back_body,
        (tokens // QUERY_TILE,),
        [
            pl.BlockSpec((QUERY_TILE, width), tile),
            pl.BlockSpec((tokens, width), lambda b, lo, hi: (0, 1)),
            pl.BlockSpec((tokens, width), lambda b, lo, hi: (0, 2)),
            pl.BlockSpec((QUERY_TILE, width), tile),
            pl.BlockSpec((QUERY_TILE, width), tile),
            pl.BlockSpec((count, QUERY_TILE, 1), lambda b, lo, hi: (0, b, 0)),
            pl.BlockSpec((QUERY_TILE, 1), tile),
            pl.BlockSpec((1, tokens), whole),
            pl.BlockSpec((QUERY_TILE, width), tile),
            pl.BlockSpec((tokens, width), lambda b, lo, hi: (0, 1)),
            pl.BlockSpec((tokens, HS), whole),
            pl.BlockSpec((tokens, HS), whole),
            pl.BlockSpec((2, HS), whole),
        ],
        [
            pl.BlockSpec((tokens, columns), whole),
            pl.BlockSpec((2, HS), whole),
            pl.BlockSpec((tokens, 1), whole),
        ],
        [shape((tokens, columns), BF), shape((2, HS), F32), shape((tokens, 1), F32)],
        scratch=[
            pltpu.VMEM((tokens, width), F32),
            pltpu.VMEM((tokens, width), F32),
            pltpu.VMEM((count, QUERY_TILE, 1), F32),
        ],
        prefetch=2,
        name="attend_back",
        deps=deps,
    )(
        low, high, heads, heads, heads, grad_mixed, mixed, sums, segment[:, None],
        segment[None, :], raw, raw, cosine, sine, gains,
    )


def dispatch_body(slot_ref, x_ref, out_ref):
    local, capacity = out_ref.shape[1], out_ref.shape[3]
    tokens = x_ref.shape[1]
    rows = x_ref[0]
    order = lax.broadcasted_iota(jnp.int32, (capacity, tokens), 0)
    for index in range(local):
        hot = jnp.where(order == slot_ref[0, 0, index : index + 1, :], 1.0, 0.0).astype(BF)
        out_ref[0, index, 0] = dot(hot, rows).astype(BF)


def dispatch(slots, rows, capacity, deps=()):
    groups, targets, local, tokens = slots.shape
    features = rows.shape[2]
    return call(
        dispatch_body,
        (groups, targets),
        [
            pl.BlockSpec((1, 1, local, tokens), lambda g, d: (g, d, 0, 0)),
            pl.BlockSpec((1, tokens, features), lambda g, d: (g, 0, 0)),
        ],
        pl.BlockSpec((1, local, 1, capacity, features), lambda g, d: (d, 0, g, 0, 0)),
        shape((targets, local, groups, capacity, features), BF),
        name="dispatch",
        deps=deps,
    )(slots, rows)


def combine_body(*refs):
    slot_ref, rows_refs, out_ref = refs[0], refs[1:-1], refs[-1]
    targets, local, _, capacity, features = rows_refs[0].shape
    total_local = local * len(rows_refs)
    tile = out_ref.shape[1]
    order = lax.broadcasted_iota(jnp.int32, (tile, capacity), 1)
    slots = slot_ref[0]
    total = jnp.zeros((tile, features), F32)
    for target in range(targets):
        for part, rows_ref in enumerate(rows_refs):
            first = target * total_local + part * local
            hot = jnp.concatenate(
                [
                    jnp.where(order == slots[:, first + i : first + i + 1], 1.0, 0.0).astype(BF)
                    for i in range(local)
                ],
                axis=1,
            )
            total = total + dot(hot, rows_ref[target].reshape(local * capacity, features))
    out_ref[0] = total.astype(BF)


def combine(slots_by_token, parts, chunk, features, deps=()):
    groups, tokens, experts = slots_by_token.shape
    targets, local, _, capacity, _ = parts[0].shape
    tile = 512
    return call(
        combine_body,
        (groups, tokens // tile),
        [pl.BlockSpec((1, tile, experts), lambda g, t: (g, t, 0))]
        + [
            pl.BlockSpec(
                (targets, local, 1, capacity, features), lambda g, t: (0, 0, g, 0, chunk)
            )
        ]
        * len(parts),
        pl.BlockSpec((1, tile, features), lambda g, t: (g, t, 0)),
        shape((groups, tokens, features), BF),
        name="combine",
        flops=2 * groups * experts * capacity * tokens * features,
        deps=deps,
    )(slots_by_token, *parts)


def block_rows(ref, row=0):
    _, cores, _, groups, capacity, features = ref.shape
    return ref[row].reshape(cores * groups * capacity, features)


def expert_body(*refs):
    x_ref, c_refs = refs[0], refs[1 : 1 + CHUNKS]
    gate_w, up_w, down_w, prob_ref, act_ref, gate_out, up_out = refs[1 + CHUNKS :]
    rows, width = x_ref.shape[0], x_ref.shape[-1]
    prob = prob_ref[0]
    gate = up = grad = None
    for row in range(rows):
        features = pl.ds(row * width, width)
        x = block_rows(x_ref, row)
        gate_part = dot(x, gate_w[0, features, :])
        up_part = dot(x, up_w[0, features, :])
        grad_part = None
        for chunk, c_ref in enumerate(c_refs):
            c = (block_rows(c_ref, row).astype(F32) * prob).astype(BF)
            part_width = width // CHUNKS
            part = dot(c, down_w[0, pl.ds(row * width + chunk * part_width, part_width), :])
            grad_part = part if grad_part is None else grad_part + part
        gate = gate_part if gate is None else gate + gate_part
        up = up_part if up is None else up + up_part
        grad = grad_part if grad is None else grad + grad_part
    squashed = 1.0 / (1.0 + jnp.exp(-gate))
    act_ref[...] = (gate * squashed * up).astype(BF)
    gate_out[...] = (grad * up * squashed * (1.0 + gate * (1.0 - squashed))).astype(BF)
    up_out[...] = (grad * gate * squashed).astype(BF)


def expert(index, rows, cots, gate_weight, up_weight, down_weight, prob):
    row_count, cores, _, groups, capacity, width = rows.shape
    _, features, hidden = gate_weight.shape
    slots = groups * capacity
    tile = min(512, hidden, 512 * 1024 // slots)
    row_spec = pl.BlockSpec(
        (row_count, 1, 1, groups, capacity, width), lambda n, k: (0, k, 0, 0, 0, 0)
    )
    cot_spec = pl.BlockSpec(
        (row_count, 1, 1, groups, capacity, width // CHUNKS), lambda n, k: (0, k, index, 0, 0, 0)
    )
    w_spec = pl.BlockSpec((1, features, tile), lambda n, k: (index, 0, n))
    out_spec = pl.BlockSpec((slots, tile), lambda n, k: (k, n))
    return call(
        expert_body,
        (hidden // tile, cores),
        [row_spec] + [cot_spec] * CHUNKS + [w_spec, w_spec, w_spec]
        + [pl.BlockSpec((1, slots, 1), lambda n, k: (index, k, 0))],
        [out_spec] * 3,
        [shape((cores * slots, hidden), BF)] * 3,
        name="expert",
    )(rows, *cots, gate_weight, up_weight, down_weight, prob)


def produce_body(act_ref, w_ref, prob_ref, *refs):
    c_refs, out_refs, inner_ref = refs[:CHUNKS], refs[-CHUNKS - 1 : -1], refs[-1]
    width = out_refs[0].shape[-1]

    @pl.when(pl.program_id(1) == 0)
    def _():
        inner_ref[...] = jnp.zeros_like(inner_ref)

    made = dot(act_ref[...], w_ref[0], 1, 1)
    weighted = (made * prob_ref[0]).astype(BF)
    for chunk, out_ref in enumerate(out_refs):
        columns = slice(chunk * width, (chunk + 1) * width)
        inner_ref[...] += jnp.sum(
            made[:, columns] * block_rows(c_refs[chunk]).astype(F32), axis=1, keepdims=True
        )
        out_ref[...] = weighted[:, columns].reshape(out_ref.shape)


def produce(index, activated, down_weight, prob, cots, dims, buffers):
    rows, cores, local, groups, capacity, width = dims
    hidden = activated.shape[1]
    slots = groups * capacity
    given = () if buffers is None else tuple(buffers)
    outs = pl.pallas_call(
        produce_body,
        out_shape=[shape(dims, BF)] * CHUNKS + [shape((cores * slots, 1), F32)],
        grid=(cores, rows),
        in_specs=[
            pl.BlockSpec((slots, hidden), lambda k, r: (k, 0)),
            pl.BlockSpec((1, width * CHUNKS, hidden), lambda k, r: (index, r, 0)),
            pl.BlockSpec((1, slots, 1), lambda k, r: (index, k, 0)),
        ]
        + [
            pl.BlockSpec((1, 1, 1, groups, capacity, width), lambda k, r: (r, k, index, 0, 0, 0))
        ]
        * CHUNKS
        + [pl.BlockSpec(memory_space=pl.ANY)] * len(given),
        out_specs=[
            pl.BlockSpec(
                (1, 1, 1, groups, capacity, width), lambda k, r: (r, k, index, 0, 0, 0)
            )
        ]
        * CHUNKS
        + [pl.BlockSpec((slots, 1), lambda k, r: (k, 0))],
        input_output_aliases={3 + CHUNKS + chunk: chunk for chunk in range(len(given))},
        compiler_params=pltpu.CompilerParams(
            dimension_semantics=("arbitrary",) * 2, vmem_limit_bytes=VMEM_BYTES
        ),
        cost_estimate=pl.CostEstimate(
            flops=2 * cores * slots * D * hidden,
            bytes_accessed=2 * D * hidden + 8 * cores * slots * D,
            transcendentals=0,
        ),
        name="produce",
    )(activated, down_weight, prob, *cots, *given)
    return outs[:CHUNKS], outs[CHUNKS]


def held_while(expert_index, last):
    return lambda i, r: jnp.where(i == expert_index, r, jnp.where(i < expert_index, 0, last))


def down_grad_body(*refs):
    prob_ref, c_refs, act_refs, out_ref = (
        refs[0], refs[1 : 1 + CHUNKS], refs[1 + CHUNKS : -1], refs[-1]
    )
    width = c_refs[0].shape[-1]
    for index, act_ref in enumerate(act_refs):

        @pl.when(pl.program_id(0) == index)
        def _():
            for chunk, c_ref in enumerate(c_refs):
                c = (block_rows(c_ref).astype(F32) * prob_ref[0]).astype(BF)
                out_ref[0, pl.ds(chunk * width, width), :] = dot(c, act_ref[...], 0, 0)


def row_specs(local, shape_of):
    rows, cores, _, groups, capacity, width = shape_of

    def spec(index):
        where = held_while(index, rows - 1)
        return pl.BlockSpec(
            (1, cores, 1, groups, capacity, width), lambda i, r: (where(i, r), 0, 0, 0, 0, 0)
        )

    return [spec(index) for index in range(local)]


def down_grad(cots, prob, activated, deps=()):
    rows, cores, local, groups, capacity, width = cots[0].shape
    slots, hidden = activated[0].shape
    return call(
        down_grad_body,
        (local, rows),
        [pl.BlockSpec((1, slots, 1), lambda i, r: (i, 0, 0))]
        + [pl.BlockSpec((1, cores, 1, groups, capacity, width), lambda i, r: (r, 0, i, 0, 0, 0))]
        * CHUNKS
        + [pl.BlockSpec((slots, hidden), lambda i, r: (0, 0))] * local,
        pl.BlockSpec((1, width * CHUNKS, hidden), lambda i, r: (i, r, 0)),
        shape((local, rows * width * CHUNKS, hidden), F32),
        name="down_grad",
        flops=2 * local * slots * D * hidden,
        deps=deps,
    )(prob, *cots, *activated)


def gate_grad_body(*refs):
    local = (len(refs) - 2) // 3
    x_refs, gate_refs, up_refs = refs[:local], refs[local : 2 * local], refs[2 * local : -2]
    gate_out, up_out = refs[-2:]
    for index in range(local):

        @pl.when(pl.program_id(0) == index)
        def _():
            x = block_rows(x_refs[index])
            gate_out[0] = dot(x, gate_refs[index][...], 0, 0)
            up_out[0] = dot(x, up_refs[index][...], 0, 0)


def gate_grad(parts, grad_gate_pre, grad_up_pre, deps=()):
    rows, cores, _, groups, capacity, width = parts[0].shape
    slots, hidden = grad_gate_pre[0].shape
    local = len(parts)
    wide = pl.BlockSpec((slots, hidden), lambda i, r: (0, 0))
    out = pl.BlockSpec((1, width, hidden), lambda i, r: (i, r, 0))
    return call(
        gate_grad_body,
        (local, rows),
        row_specs(local, parts[0].shape) + [wide] * (2 * local),
        [out, out],
        [shape((local, rows * width, hidden), F32)] * 2,
        name="gate_grad",
        deps=deps,
    )(*parts, *grad_gate_pre, *grad_up_pre)


def rows_back_body(gate_ref, up_ref, gate_w, up_w, *refs):
    out_ref = refs[-1]
    made = dot(gate_ref[...], gate_w[0], 1, 1) + dot(up_ref[...], up_w[0], 1, 1)
    out_ref[...] = made.astype(BF).reshape(out_ref.shape)


def rows_back(
    index, grad_gate_pre, grad_up_pre, gate_weight, up_weight, chunk, dims, buffer, deps=()
):
    rows, cores, local, groups, capacity, width = dims
    hidden = gate_weight.shape[2]
    slots = groups * capacity
    pre = pl.BlockSpec((slots, hidden), lambda k, r: (k, 0))
    weight = pl.BlockSpec((1, width, hidden), lambda k, r: (index, r * CHUNKS + chunk, 0))
    given = () if buffer is None else (buffer,)
    return pl.pallas_call(
        rows_back_body,
        out_shape=shape(dims, BF),
        grid=(cores, rows),
        in_specs=[pre, pre, weight, weight]
        + [pl.BlockSpec(memory_space=pl.ANY)] * len(given + tuple(deps)),
        out_specs=pl.BlockSpec(
            (1, 1, 1, groups, capacity, width), lambda k, r: (r, k, index, 0, 0, 0)
        ),
        input_output_aliases={4: 0} if given else {},
        compiler_params=pltpu.CompilerParams(
            dimension_semantics=("arbitrary",) * 2, vmem_limit_bytes=VMEM_BYTES
        ),
        cost_estimate=pl.CostEstimate(
            flops=4 * cores * slots * width * rows * hidden,
            bytes_accessed=4 * rows * width * hidden + 6 * cores * slots * width * rows,
            transcendentals=0,
        ),
        name="rows_back",
    )(grad_gate_pre, grad_up_pre, gate_weight, up_weight, *given, *deps)


def swap(rows):
    return lax.all_to_all(rows, SWAP_AXES, split_axis=0, concat_axis=0, tiled=True)


def slot_positions(routes, ranks, capacity):
    experts = jnp.arange(E, dtype=jnp.int32)
    member = jnp.any(routes.T[:, None, :] == experts[None, :, None], axis=0)
    earlier = (ranks[:, None] < ranks[None, :]).astype(BF)
    position = jnp.dot(member.astype(BF), earlier, preferred_element_type=F32)
    return jnp.where(member & (position < capacity), position, -1.0)


def per_device(
    hidden_in,
    attention_gain,
    query_weight,
    key_weight,
    value_weight,
    projection,
    query_gain,
    key_gain,
    feedforward_gain,
    router_weight,
    gate_weight,
    up_weight,
    down_weight,
    segments,
    routes,
    priority,
    cotangent,
):
    tokens, width_here = hidden_in.shape
    row_count = lax.axis_size("row")
    z_count = lax.axis_size("z")
    core_count = lax.axis_size("core")
    local = gate_weight.shape[0]
    piece_count = row_count * z_count * core_count * local
    pieces = max(1, piece_count // E)
    capacity = tokens * TOPK // E
    width = width_here // CHUNKS
    row_index = lax.axis_index("row")
    z_index = lax.axis_index("z")
    core_index = lax.axis_index("core")
    head_columns = query_weight.shape[1]
    experts_here = E // row_count
    head_count = head_columns // HS

    hidden_pieces, hidden_starts = row_gather(
        jnp.concatenate(
            [hidden_in, jnp.broadcast_to(attention_gain[None, :], (GAIN_ROWS, width_here))], axis=0
        )
    )
    qkv_full = lax.all_gather(
        jnp.concatenate([query_weight, key_weight, value_weight], axis=1),
        TOKENS_AXES,
        axis=0,
        tiled=True,
    )
    with_router = lax.all_gather(
        jnp.concatenate([projection, router_weight], axis=1),
        TOKENS_AXES,
        axis=0,
        tiled=True,
    )
    projection_full = with_router[:, :head_columns]
    router_rows = with_router[:, head_columns:].reshape(row_count, width_here, -1)
    router_here = jnp.swapaxes(small_row_swap(router_rows), 1, 2).reshape(E, width_here)

    position = slot_positions(routes, priority[0], capacity)
    by_piece = jnp.repeat(position.astype(BF), pieces, axis=0).reshape(
        row_count, z_count, core_count * local, tokens
    )
    mine = lax.all_to_all(jnp.swapaxes(by_piece, 0, 1), "z", 0, 0, tiled=True).astype(jnp.int32)
    slots = mine.reshape(z_count, row_count * core_count, local, tokens)
    slots_by_token = jnp.swapaxes(
        mine.reshape(z_count, row_count * core_count * local, tokens), 1, 2
    )
    dims = (row_count, core_count, local, z_count, capacity, width)

    expert_dims = (row_count, core_count, 1, z_count, capacity, width_here)
    def scatter_back(summed):
        return lax.psum_scatter(summed, "z", scatter_dimension=0, tiled=True).reshape(
            tokens, width
        )

    spread_cots = [
        lax.all_gather(
            after(cotangent[:, chunk * width : (chunk + 1) * width], *hidden_pieces[2:6]),
            "z",
            axis=0,
        )
        for chunk in range(CHUNKS)
    ]
    first_picked = dispatch(slots, spread_cots[0], capacity)

    cosine, sine = rotary_tables()
    first_gain = attention_gain.astype(F32)
    second_gain = feedforward_gain.astype(F32)
    head_gains = jnp.stack([query_gain, key_gain]).astype(F32)
    residual = hidden_in.astype(F32)
    normed_one, heads, raw, first_factor = project(
        hidden_starts,
        hidden_pieces,
        qkv_full,
        cosine,
        sine,
        jnp.repeat(head_gains, head_count, axis=0).reshape(1, -1),
        (mine, router_here),
    )
    segment = segments[0]
    low, high = key_ranges(segment)
    mixed, sums = attend(heads, segment, low, high)
    middle = residual + row_scatter(
        mixed, row_scatter_order(projection_full), first_picked
    )[0]
    second_factor = lax.rsqrt(lax.psum(jnp.sum(middle * middle, axis=1), "row") / D + EPSILON)[
        :, None
    ]
    normed_two = (middle * second_factor * second_gain).astype(BF)

    logits = row_sum(dot(router_here, normed_two, 1, 1))
    raised = jnp.exp(logits)
    router_probs = raised / jnp.sum(raised, axis=0, keepdims=True)

    cots = [swap(after(first_picked, normed_two)).reshape(dims)]
    for spread in spread_cots[1:]:
        picked = dispatch(slots, spread, capacity, [normed_two])
        cots.append(swap(after(picked, cots[-1])).reshape(dims))
    spread_rows = lax.all_gather(normed_two, "z", axis=0)
    rows = []
    for index in range(local):
        picked = dispatch(slots[:, :, index : index + 1], spread_rows, capacity, cots[:1])
        rows.append(swap(after(picked, logits, cots[-1], *rows[-1:])).reshape(expert_dims))
    own_slots = lax.dynamic_slice_in_dim(position, row_index * experts_here, experts_here, 0)
    own_probs = lax.dynamic_slice_in_dim(router_probs, row_index * experts_here, experts_here, 0)
    order = jnp.arange(capacity, dtype=jnp.int32).astype(F32)
    slot_prob = jnp.sum(
        jnp.where(own_slots[:, None, :] == order[None, :, None], own_probs[:, None, :], 0.0), axis=2
    )
    prob_groups = jnp.repeat(
        lax.all_gather(slot_prob, TOKENS_AXES, axis=0), pieces, axis=1
    ).reshape(z_count, core_count, z_count, core_count, local, capacity)
    prob_here = lax.dynamic_index_in_dim(
        lax.dynamic_index_in_dim(prob_groups, z_index, 2, keepdims=False),
        core_index,
        2,
        keepdims=False,
    )
    prob = jnp.transpose(prob_here, (2, 1, 0, 3)).reshape(
        local, core_count * z_count * capacity, 1
    )
    swapped_dims = (row_count * core_count,) + dims[2:]
    activated, grad_gate_pre, grad_up_pre = [], [], []
    buffers = [None] * CHUNKS
    for index in range(local):
        rows_here = rows[index]
        act, gate_pre, up_pre = expert(
            index, rows_here, cots, gate_weight, up_weight, down_weight, prob
        )
        activated.append(act)
        grad_gate_pre.append(gate_pre)
        grad_up_pre.append(up_pre)
        for chunk in range(CHUNKS):
            buffers[chunk] = rows_back(
                index, gate_pre, up_pre, gate_weight, up_weight, chunk, dims, buffers[chunk],
                buffers[:chunk] if index == local - 1 else (),
            )
    inners, made_buffers = [], None
    for index in range(local):
        made_buffers, inner = produce(
            index, activated[index], down_weight, prob, cots, dims, made_buffers
        )
        inners.append(inner)

    inner = jnp.stack(inners).reshape(local, core_count, z_count, capacity)
    to_groups = jnp.transpose(inner, (2, 1, 0, 3)).reshape(
        z_count * core_count, local * capacity
    )
    back_rows = [swap(buffers[0].reshape(swapped_dims))]
    to_groups = after(to_groups, back_rows[0], buffers[1])
    of_group = lax.all_to_all(to_groups, TOKENS_AXES, 0, 0, tiled=True).reshape(-1, capacity)
    slot_grads = jnp.sum(small_row_gather(of_group).reshape(E, pieces, capacity), axis=1)
    grad_down = down_grad(cots, prob, activated, inners)
    ready = after(buffers[1], grad_down, slot_grads)
    back_rows.append(swap(ready.reshape(swapped_dims)))
    grad_prob = jnp.sum(
        jnp.where(position[:, None, :] == order[None, :, None], slot_grads[:, :, None], 0.0), axis=1
    )
    grad_logits = (
        router_probs * (grad_prob - jnp.sum(router_probs * grad_prob, axis=0, keepdims=True))
    ).astype(BF)
    from_router = dot(grad_logits, router_here, 0, 0)
    first_sum = combine(slots_by_token, [back_rows[0]], 0, width, [grad_down, to_groups])
    grad_gate, grad_up = gate_grad(rows, grad_gate_pre, grad_up_pre, [first_sum])
    first_sum = scatter_back(first_sum)
    second_sum = scatter_back(
        combine(slots_by_token, [back_rows[1]], 0, width, [grad_gate, first_sum, from_router])
    )
    grad_normed_two = from_router + jnp.concatenate(
        [first_sum, second_sum], axis=1
    ).astype(F32)
    router_part = dot(grad_logits, normed_two)
    router_swapped = lax.all_to_all(
        router_part.reshape(row_count, experts_here, width_here), "row", 0, 0, tiled=True
    )
    grad_router = lax.psum_scatter(
        jnp.swapaxes(router_swapped, 0, 1).reshape(experts_here, D),
        TOKENS_AXES,
        scatter_dimension=1,
        tiled=True,
    )

    scaled_two = grad_normed_two * second_gain
    second_inner = lax.psum(jnp.sum(scaled_two * middle, axis=1), "row")[:, None]
    grad_middle = (
        cotangent.astype(F32)
        + scaled_two * second_factor
        - middle * second_factor**3 * second_inner / D
    )
    grad_feedforward_gain = jnp.sum(grad_normed_two * middle * second_factor, axis=0)

    grad_branch = grad_middle.astype(BF)
    made_rows = [swap(after(made_buffers[0], back_rows[1], router_swapped).reshape(swapped_dims))]
    branch_pieces, branch_starts = row_gather(after(grad_branch, made_rows[0]))
    made_rows.append(swap(after(made_buffers[1], *branch_pieces).reshape(swapped_dims)))
    made_sums = [combine(slots_by_token, [made_rows[0]], 0, width, [grad_branch])]
    grad_projection = projection_grad(branch_starts, branch_pieces, mixed, made_sums)
    grad_mixed = mix_back(
        branch_starts, branch_pieces, projection_full, [grad_projection, router_swapped]
    )
    projection_sum = core_sum(grad_projection)
    grad_raw, head_gain_grads, along = attend_back(
        heads, grad_mixed, mixed, sums, segment, low, high, raw, cosine, sine, head_gains,
        [projection_sum],
    )
    from_experts = [scatter_back(made_sums[0])]
    grad_raw = after(grad_raw, made_rows[1], from_experts[0], grad_router)
    grad_first, sent, received = row_scatter(grad_raw, row_scatter_order(qkv_full))
    from_experts.append(
        scatter_back(combine(slots_by_token, [made_rows[1]], 0, width, sent))
    )
    small = jnp.concatenate([along.reshape(-1, HS), head_gain_grads], axis=0)
    small = jnp.sum(small_row_gather(small), axis=0)
    first_inner = small[:-2].reshape(-1, 1) / first_factor
    head_gain_grads = small[-2:]
    grad_qkv = dot(after(normed_one, *received), grad_raw, 0, 0).astype(BF)
    scaled_one = grad_first * first_gain
    grad_input = (
        grad_middle + scaled_one * first_factor - residual * first_factor**3 * first_inner / D
    )
    grad_attention_gain = jnp.sum(grad_first * residual * first_factor, axis=0)

    grad_attention_gain, grad_feedforward_gain, head_gain_grads = lax.psum(
        (grad_attention_gain, grad_feedforward_gain, head_gain_grads), TOKENS_AXES
    )
    grad_projection = z_scatter(projection_sum).astype(F32)
    grad_qkv = z_scatter(core_sum(grad_qkv)).astype(F32)
    from_experts = jnp.concatenate(from_experts, axis=1).astype(F32)
    output = (after(middle, grad_first) + from_experts).astype(BF)
    return (
        output,
        grad_input,
        grad_attention_gain,
        grad_qkv[:, :head_columns],
        grad_qkv[:, head_columns : 2 * head_columns],
        grad_qkv[:, 2 * head_columns :],
        grad_projection,
        head_gain_grads[0],
        head_gain_grads[1],
        grad_feedforward_gain,
        grad_router.T,
        grad_gate,
        grad_up,
        grad_down,
    )


def solution(mesh):
    rows, columns = mesh.shape["row"], mesh.shape["col"]
    split_mesh = Mesh(
        mesh.devices.reshape(rows, columns // 2, 2), ("row", "z", "core")
    )
    both = P(TOKENS_AXES, "row")
    expert = P(ALL_AXES, None, None)
    grouped = P(TOKENS_AXES, None)
    return jax.shard_map(
        per_device,
        mesh=split_mesh,
        in_specs=(
            both, P("row"), both, both, both, both, P(), P(), P("row"), both,
            expert, expert, expert, grouped, grouped, grouped, both,
        ),
        out_specs=(
            both, both, P("row"), both, both, both, both, P(), P(), P("row"), both,
            expert, expert, expert,
        ),
        check_vma=False,
    )
```

```python
import functools

import jax
import jax.numpy as jnp
from jax import lax
from jax.experimental import pallas as pl
from jax.experimental.pallas import tpu as pltpu
from jax.sharding import Mesh, PartitionSpec as P

D = 2048
HS = 128
E = 64
TOPK = 8
SEQ = 2048
EPSILON = 1e-06
SCALE = HS ** (-0.5)
CHUNKS = 2
GAIN_ROWS = 16
TOKENS_AXES = ("z", "core")
SWAP_AXES = ("row", "core")
ALL_AXES = ("row", "z", "core")
BF = jnp.bfloat16
F32 = jnp.float32
VMEM_BYTES = 60 * 1024 * 1024


def call(body, grid, in_specs, out_specs, out_shape, scratch=(), prefetch=0, name=None, deps=(), flops=0):
    deps = tuple(deps)

    def without_deps(*refs):
        body(*refs[:prefetch], *refs[prefetch + len(deps) :])

    kernel = pl.pallas_call(
        without_deps,
        out_shape=out_shape,
        grid_spec=pltpu.PrefetchScalarGridSpec(
            num_scalar_prefetch=prefetch,
            grid=grid,
            in_specs=[pl.BlockSpec(memory_space=pl.ANY)] * len(deps) + list(in_specs),
            out_specs=out_specs,
            scratch_shapes=list(scratch),
        ),
        compiler_params=pltpu.CompilerParams(
            dimension_semantics=("arbitrary",) * len(grid), vmem_limit_bytes=VMEM_BYTES
        ),
        cost_estimate=pl.CostEstimate(flops=flops, bytes_accessed=0, transcendentals=0),
        name=name,
    )
    return lambda *args: kernel(*args[:prefetch], *deps, *args[prefetch:])


def shape(dims, dtype):
    return jax.ShapeDtypeStruct(dims, dtype)


def dot(left, right, left_dim=1, right_dim=0):
    return lax.dot_general(
        left, right, (((left_dim,), (right_dim,)), ((), ())), preferred_element_type=F32
    )


def rotary_tables():
    half_size = HS // 2
    inverse = 50000.0 ** (-(jnp.arange(half_size, dtype=F32) * 2.0) / HS)
    angles = jnp.arange(SEQ, dtype=F32)[:, None] * inverse[None, :]
    cosine, sine = jnp.cos(angles), jnp.sin(angles)
    return (
        jnp.concatenate([cosine, cosine], axis=1),
        jnp.concatenate([-sine, sine], axis=1),
    )


def project_body(starts, *refs):
    count = starts.shape[0]
    x_refs, gain_refs, refs = refs[:count], refs[count : 2 * count], refs[2 * count :]
    w_ref, cos_ref, sin_ref, hg_ref, normed_ref, heads_ref, raw_ref, factor_ref = refs
    width = x_refs[0].shape[1]
    square = sum(
        jnp.sum(jnp.square(x_ref[...].astype(F32)), axis=1, keepdims=True) for x_ref in x_refs
    )
    factor = lax.rsqrt(square / (width * count) + EPSILON)
    factor_ref[...] = factor
    raw = None
    for index, x_ref in enumerate(x_refs):
        features = pl.ds(pl.multiple_of(starts[index], width), width)
        gain = gain_refs[index][0:1, :].astype(F32)
        normed = (x_ref[...].astype(F32) * factor * gain).astype(BF)
        normed_ref[:, features] = normed
        part = dot(normed, w_ref[features, :])
        raw = part if raw is None else raw + part
    turned = raw_ref.shape[1]
    raw_ref[...] = raw[:, :turned]
    cosine, sine = cos_ref[...], sin_ref[...]
    for head in range(turned // HS):
        part = raw[:, head * HS : (head + 1) * HS]
        unit = part * lax.rsqrt(jnp.mean(part * part, axis=1, keepdims=True) + EPSILON)
        scaled = unit * hg_ref[:, head * HS : (head + 1) * HS]
        heads_ref[:, head * HS : (head + 1) * HS] = (
            scaled * cosine + pltpu.roll(scaled, HS // 2, 1) * sine
        ).astype(BF)
    heads_ref[:, turned:] = raw[:, turned:].astype(BF)


def project(starts, pieces, weights, cosine, sine, head_gains, deps=()):
    tokens, piece = cosine.shape[0], pieces[0].shape[1]
    width, columns = weights.shape
    turned = columns // 3 * 2
    tile = 256
    own = lambda t, s: (t, 0)
    whole = lambda t, s: (0, 0)
    return call(
        project_body,
        (tokens // tile,),
        [pl.BlockSpec((tile, piece), own)] * len(pieces)
        + [pl.BlockSpec((GAIN_ROWS, piece), lambda t, s: (tokens // GAIN_ROWS, 0))] * len(pieces)
        + [
            pl.BlockSpec((width, columns), whole),
            pl.BlockSpec((tile, HS), own),
            pl.BlockSpec((tile, HS), own),
            pl.BlockSpec((1, turned), whole),
        ],
        [
            pl.BlockSpec((tile, width), own),
            pl.BlockSpec((tile, columns), own),
            pl.BlockSpec((tile, turned), own),
            pl.BlockSpec((tile, 1), own),
        ],
        [
            shape((tokens, width), BF),
            shape((tokens, columns), BF),
            shape((tokens, turned), F32),
            shape((tokens, 1), F32),
        ],
        prefetch=1,
        name="project",
        deps=deps,
    )(starts, *pieces, *pieces, weights, cosine, sine, head_gains)


def mix_back_body(starts, *refs):
    count = starts.shape[0]
    g_refs, (w_ref, out_ref) = refs[:count], refs[count:]
    width = g_refs[0].shape[1]
    total = None
    for index, g_ref in enumerate(g_refs):
        part = dot(g_ref[...], w_ref[pl.ds(pl.multiple_of(starts[index], width), width), :])
        total = part if total is None else total + part
    out_ref[...] = total.astype(BF)


def mix_back(starts, pieces, weights, deps=()):
    tokens, piece = pieces[0].shape
    width, columns = weights.shape
    tile = 256
    return call(
        mix_back_body,
        (tokens // tile,),
        [pl.BlockSpec((tile, piece), lambda t, s: (t, 0))] * len(pieces)
        + [pl.BlockSpec((width, columns), lambda t, s: (0, 0))],
        pl.BlockSpec((tile, columns), lambda t, s: (t, 0)),
        shape((tokens, columns), BF),
        prefetch=1,
        name="mix_back",
        deps=deps,
    )(starts, *pieces, weights)


def projection_grad_body(starts, *refs):
    count = starts.shape[0]
    g_refs, (mixed_ref, out_ref, total_ref) = refs[:count], refs[count:]
    width = g_refs[0].shape[1]

    @pl.when(pl.program_id(0) == 0)
    def _():
        total_ref[...] = jnp.zeros_like(total_ref)

    for index, g_ref in enumerate(g_refs):
        rows = pl.ds(pl.multiple_of(starts[index], width), width)
        total_ref[rows, :] += dot(g_ref[...], mixed_ref[...], 0, 0)

    @pl.when(pl.program_id(0) == pl.num_programs(0) - 1)
    def _():
        out_ref[...] = total_ref[...].astype(BF)


def projection_grad(starts, pieces, mixed, deps=()):
    tokens, piece = pieces[0].shape
    columns = mixed.shape[1]
    width = piece * len(pieces)
    tile = 512
    return call(
        projection_grad_body,
        (tokens // tile,),
        [pl.BlockSpec((tile, piece), lambda t, s: (t, 0))] * len(pieces)
        + [pl.BlockSpec((tile, columns), lambda t, s: (t, 0))],
        pl.BlockSpec((width, columns), lambda t, s: (0, 0)),
        shape((width, columns), BF),
        scratch=[pltpu.VMEM((width, columns), F32)],
        prefetch=1,
        name="projection_grad",
        deps=deps,
    )(starts, *pieces, mixed)


def permute(values, mask):
    return lax.ppermute(values, "row", [(i, i ^ mask) for i in range(4)])


def row_gather(values):
    width = values.shape[1]
    if lax.axis_size("row") != 4:
        return [lax.all_gather(values, "row", axis=1, tiled=True)], jnp.zeros((1,), jnp.int32)
    half = width // 2
    left, right = values[:, :half], values[:, half:]
    left_1, right_2 = permute(left, 1), permute(right, 2)
    left_2, right_1 = permute(left, 2), permute(right, 1)
    left_3, right_3 = permute(left_1, 2), permute(right_2, 1)
    me = lax.axis_index("row")
    starts = jnp.stack(
        [(me ^ mask) * width + side * half for mask in range(4) for side in range(2)]
    ).astype(jnp.int32)
    return [left, right, left_1, right_1, left_2, right_2, left_3, right_3], starts


def small_row_gather(values):
    if lax.axis_size("row") != 4:
        return lax.all_gather(values, "row", axis=0)
    stacked = jnp.stack([values] + [permute(values, mask) for mask in (1, 2, 3)])
    return jnp.take(stacked, lax.axis_index("row") ^ jnp.arange(4), axis=0)


def small_row_swap(blocks):
    if lax.axis_size("row") != 4:
        return lax.all_to_all(blocks, "row", 0, 0, tiled=True)
    me = lax.axis_index("row")
    near = jnp.take(blocks, me ^ jnp.arange(4), axis=0)
    stacked = jnp.stack([near[0]] + [permute(near[mask], mask) for mask in (1, 2, 3)])
    return jnp.take(stacked, me ^ jnp.arange(4), axis=0)


def core_sum(values):
    z_count, core_count = lax.axis_size("z"), lax.axis_size("core")
    rows, columns = values.shape
    blocks = values.reshape(z_count, core_count, rows // (z_count * core_count), columns)
    core = lax.axis_index("core")
    keep = lax.dynamic_index_in_dim(blocks, core, 1, keepdims=False)
    give = lax.dynamic_index_in_dim(blocks, 1 - core, 1, keepdims=False)
    got = lax.ppermute(give, "core", [(0, 1), (1, 0)])
    return (keep.astype(F32) + got.astype(F32)).astype(values.dtype).reshape(-1, columns)


def z_scatter(values):
    return lax.psum_scatter(values, "z", scatter_dimension=0, tiled=True)


def row_sum(values):
    if lax.axis_size("row") != 4:
        return jnp.sum(lax.all_gather(values, "row", axis=0), axis=0)
    half = values.shape[1] // 2
    left, right = values[:, :half], values[:, half:]
    left, right = left + permute(left, 1), right + permute(right, 2)
    return jnp.concatenate([left + permute(left, 2), right + permute(right, 1)], axis=1)


def after(value, *others):
    others = [other for other in others if other is not None]
    return pl.pallas_call(
        lambda *refs: None,
        out_shape=shape(value.shape, value.dtype),
        in_specs=[pl.BlockSpec(memory_space=pl.ANY)] * (1 + len(others)),
        out_specs=pl.BlockSpec(memory_space=pl.ANY),
        input_output_aliases={0: 0},
        cost_estimate=pl.CostEstimate(flops=0, bytes_accessed=0, transcendentals=0),
        name="after",
    )(value, *others)


def row_scatter_order(weights):
    if lax.axis_size("row") != 4:
        return weights
    width = weights.shape[0] // 4
    half = width // 2
    me = lax.axis_index("row")
    order = [(1, 0), (3, 0), (2, 1), (3, 1), (2, 0), (1, 1), (0, 0), (0, 1)]
    return jnp.concatenate(
        [
            lax.dynamic_slice_in_dim(weights, (me ^ mask) * width + side * half, half, 0)
            for mask, side in order
        ],
        axis=0,
    )


def row_scatter(left, ordered, *meanwhile):
    if lax.axis_size("row") != 4:
        return lax.psum_scatter(
            dot(left, ordered, 1, 1).astype(BF), "row", scatter_dimension=1, tiled=True
        ).astype(F32), (), ()
    width = ordered.shape[0] // 4
    half = width // 2
    part = lambda index: dot(left, ordered[index * width : (index + 1) * width], 1, 1)
    sent = [part(0).astype(BF), part(1).astype(BF)]
    received = [permute(sent[0], 1), permute(sent[1], 2)]
    from_x, from_y = received[0].astype(F32), received[1].astype(F32)
    onward, own = part(2), part(3)
    onward_left = (onward[:, :half] + from_x[:, half:]).astype(BF)
    onward_right = (onward[:, half:] + from_y[:, half:]).astype(BF)
    if meanwhile:
        onward_left = after(onward_left, *meanwhile)
        onward_right = after(onward_right, *meanwhile)
    last_left = permute(onward_left, 2).astype(F32)
    last_right = permute(onward_right, 1).astype(F32)
    total = jnp.concatenate(
        [
            own[:, :half] + from_x[:, :half] + last_left,
            own[:, half:] + from_y[:, :half] + last_right,
        ],
        axis=1,
    )
    return total, sent, received


QUERY_TILE = 256
KEY_TILE = 256
EXP2_SCALE = SCALE * 1.4426950408889634


def key_ranges(segment):
    first = segment[::QUERY_TILE]
    last = segment[QUERY_TILE - 1 :: QUERY_TILE]
    key_first = segment[::KEY_TILE]
    key_last = segment[KEY_TILE - 1 :: KEY_TILE]
    meets = (key_first[None, :] <= last[:, None]) & (key_last[None, :] >= first[:, None])
    order = jnp.arange(meets.shape[1], dtype=jnp.int32)[None, :]
    low = jnp.min(jnp.where(meets, order, meets.shape[1]), axis=1)
    high = jnp.max(jnp.where(meets, order + 1, 0), axis=1)
    return low.astype(jnp.int32), high.astype(jnp.int32)


def key_rows(step):
    return pl.ds(pl.multiple_of(step * KEY_TILE, KEY_TILE), KEY_TILE)


def head(ref, index, rows=slice(None)):
    return ref[rows, index * HS : (index + 1) * HS]


def attend_body(low, high, q_ref, k_ref, v_ref, qs_ref, ks_ref, out_ref, sum_ref):
    block = pl.program_id(0)
    count = q_ref.shape[1] // HS
    query_docs = qs_ref[...]

    def step(index, state):
        rows = key_rows(index)
        allowed = query_docs == ks_ref[:, rows]
        scores = [dot(head(q_ref, h), head(k_ref, h, rows), 1, 1) for h in range(count)]
        raised = [jnp.where(allowed, jnp.exp2(each * EXP2_SCALE), 0.0) for each in scores]
        return tuple(
            (
                total + jnp.sum(each, axis=1, keepdims=True),
                mixed + dot(each.astype(BF), head(v_ref, h, rows)),
            )
            for h, (each, (total, mixed)) in enumerate(zip(raised, state))
        )

    state = lax.fori_loop(
        low[block],
        high[block],
        step,
        ((jnp.zeros((QUERY_TILE, 1), F32), jnp.zeros((QUERY_TILE, HS), F32)),) * count,
    )
    for h, (total, mixed) in enumerate(state):
        out_ref[:, h * HS : (h + 1) * HS] = (mixed / total).astype(BF)
        sum_ref[h] = total


def attend(heads, segment, low, high):
    tokens, columns = heads.shape
    width = columns // 3
    count = width // HS
    return call(
        attend_body,
        (tokens // QUERY_TILE,),
        [
            pl.BlockSpec((QUERY_TILE, width), lambda b, lo, hi: (b, 0)),
            pl.BlockSpec((tokens, width), lambda b, lo, hi: (0, 1)),
            pl.BlockSpec((tokens, width), lambda b, lo, hi: (0, 2)),
            pl.BlockSpec((QUERY_TILE, 1), lambda b, lo, hi: (b, 0)),
            pl.BlockSpec((1, tokens), lambda b, lo, hi: (0, 0)),
        ],
        [
            pl.BlockSpec((QUERY_TILE, width), lambda b, lo, hi: (b, 0)),
            pl.BlockSpec((count, QUERY_TILE, 1), lambda b, lo, hi: (0, b, 0)),
        ],
        [shape((tokens, width), BF), shape((count, tokens, 1), F32)],
        prefetch=2,
        name="attend",
    )(low, high, heads, heads, heads, segment[:, None], segment[None, :])


def head_back(grad, raw, gain, cosine, sine):
    turned = grad * cosine - pltpu.roll(grad, HS // 2, 1) * sine
    factor = lax.rsqrt(jnp.mean(raw * raw, axis=1, keepdims=True) + EPSILON)
    unit = raw * factor
    gain_part = jnp.sum(turned * unit, axis=0, keepdims=True)
    pulled = turned * gain
    inner = jnp.mean(pulled * unit, axis=1, keepdims=True)
    return (pulled - unit * inner) * factor, gain_part


def attend_back_body(
    low, high, q_ref, k_ref, v_ref, g_ref, o_ref, s_ref, qs_ref, ks_ref, qr_ref, kr_ref,
    cos_ref, sin_ref, hg_ref, grad_ref, gain_ref, along_ref, keys_ref, values_ref,
    inner_ref,
):
    block = pl.program_id(0)
    count = q_ref.shape[1] // HS

    @pl.when(block == 0)
    def _():
        keys_ref[...] = jnp.zeros_like(keys_ref)
        values_ref[...] = jnp.zeros_like(values_ref)
        gain_ref[...] = jnp.zeros_like(gain_ref)

    for h in range(count):
        inner_ref[h] = jnp.sum(
            head(g_ref, h).astype(F32) * head(o_ref, h).astype(F32), axis=1, keepdims=True
        )

    def step(index, state):
        rows = key_rows(index)
        allowed = qs_ref[...] == ks_ref[:, rows]
        scores = [dot(head(q_ref, h), head(k_ref, h, rows), 1, 1) for h in range(count)]
        grads = [dot(head(g_ref, h), head(v_ref, h, rows), 1, 1) for h in range(count)]
        new = []
        for h in range(count):
            columns = slice(h * HS, (h + 1) * HS)
            weights = jnp.where(
                allowed, jnp.exp2(scores[h] * EXP2_SCALE) * (1.0 / s_ref[h]), 0.0
            )
            grad_scores = (weights * (grads[h] - inner_ref[h])).astype(BF)
            values_ref[rows, columns] += dot(weights.astype(BF), head(g_ref, h), 0, 0)
            keys_ref[rows, columns] += dot(grad_scores, head(q_ref, h), 0, 0)
            new.append(state[h] + dot(grad_scores, head(k_ref, h, rows)))
        return tuple(new)

    grad_queries = lax.fori_loop(
        low[block], high[block], step, (jnp.zeros((QUERY_TILE, HS), F32),) * count
    )
    rows = pl.ds(pl.multiple_of(block * QUERY_TILE, QUERY_TILE), QUERY_TILE)
    along = jnp.zeros((QUERY_TILE, 1), F32)
    for h, grad_query in enumerate(grad_queries):
        back, part = head_back(
            grad_query * SCALE, head(qr_ref, h), hg_ref[0:1, :], cos_ref[rows, :], sin_ref[rows, :]
        )
        grad_ref[rows, h * HS : (h + 1) * HS] = back.astype(BF)
        gain_ref[0:1, :] += part
        along += jnp.sum(back * head(qr_ref, h), axis=1, keepdims=True)
    along_ref[rows, :] = along

    @pl.when(block == pl.num_programs(0) - 1)
    def _():
        along_ref[...] += jnp.sum(values_ref[...] * v_ref[...].astype(F32), axis=1, keepdims=True)
        for h in range(count):
            back, part = head_back(
                head(keys_ref, h) * SCALE, head(kr_ref, h), hg_ref[1:2, :], cos_ref[...],
                sin_ref[...],
            )
            grad_ref[:, (count + h) * HS : (count + h + 1) * HS] = back.astype(BF)
            gain_ref[1:2, :] += part
            along_ref[...] += jnp.sum(back * head(kr_ref, h), axis=1, keepdims=True)
        grad_ref[:, 2 * count * HS :] = values_ref[...].astype(BF)


def attend_back(
    heads, grad_mixed, mixed, sums, segment, low, high, raw, cosine, sine, gains, deps=()
):
    tokens, columns = heads.shape
    width = columns // 3
    count = width // HS
    whole = lambda b, lo, hi: (0, 0)
    tile = lambda b, lo, hi: (b, 0)
    return call(
        attend_back_body,
        (tokens // QUERY_TILE,),
        [
            pl.BlockSpec((QUERY_TILE, width), tile),
            pl.BlockSpec((tokens, width), lambda b, lo, hi: (0, 1)),
            pl.BlockSpec((tokens, width), lambda b, lo, hi: (0, 2)),
            pl.BlockSpec((QUERY_TILE, width), tile),
            pl.BlockSpec((QUERY_TILE, width), tile),
            pl.BlockSpec((count, QUERY_TILE, 1), lambda b, lo, hi: (0, b, 0)),
            pl.BlockSpec((QUERY_TILE, 1), tile),
            pl.BlockSpec((1, tokens), whole),
            pl.BlockSpec((QUERY_TILE, width), tile),
            pl.BlockSpec((tokens, width), lambda b, lo, hi: (0, 1)),
            pl.BlockSpec((tokens, HS), whole),
            pl.BlockSpec((tokens, HS), whole),
            pl.BlockSpec((2, HS), whole),
        ],
        [
            pl.BlockSpec((tokens, columns), whole),
            pl.BlockSpec((2, HS), whole),
            pl.BlockSpec((tokens, 1), whole),
        ],
        [shape((tokens, columns), BF), shape((2, HS), F32), shape((tokens, 1), F32)],
        scratch=[
            pltpu.VMEM((tokens, width), F32),
            pltpu.VMEM((tokens, width), F32),
            pltpu.VMEM((count, QUERY_TILE, 1), F32),
        ],
        prefetch=2,
        name="attend_back",
        deps=deps,
    )(
        low, high, heads, heads, heads, grad_mixed, mixed, sums, segment[:, None],
        segment[None, :], raw, raw, cosine, sine, gains,
    )


def dispatch_body(slot_ref, x_ref, out_ref):
    local, capacity = out_ref.shape[1], out_ref.shape[3]
    tokens = x_ref.shape[1]
    rows = x_ref[0]
    order = lax.broadcasted_iota(jnp.int32, (capacity, tokens), 0)
    for index in range(local):
        hot = jnp.where(order == slot_ref[0, 0, index : index + 1, :], 1.0, 0.0).astype(BF)
        out_ref[0, index, 0] = dot(hot, rows).astype(BF)


def dispatch(slots, rows, capacity, deps=()):
    groups, targets, local, tokens = slots.shape
    features = rows.shape[2]
    return call(
        dispatch_body,
        (groups, targets),
        [
            pl.BlockSpec((1, 1, local, tokens), lambda g, d: (g, d, 0, 0)),
            pl.BlockSpec((1, tokens, features), lambda g, d: (g, 0, 0)),
        ],
        pl.BlockSpec((1, local, 1, capacity, features), lambda g, d: (d, 0, g, 0, 0)),
        shape((targets, local, groups, capacity, features), BF),
        name="dispatch",
        deps=deps,
    )(slots, rows)


def combine_body(*refs):
    slot_ref, rows_refs, out_ref = refs[0], refs[1:-1], refs[-1]
    targets, local, _, capacity, features = rows_refs[0].shape
    total_local = local * len(rows_refs)
    tile = out_ref.shape[1]
    order = lax.broadcasted_iota(jnp.int32, (tile, capacity), 1)
    slots = slot_ref[0]
    total = jnp.zeros((tile, features), F32)
    for target in range(targets):
        for part, rows_ref in enumerate(rows_refs):
            first = target * total_local + part * local
            hot = jnp.concatenate(
                [
                    jnp.where(order == slots[:, first + i : first + i + 1], 1.0, 0.0).astype(BF)
                    for i in range(local)
                ],
                axis=1,
            )
            total = total + dot(hot, rows_ref[target].reshape(local * capacity, features))
    out_ref[0] = total.astype(BF)


def combine(slots_by_token, parts, chunk, features, deps=()):
    groups, tokens, experts = slots_by_token.shape
    targets, local, _, capacity, _ = parts[0].shape
    tile = 512
    return call(
        combine_body,
        (groups, tokens // tile),
        [pl.BlockSpec((1, tile, experts), lambda g, t: (g, t, 0))]
        + [
            pl.BlockSpec(
                (targets, local, 1, capacity, features), lambda g, t: (0, 0, g, 0, chunk)
            )
        ]
        * len(parts),
        pl.BlockSpec((1, tile, features), lambda g, t: (g, t, 0)),
        shape((groups, tokens, features), BF),
        name="combine",
        flops=2 * groups * experts * capacity * tokens * features,
        deps=deps,
    )(slots_by_token, *parts)


def block_rows(ref, row=0):
    _, cores, _, groups, capacity, features = ref.shape
    return ref[row].reshape(cores * groups * capacity, features)


def expert_body(*refs):
    x_ref, c_refs = refs[0], refs[1 : 1 + CHUNKS]
    gate_w, up_w, down_w, prob_ref, act_ref, gate_out, up_out = refs[1 + CHUNKS :]
    rows, width = x_ref.shape[0], x_ref.shape[-1]
    prob = prob_ref[0]
    gate = up = grad = None
    for row in range(rows):
        features = pl.ds(row * width, width)
        x = block_rows(x_ref, row)
        gate_part = dot(x, gate_w[0, features, :])
        up_part = dot(x, up_w[0, features, :])
        grad_part = None
        for chunk, c_ref in enumerate(c_refs):
            c = (block_rows(c_ref, row).astype(F32) * prob).astype(BF)
            part_width = width // CHUNKS
            part = dot(c, down_w[0, pl.ds(row * width + chunk * part_width, part_width), :])
            grad_part = part if grad_part is None else grad_part + part
        gate = gate_part if gate is None else gate + gate_part
        up = up_part if up is None else up + up_part
        grad = grad_part if grad is None else grad + grad_part
    squashed = 1.0 / (1.0 + jnp.exp(-gate))
    act_ref[...] = (gate * squashed * up).astype(BF)
    gate_out[...] = (grad * up * squashed * (1.0 + gate * (1.0 - squashed))).astype(BF)
    up_out[...] = (grad * gate * squashed).astype(BF)


def expert(index, rows, cots, gate_weight, up_weight, down_weight, prob):
    row_count, cores, _, groups, capacity, width = rows.shape
    _, features, hidden = gate_weight.shape
    slots = groups * capacity
    tile = min(512, hidden, 512 * 1024 // slots)
    row_spec = pl.BlockSpec(
        (row_count, 1, 1, groups, capacity, width), lambda n, k: (0, k, 0, 0, 0, 0)
    )
    cot_spec = pl.BlockSpec(
        (row_count, 1, 1, groups, capacity, width // CHUNKS), lambda n, k: (0, k, index, 0, 0, 0)
    )
    w_spec = pl.BlockSpec((1, features, tile), lambda n, k: (index, 0, n))
    out_spec = pl.BlockSpec((slots, tile), lambda n, k: (k, n))
    return call(
        expert_body,
        (hidden // tile, cores),
        [row_spec] + [cot_spec] * CHUNKS + [w_spec, w_spec, w_spec]
        + [pl.BlockSpec((1, slots, 1), lambda n, k: (index, k, 0))],
        [out_spec] * 3,
        [shape((cores * slots, hidden), BF)] * 3,
        name="expert",
    )(rows, *cots, gate_weight, up_weight, down_weight, prob)


def produce_body(act_ref, w_ref, prob_ref, *refs):
    c_refs, out_refs, inner_ref = refs[:CHUNKS], refs[-CHUNKS - 1 : -1], refs[-1]
    width = out_refs[0].shape[-1]

    @pl.when(pl.program_id(1) == 0)
    def _():
        inner_ref[...] = jnp.zeros_like(inner_ref)

    made = dot(act_ref[...], w_ref[0], 1, 1)
    weighted = (made * prob_ref[0]).astype(BF)
    for chunk, out_ref in enumerate(out_refs):
        columns = slice(chunk * width, (chunk + 1) * width)
        inner_ref[...] += jnp.sum(
            made[:, columns] * block_rows(c_refs[chunk]).astype(F32), axis=1, keepdims=True
        )
        out_ref[...] = weighted[:, columns].reshape(out_ref.shape)


def produce(index, activated, down_weight, prob, cots, dims, buffers):
    rows, cores, local, groups, capacity, width = dims
    hidden = activated.shape[1]
    slots = groups * capacity
    given = () if buffers is None else tuple(buffers)
    outs = pl.pallas_call(
        produce_body,
        out_shape=[shape(dims, BF)] * CHUNKS + [shape((cores * slots, 1), F32)],
        grid=(cores, rows),
        in_specs=[
            pl.BlockSpec((slots, hidden), lambda k, r: (k, 0)),
            pl.BlockSpec((1, width * CHUNKS, hidden), lambda k, r: (index, r, 0)),
            pl.BlockSpec((1, slots, 1), lambda k, r: (index, k, 0)),
        ]
        + [
            pl.BlockSpec((1, 1, 1, groups, capacity, width), lambda k, r: (r, k, index, 0, 0, 0))
        ]
        * CHUNKS
        + [pl.BlockSpec(memory_space=pl.ANY)] * len(given),
        out_specs=[
            pl.BlockSpec(
                (1, 1, 1, groups, capacity, width), lambda k, r: (r, k, index, 0, 0, 0)
            )
        ]
        * CHUNKS
        + [pl.BlockSpec((slots, 1), lambda k, r: (k, 0))],
        input_output_aliases={3 + CHUNKS + chunk: chunk for chunk in range(len(given))},
        compiler_params=pltpu.CompilerParams(
            dimension_semantics=("arbitrary",) * 2, vmem_limit_bytes=VMEM_BYTES
        ),
        cost_estimate=pl.CostEstimate(
            flops=2 * cores * slots * D * hidden,
            bytes_accessed=2 * D * hidden + 8 * cores * slots * D,
            transcendentals=0,
        ),
        name="produce",
    )(activated, down_weight, prob, *cots, *given)
    return outs[:CHUNKS], outs[CHUNKS]


def held_while(expert_index, last):
    return lambda i, r: jnp.where(i == expert_index, r, jnp.where(i < expert_index, 0, last))


def down_grad_body(*refs):
    prob_ref, c_refs, act_refs, out_ref = (
        refs[0], refs[1 : 1 + CHUNKS], refs[1 + CHUNKS : -1], refs[-1]
    )
    width = c_refs[0].shape[-1]
    for index, act_ref in enumerate(act_refs):

        @pl.when(pl.program_id(0) == index)
        def _():
            for chunk, c_ref in enumerate(c_refs):
                c = (block_rows(c_ref).astype(F32) * prob_ref[0]).astype(BF)
                out_ref[0, pl.ds(chunk * width, width), :] = dot(c, act_ref[...], 0, 0)


def row_specs(local, shape_of):
    rows, cores, _, groups, capacity, width = shape_of

    def spec(index):
        where = held_while(index, rows - 1)
        return pl.BlockSpec(
            (1, cores, 1, groups, capacity, width), lambda i, r: (where(i, r), 0, 0, 0, 0, 0)
        )

    return [spec(index) for index in range(local)]


def down_grad(cots, prob, activated, deps=()):
    rows, cores, local, groups, capacity, width = cots[0].shape
    slots, hidden = activated[0].shape
    return call(
        down_grad_body,
        (local, rows),
        [pl.BlockSpec((1, slots, 1), lambda i, r: (i, 0, 0))]
        + [pl.BlockSpec((1, cores, 1, groups, capacity, width), lambda i, r: (r, 0, i, 0, 0, 0))]
        * CHUNKS
        + [pl.BlockSpec((slots, hidden), lambda i, r: (0, 0))] * local,
        pl.BlockSpec((1, width * CHUNKS, hidden), lambda i, r: (i, r, 0)),
        shape((local, rows * width * CHUNKS, hidden), F32),
        name="down_grad",
        flops=2 * local * slots * D * hidden,
        deps=deps,
    )(prob, *cots, *activated)


def gate_grad_body(*refs):
    local = (len(refs) - 2) // 3
    x_refs, gate_refs, up_refs = refs[:local], refs[local : 2 * local], refs[2 * local : -2]
    gate_out, up_out = refs[-2:]
    for index in range(local):

        @pl.when(pl.program_id(0) == index)
        def _():
            x = block_rows(x_refs[index])
            gate_out[0] = dot(x, gate_refs[index][...], 0, 0)
            up_out[0] = dot(x, up_refs[index][...], 0, 0)


def gate_grad(parts, grad_gate_pre, grad_up_pre, deps=()):
    rows, cores, _, groups, capacity, width = parts[0].shape
    slots, hidden = grad_gate_pre[0].shape
    local = len(parts)
    wide = pl.BlockSpec((slots, hidden), lambda i, r: (0, 0))
    out = pl.BlockSpec((1, width, hidden), lambda i, r: (i, r, 0))
    return call(
        gate_grad_body,
        (local, rows),
        row_specs(local, parts[0].shape) + [wide] * (2 * local),
        [out, out],
        [shape((local, rows * width, hidden), F32)] * 2,
        name="gate_grad",
        deps=deps,
    )(*parts, *grad_gate_pre, *grad_up_pre)


def rows_back_body(gate_ref, up_ref, gate_w, up_w, *refs):
    out_ref = refs[-1]
    made = dot(gate_ref[...], gate_w[0], 1, 1) + dot(up_ref[...], up_w[0], 1, 1)
    out_ref[...] = made.astype(BF).reshape(out_ref.shape)


def rows_back(
    index, grad_gate_pre, grad_up_pre, gate_weight, up_weight, chunk, dims, buffer, deps=()
):
    rows, cores, local, groups, capacity, width = dims
    hidden = gate_weight.shape[2]
    slots = groups * capacity
    pre = pl.BlockSpec((slots, hidden), lambda k, r: (k, 0))
    weight = pl.BlockSpec((1, width, hidden), lambda k, r: (index, r * CHUNKS + chunk, 0))
    given = () if buffer is None else (buffer,)
    return pl.pallas_call(
        rows_back_body,
        out_shape=shape(dims, BF),
        grid=(cores, rows),
        in_specs=[pre, pre, weight, weight]
        + [pl.BlockSpec(memory_space=pl.ANY)] * len(given + tuple(deps)),
        out_specs=pl.BlockSpec(
            (1, 1, 1, groups, capacity, width), lambda k, r: (r, k, index, 0, 0, 0)
        ),
        input_output_aliases={4: 0} if given else {},
        compiler_params=pltpu.CompilerParams(
            dimension_semantics=("arbitrary",) * 2, vmem_limit_bytes=VMEM_BYTES
        ),
        cost_estimate=pl.CostEstimate(
            flops=4 * cores * slots * width * rows * hidden,
            bytes_accessed=4 * rows * width * hidden + 6 * cores * slots * width * rows,
            transcendentals=0,
        ),
        name="rows_back",
    )(grad_gate_pre, grad_up_pre, gate_weight, up_weight, *given, *deps)


def swap(rows):
    return lax.all_to_all(rows, SWAP_AXES, split_axis=0, concat_axis=0, tiled=True)


def slot_positions(routes, ranks, capacity):
    experts = jnp.arange(E, dtype=jnp.int32)
    member = jnp.any(routes.T[:, None, :] == experts[None, :, None], axis=0)
    earlier = (ranks[:, None] < ranks[None, :]).astype(BF)
    position = jnp.dot(member.astype(BF), earlier, preferred_element_type=F32)
    return jnp.where(member & (position < capacity), position, -1.0)


def per_device(
    hidden_in,
    attention_gain,
    query_weight,
    key_weight,
    value_weight,
    projection,
    query_gain,
    key_gain,
    feedforward_gain,
    router_weight,
    gate_weight,
    up_weight,
    down_weight,
    segments,
    routes,
    priority,
    cotangent,
):
    tokens, width_here = hidden_in.shape
    row_count = lax.axis_size("row")
    z_count = lax.axis_size("z")
    core_count = lax.axis_size("core")
    local = gate_weight.shape[0]
    piece_count = row_count * z_count * core_count * local
    pieces = max(1, piece_count // E)
    capacity = tokens * TOPK // E
    width = width_here // CHUNKS
    row_index = lax.axis_index("row")
    z_index = lax.axis_index("z")
    core_index = lax.axis_index("core")
    head_columns = query_weight.shape[1]
    experts_here = E // row_count
    head_count = head_columns // HS

    hidden_pieces, hidden_starts = row_gather(
        jnp.concatenate(
            [hidden_in, jnp.broadcast_to(attention_gain[None, :], (GAIN_ROWS, width_here))], axis=0
        )
    )
    qkv_full = lax.all_gather(
        jnp.concatenate([query_weight, key_weight, value_weight], axis=1),
        TOKENS_AXES,
        axis=0,
        tiled=True,
    )
    with_router = lax.all_gather(
        jnp.concatenate([projection, router_weight], axis=1),
        TOKENS_AXES,
        axis=0,
        tiled=True,
    )
    projection_full = with_router[:, :head_columns]
    router_rows = with_router[:, head_columns:].reshape(row_count, width_here, -1)
    router_here = jnp.swapaxes(small_row_swap(router_rows), 1, 2).reshape(E, width_here)

    position = slot_positions(routes, priority[0], capacity)
    by_piece = jnp.repeat(position.astype(BF), pieces, axis=0).reshape(
        row_count, z_count, core_count * local, tokens
    )
    mine = lax.all_to_all(jnp.swapaxes(by_piece, 0, 1), "z", 0, 0, tiled=True).astype(jnp.int32)
    slots = mine.reshape(z_count, row_count * core_count, local, tokens)
    slots_by_token = jnp.swapaxes(
        mine.reshape(z_count, row_count * core_count * local, tokens), 1, 2
    )
    dims = (row_count, core_count, local, z_count, capacity, width)

    expert_dims = (row_count, core_count, 1, z_count, capacity, width_here)
    def scatter_back(summed):
        return lax.psum_scatter(summed, "z", scatter_dimension=0, tiled=True).reshape(
            tokens, width
        )

    spread_cots = [
        lax.all_gather(
            after(cotangent[:, chunk * width : (chunk + 1) * width], *hidden_pieces[2:6]),
            "z",
            axis=0,
        )
        for chunk in range(CHUNKS)
    ]
    first_picked = dispatch(slots, spread_cots[0], capacity)

    cosine, sine = rotary_tables()
    first_gain = attention_gain.astype(F32)
    second_gain = feedforward_gain.astype(F32)
    head_gains = jnp.stack([query_gain, key_gain]).astype(F32)
    residual = hidden_in.astype(F32)
    normed_one, heads, raw, first_factor = project(
        hidden_starts,
        hidden_pieces,
        qkv_full,
        cosine,
        sine,
        jnp.repeat(head_gains, head_count, axis=0).reshape(1, -1),
        (mine, router_here),
    )
    segment = segments[0]
    low, high = key_ranges(segment)
    mixed, sums = attend(heads, segment, low, high)
    middle = residual + row_scatter(
        mixed, row_scatter_order(projection_full), first_picked
    )[0]
    second_factor = lax.rsqrt(lax.psum(jnp.sum(middle * middle, axis=1), "row") / D + EPSILON)[
        :, None
    ]
    normed_two = (middle * second_factor * second_gain).astype(BF)

    later_picked = [dispatch(slots, spread, capacity, [normed_two]) for spread in spread_cots[1:]]
    logits = row_sum(after(dot(router_here, normed_two, 1, 1), *later_picked))
    raised = jnp.exp(logits)
    router_probs = raised / jnp.sum(raised, axis=0, keepdims=True)

    cots = [swap(after(first_picked, normed_two)).reshape(dims)]
    for picked in later_picked:
        cots.append(swap(after(picked, cots[-1], logits)).reshape(dims))
    spread_rows = lax.all_gather(normed_two, "z", axis=0)
    rows = []
    for index in range(local):
        picked = dispatch(slots[:, :, index : index + 1], spread_rows, capacity, cots[:1])
        rows.append(swap(after(picked, cots[-1], *rows[-1:])).reshape(expert_dims))
    own_slots = lax.dynamic_slice_in_dim(position, row_index * experts_here, experts_here, 0)
    own_probs = lax.dynamic_slice_in_dim(router_probs, row_index * experts_here, experts_here, 0)
    order = jnp.arange(capacity, dtype=jnp.int32).astype(F32)
    slot_prob = jnp.sum(
        jnp.where(own_slots[:, None, :] == order[None, :, None], own_probs[:, None, :], 0.0), axis=2
    )
    prob_groups = jnp.repeat(
        lax.all_gather(slot_prob, TOKENS_AXES, axis=0), pieces, axis=1
    ).reshape(z_count, core_count, z_count, core_count, local, capacity)
    prob_here = lax.dynamic_index_in_dim(
        lax.dynamic_index_in_dim(prob_groups, z_index, 2, keepdims=False),
        core_index,
        2,
        keepdims=False,
    )
    prob = jnp.transpose(prob_here, (2, 1, 0, 3)).reshape(
        local, core_count * z_count * capacity, 1
    )
    swapped_dims = (row_count * core_count,) + dims[2:]
    activated, grad_gate_pre, grad_up_pre = [], [], []
    buffers = [None] * CHUNKS
    for index in range(local):
        rows_here = rows[index]
        act, gate_pre, up_pre = expert(
            index, rows_here, cots, gate_weight, up_weight, down_weight, prob
        )
        activated.append(act)
        grad_gate_pre.append(gate_pre)
        grad_up_pre.append(up_pre)
        for chunk in range(CHUNKS):
            buffers[chunk] = rows_back(
                index, gate_pre, up_pre, gate_weight, up_weight, chunk, dims, buffers[chunk],
                buffers[:chunk] if index == local - 1 else (),
            )
    inners, made_buffers = [], None
    for index in range(local):
        made_buffers, inner = produce(
            index, activated[index], down_weight, prob, cots, dims, made_buffers
        )
        inners.append(inner)

    inner = jnp.stack(inners).reshape(local, core_count, z_count, capacity)
    to_groups = jnp.transpose(inner, (2, 1, 0, 3)).reshape(
        z_count * core_count, local * capacity
    )
    back_rows = [swap(buffers[0].reshape(swapped_dims))]
    ready = after(buffers[1], *inners)
    back_rows.append(swap(ready.reshape(swapped_dims)))
    of_group = lax.all_to_all(
        after(to_groups, *back_rows), TOKENS_AXES, 0, 0, tiled=True
    ).reshape(-1, capacity)
    slot_grads = jnp.sum(small_row_gather(of_group).reshape(E, pieces, capacity), axis=1)
    grad_prob = jnp.sum(
        jnp.where(position[:, None, :] == order[None, :, None], slot_grads[:, :, None], 0.0), axis=1
    )
    grad_logits = (
        router_probs * (grad_prob - jnp.sum(router_probs * grad_prob, axis=0, keepdims=True))
    ).astype(BF)
    from_router = dot(grad_logits, router_here, 0, 0)
    first_sum = combine(slots_by_token, [back_rows[0]], 0, width, [ready])
    grad_gate, grad_up = gate_grad(rows, grad_gate_pre, grad_up_pre, [first_sum])
    first_sum = scatter_back(first_sum)
    second_sum = combine(slots_by_token, [back_rows[1]], 0, width, [grad_gate, first_sum])
    grad_down = down_grad(cots, prob, activated, [second_sum, slot_grads])
    second_sum = scatter_back(second_sum)
    grad_normed_two = after(from_router, grad_down) + jnp.concatenate(
        [first_sum, second_sum], axis=1
    ).astype(F32)
    router_part = dot(grad_logits, normed_two)
    router_swapped = lax.all_to_all(
        router_part.reshape(row_count, experts_here, width_here), "row", 0, 0, tiled=True
    )
    grad_router = lax.psum_scatter(
        jnp.swapaxes(router_swapped, 0, 1).reshape(experts_here, D),
        TOKENS_AXES,
        scatter_dimension=1,
        tiled=True,
    )

    scaled_two = grad_normed_two * second_gain
    second_inner = lax.psum(jnp.sum(scaled_two * middle, axis=1), "row")[:, None]
    grad_middle = (
        cotangent.astype(F32)
        + scaled_two * second_factor
        - middle * second_factor**3 * second_inner / D
    )
    grad_feedforward_gain = jnp.sum(grad_normed_two * middle * second_factor, axis=0)

    grad_branch = grad_middle.astype(BF)
    made_rows = [swap(after(made_buffers[0], back_rows[1], slot_grads).reshape(swapped_dims))]
    branch_pieces, branch_starts = row_gather(after(grad_branch, made_rows[0], router_swapped))
    made_rows.append(swap(after(made_buffers[1], *branch_pieces).reshape(swapped_dims)))
    made_sums = [combine(slots_by_token, [made_rows[0]], 0, width, [grad_branch])]
    grad_projection = projection_grad(branch_starts, branch_pieces, mixed, made_sums)
    grad_mixed = mix_back(
        branch_starts, branch_pieces, projection_full, [grad_projection, router_swapped]
    )
    projection_sum = core_sum(grad_projection)
    grad_raw, head_gain_grads, along = attend_back(
        heads, grad_mixed, mixed, sums, segment, low, high, raw, cosine, sine, head_gains,
        [projection_sum],
    )
    made_sums.append(combine(slots_by_token, [made_rows[1]], 0, width, [grad_raw]))
    from_experts = [scatter_back(each) for each in made_sums]
    grad_raw = after(grad_raw, made_sums[1], from_experts[0], grad_router)
    grad_first, sent, received = row_scatter(grad_raw, row_scatter_order(qkv_full))
    small = jnp.concatenate([along.reshape(-1, HS), head_gain_grads], axis=0)
    small = jnp.sum(small_row_gather(small), axis=0)
    first_inner = small[:-2].reshape(-1, 1) / first_factor
    head_gain_grads = small[-2:]
    grad_qkv = dot(after(normed_one, *received), grad_raw, 0, 0).astype(BF)
    scaled_one = grad_first * first_gain
    grad_input = (
        grad_middle + scaled_one * first_factor - residual * first_factor**3 * first_inner / D
    )
    grad_attention_gain = jnp.sum(grad_first * residual * first_factor, axis=0)

    grad_attention_gain, grad_feedforward_gain, head_gain_grads = lax.psum(
        (grad_attention_gain, grad_feedforward_gain, head_gain_grads), TOKENS_AXES
    )
    grad_projection = z_scatter(projection_sum).astype(F32)
    grad_qkv = z_scatter(core_sum(grad_qkv)).astype(F32)
    from_experts = jnp.concatenate(from_experts, axis=1).astype(F32)
    output = (after(middle, grad_first) + from_experts).astype(BF)
    return (
        output,
        grad_input,
        grad_attention_gain,
        grad_qkv[:, :head_columns],
        grad_qkv[:, head_columns : 2 * head_columns],
        grad_qkv[:, 2 * head_columns :],
        grad_projection,
        head_gain_grads[0],
        head_gain_grads[1],
        grad_feedforward_gain,
        grad_router.T,
        grad_gate,
        grad_up,
        grad_down,
    )


def solution(mesh):
    rows, columns = mesh.shape["row"], mesh.shape["col"]
    split_mesh = Mesh(
        mesh.devices.reshape(rows, columns // 2, 2), ("row", "z", "core")
    )
    both = P(TOKENS_AXES, "row")
    expert = P(ALL_AXES, None, None)
    grouped = P(TOKENS_AXES, None)
    return jax.shard_map(
        per_device,
        mesh=split_mesh,
        in_specs=(
            both, P("row"), both, both, both, both, P(), P(), P("row"), both,
            expert, expert, expert, grouped, grouped, grouped, both,
        ),
        out_specs=(
            both, both, P("row"), both, both, both, both, P(), P(), P("row"), both,
            expert, expert, expert,
        ),
        check_vma=False,
    )
```

```python
import functools

import jax
import jax.numpy as jnp
from jax import lax
from jax.experimental import pallas as pl
from jax.experimental.pallas import tpu as pltpu
from jax.sharding import Mesh, PartitionSpec as P

D = 2048
HS = 128
E = 64
TOPK = 8
SEQ = 2048
EPSILON = 1e-06
SCALE = HS ** (-0.5)
CHUNKS = 2
GAIN_ROWS = 16
TOKENS_AXES = ("z", "core")
SWAP_AXES = ("row", "core")
ALL_AXES = ("row", "z", "core")
BF = jnp.bfloat16
F32 = jnp.float32
VMEM_BYTES = 60 * 1024 * 1024


def call(body, grid, in_specs, out_specs, out_shape, scratch=(), prefetch=0, name=None, deps=(), flops=0):
    deps = tuple(deps)

    def without_deps(*refs):
        body(*refs[:prefetch], *refs[prefetch + len(deps) :])

    kernel = pl.pallas_call(
        without_deps,
        out_shape=out_shape,
        grid_spec=pltpu.PrefetchScalarGridSpec(
            num_scalar_prefetch=prefetch,
            grid=grid,
            in_specs=[pl.BlockSpec(memory_space=pl.ANY)] * len(deps) + list(in_specs),
            out_specs=out_specs,
            scratch_shapes=list(scratch),
        ),
        compiler_params=pltpu.CompilerParams(
            dimension_semantics=("arbitrary",) * len(grid), vmem_limit_bytes=VMEM_BYTES
        ),
        cost_estimate=pl.CostEstimate(flops=flops, bytes_accessed=0, transcendentals=0),
        name=name,
    )
    return lambda *args: kernel(*args[:prefetch], *deps, *args[prefetch:])


def shape(dims, dtype):
    return jax.ShapeDtypeStruct(dims, dtype)


def dot(left, right, left_dim=1, right_dim=0):
    return lax.dot_general(
        left, right, (((left_dim,), (right_dim,)), ((), ())), preferred_element_type=F32
    )


def rotary_tables():
    half_size = HS // 2
    inverse = 50000.0 ** (-(jnp.arange(half_size, dtype=F32) * 2.0) / HS)
    angles = jnp.arange(SEQ, dtype=F32)[:, None] * inverse[None, :]
    cosine, sine = jnp.cos(angles), jnp.sin(angles)
    return (
        jnp.concatenate([cosine, cosine], axis=1),
        jnp.concatenate([-sine, sine], axis=1),
    )


def project_body(starts, *refs):
    count = starts.shape[0]
    x_refs, gain_refs, refs = refs[:count], refs[count : 2 * count], refs[2 * count :]
    w_ref, cos_ref, sin_ref, hg_ref, normed_ref, heads_ref, raw_ref, factor_ref = refs
    width = x_refs[0].shape[1]
    square = sum(
        jnp.sum(jnp.square(x_ref[...].astype(F32)), axis=1, keepdims=True) for x_ref in x_refs
    )
    factor = lax.rsqrt(square / (width * count) + EPSILON)
    factor_ref[...] = factor
    raw = None
    for index, x_ref in enumerate(x_refs):
        features = pl.ds(pl.multiple_of(starts[index], width), width)
        gain = gain_refs[index][0:1, :].astype(F32)
        normed = (x_ref[...].astype(F32) * factor * gain).astype(BF)
        normed_ref[:, features] = normed
        part = dot(normed, w_ref[features, :])
        raw = part if raw is None else raw + part
    turned = raw_ref.shape[1]
    raw_ref[...] = raw[:, :turned]
    cosine, sine = cos_ref[...], sin_ref[...]
    for head in range(turned // HS):
        part = raw[:, head * HS : (head + 1) * HS]
        unit = part * lax.rsqrt(jnp.mean(part * part, axis=1, keepdims=True) + EPSILON)
        scaled = unit * hg_ref[:, head * HS : (head + 1) * HS]
        heads_ref[:, head * HS : (head + 1) * HS] = (
            scaled * cosine + pltpu.roll(scaled, HS // 2, 1) * sine
        ).astype(BF)
    heads_ref[:, turned:] = raw[:, turned:].astype(BF)


def project(starts, pieces, weights, cosine, sine, head_gains, deps=()):
    tokens, piece = cosine.shape[0], pieces[0].shape[1]
    width, columns = weights.shape
    turned = columns // 3 * 2
    tile = 256
    own = lambda t, s: (t, 0)
    whole = lambda t, s: (0, 0)
    return call(
        project_body,
        (tokens // tile,),
        [pl.BlockSpec((tile, piece), own)] * len(pieces)
        + [pl.BlockSpec((GAIN_ROWS, piece), lambda t, s: (tokens // GAIN_ROWS, 0))] * len(pieces)
        + [
            pl.BlockSpec((width, columns), whole),
            pl.BlockSpec((tile, HS), own),
            pl.BlockSpec((tile, HS), own),
            pl.BlockSpec((1, turned), whole),
        ],
        [
            pl.BlockSpec((tile, width), own),
            pl.BlockSpec((tile, columns), own),
            pl.BlockSpec((tile, turned), own),
            pl.BlockSpec((tile, 1), own),
        ],
        [
            shape((tokens, width), BF),
            shape((tokens, columns), BF),
            shape((tokens, turned), F32),
            shape((tokens, 1), F32),
        ],
        prefetch=1,
        name="project",
        deps=deps,
    )(starts, *pieces, *pieces, weights, cosine, sine, head_gains)


def mix_back_body(starts, *refs):
    count = starts.shape[0]
    g_refs, (w_ref, out_ref) = refs[:count], refs[count:]
    width = g_refs[0].shape[1]
    total = None
    for index, g_ref in enumerate(g_refs):
        part = dot(g_ref[...], w_ref[pl.ds(pl.multiple_of(starts[index], width), width), :])
        total = part if total is None else total + part
    out_ref[...] = total.astype(BF)


def mix_back(starts, pieces, weights, deps=()):
    tokens, piece = pieces[0].shape
    width, columns = weights.shape
    tile = 256
    return call(
        mix_back_body,
        (tokens // tile,),
        [pl.BlockSpec((tile, piece), lambda t, s: (t, 0))] * len(pieces)
        + [pl.BlockSpec((width, columns), lambda t, s: (0, 0))],
        pl.BlockSpec((tile, columns), lambda t, s: (t, 0)),
        shape((tokens, columns), BF),
        prefetch=1,
        name="mix_back",
        deps=deps,
    )(starts, *pieces, weights)


def projection_grad_body(starts, *refs):
    count = starts.shape[0]
    g_refs, (mixed_ref, out_ref, total_ref) = refs[:count], refs[count:]
    width = g_refs[0].shape[1]

    @pl.when(pl.program_id(0) == 0)
    def _():
        total_ref[...] = jnp.zeros_like(total_ref)

    for index, g_ref in enumerate(g_refs):
        rows = pl.ds(pl.multiple_of(starts[index], width), width)
        total_ref[rows, :] += dot(g_ref[...], mixed_ref[...], 0, 0)

    @pl.when(pl.program_id(0) == pl.num_programs(0) - 1)
    def _():
        out_ref[...] = total_ref[...].astype(BF)


def projection_grad(starts, pieces, mixed, deps=()):
    tokens, piece = pieces[0].shape
    columns = mixed.shape[1]
    width = piece * len(pieces)
    tile = 512
    return call(
        projection_grad_body,
        (tokens // tile,),
        [pl.BlockSpec((tile, piece), lambda t, s: (t, 0))] * len(pieces)
        + [pl.BlockSpec((tile, columns), lambda t, s: (t, 0))],
        pl.BlockSpec((width, columns), lambda t, s: (0, 0)),
        shape((width, columns), BF),
        scratch=[pltpu.VMEM((width, columns), F32)],
        prefetch=1,
        name="projection_grad",
        deps=deps,
    )(starts, *pieces, mixed)


def permute(values, mask):
    return lax.ppermute(values, "row", [(i, i ^ mask) for i in range(4)])


def row_gather(values):
    width = values.shape[1]
    if lax.axis_size("row") != 4:
        return [lax.all_gather(values, "row", axis=1, tiled=True)], jnp.zeros((1,), jnp.int32)
    half = width // 2
    left, right = values[:, :half], values[:, half:]
    left_1, right_2 = permute(left, 1), permute(right, 2)
    left_2, right_1 = permute(left, 2), permute(right, 1)
    left_3, right_3 = permute(left_1, 2), permute(right_2, 1)
    me = lax.axis_index("row")
    starts = jnp.stack(
        [(me ^ mask) * width + side * half for mask in range(4) for side in range(2)]
    ).astype(jnp.int32)
    return [left, right, left_1, right_1, left_2, right_2, left_3, right_3], starts


def small_row_gather(values):
    if lax.axis_size("row") != 4:
        return lax.all_gather(values, "row", axis=0)
    stacked = jnp.stack([values] + [permute(values, mask) for mask in (1, 2, 3)])
    return jnp.take(stacked, lax.axis_index("row") ^ jnp.arange(4), axis=0)


def small_row_swap(blocks):
    if lax.axis_size("row") != 4:
        return lax.all_to_all(blocks, "row", 0, 0, tiled=True)
    me = lax.axis_index("row")
    near = jnp.take(blocks, me ^ jnp.arange(4), axis=0)
    stacked = jnp.stack([near[0]] + [permute(near[mask], mask) for mask in (1, 2, 3)])
    return jnp.take(stacked, me ^ jnp.arange(4), axis=0)


def core_sum(values):
    z_count, core_count = lax.axis_size("z"), lax.axis_size("core")
    rows, columns = values.shape
    blocks = values.reshape(z_count, core_count, rows // (z_count * core_count), columns)
    core = lax.axis_index("core")
    keep = lax.dynamic_index_in_dim(blocks, core, 1, keepdims=False)
    give = lax.dynamic_index_in_dim(blocks, 1 - core, 1, keepdims=False)
    got = lax.ppermute(give, "core", [(0, 1), (1, 0)])
    return (keep.astype(F32) + got.astype(F32)).astype(values.dtype).reshape(-1, columns)


def z_scatter(values):
    return lax.psum_scatter(values, "z", scatter_dimension=0, tiled=True)


def row_sum(values):
    if lax.axis_size("row") != 4:
        return jnp.sum(lax.all_gather(values, "row", axis=0), axis=0)
    half = values.shape[1] // 2
    left, right = values[:, :half], values[:, half:]
    left, right = left + permute(left, 1), right + permute(right, 2)
    return jnp.concatenate([left + permute(left, 2), right + permute(right, 1)], axis=1)


def after(value, *others):
    others = [other for other in others if other is not None]
    return pl.pallas_call(
        lambda *refs: None,
        out_shape=shape(value.shape, value.dtype),
        in_specs=[pl.BlockSpec(memory_space=pl.ANY)] * (1 + len(others)),
        out_specs=pl.BlockSpec(memory_space=pl.ANY),
        input_output_aliases={0: 0},
        cost_estimate=pl.CostEstimate(flops=0, bytes_accessed=0, transcendentals=0),
        name="after",
    )(value, *others)


def row_scatter_order(weights):
    if lax.axis_size("row") != 4:
        return weights
    width = weights.shape[0] // 4
    half = width // 2
    me = lax.axis_index("row")
    order = [(1, 0), (3, 0), (2, 1), (3, 1), (2, 0), (1, 1), (0, 0), (0, 1)]
    return jnp.concatenate(
        [
            lax.dynamic_slice_in_dim(weights, (me ^ mask) * width + side * half, half, 0)
            for mask, side in order
        ],
        axis=0,
    )


def row_scatter(left, ordered, *meanwhile):
    if lax.axis_size("row") != 4:
        return lax.psum_scatter(
            dot(left, ordered, 1, 1).astype(BF), "row", scatter_dimension=1, tiled=True
        ).astype(F32), (), ()
    width = ordered.shape[0] // 4
    half = width // 2
    part = lambda index: dot(left, ordered[index * width : (index + 1) * width], 1, 1)
    sent = [part(0).astype(BF), part(1).astype(BF)]
    received = [permute(sent[0], 1), permute(sent[1], 2)]
    from_x, from_y = received[0].astype(F32), received[1].astype(F32)
    onward, own = part(2), part(3)
    onward_left = (onward[:, :half] + from_x[:, half:]).astype(BF)
    onward_right = (onward[:, half:] + from_y[:, half:]).astype(BF)
    if meanwhile:
        onward_left = after(onward_left, *meanwhile)
        onward_right = after(onward_right, *meanwhile)
    last_left = permute(onward_left, 2).astype(F32)
    last_right = permute(onward_right, 1).astype(F32)
    total = jnp.concatenate(
        [
            own[:, :half] + from_x[:, :half] + last_left,
            own[:, half:] + from_y[:, :half] + last_right,
        ],
        axis=1,
    )
    return total, sent, received


QUERY_TILE = 256
KEY_TILE = 256
EXP2_SCALE = SCALE * 1.4426950408889634


def key_ranges(segment):
    first = segment[::QUERY_TILE]
    last = segment[QUERY_TILE - 1 :: QUERY_TILE]
    key_first = segment[::KEY_TILE]
    key_last = segment[KEY_TILE - 1 :: KEY_TILE]
    meets = (key_first[None, :] <= last[:, None]) & (key_last[None, :] >= first[:, None])
    order = jnp.arange(meets.shape[1], dtype=jnp.int32)[None, :]
    low = jnp.min(jnp.where(meets, order, meets.shape[1]), axis=1)
    high = jnp.max(jnp.where(meets, order + 1, 0), axis=1)
    return low.astype(jnp.int32), high.astype(jnp.int32)


def key_rows(step):
    return pl.ds(pl.multiple_of(step * KEY_TILE, KEY_TILE), KEY_TILE)


def head(ref, index, rows=slice(None)):
    return ref[rows, index * HS : (index + 1) * HS]


def attend_body(low, high, q_ref, k_ref, v_ref, qs_ref, ks_ref, out_ref, sum_ref):
    block = pl.program_id(0)
    count = q_ref.shape[1] // HS
    query_docs = qs_ref[...]

    def step(index, state):
        rows = key_rows(index)
        allowed = query_docs == ks_ref[:, rows]
        scores = [dot(head(q_ref, h), head(k_ref, h, rows), 1, 1) for h in range(count)]
        raised = [jnp.where(allowed, jnp.exp2(each * EXP2_SCALE), 0.0) for each in scores]
        return tuple(
            (
                total + jnp.sum(each, axis=1, keepdims=True),
                mixed + dot(each.astype(BF), head(v_ref, h, rows)),
            )
            for h, (each, (total, mixed)) in enumerate(zip(raised, state))
        )

    state = lax.fori_loop(
        low[block],
        high[block],
        step,
        ((jnp.zeros((QUERY_TILE, 1), F32), jnp.zeros((QUERY_TILE, HS), F32)),) * count,
    )
    for h, (total, mixed) in enumerate(state):
        out_ref[:, h * HS : (h + 1) * HS] = (mixed / total).astype(BF)
        sum_ref[h] = total


def attend(heads, segment, low, high):
    tokens, columns = heads.shape
    width = columns // 3
    count = width // HS
    return call(
        attend_body,
        (tokens // QUERY_TILE,),
        [
            pl.BlockSpec((QUERY_TILE, width), lambda b, lo, hi: (b, 0)),
            pl.BlockSpec((tokens, width), lambda b, lo, hi: (0, 1)),
            pl.BlockSpec((tokens, width), lambda b, lo, hi: (0, 2)),
            pl.BlockSpec((QUERY_TILE, 1), lambda b, lo, hi: (b, 0)),
            pl.BlockSpec((1, tokens), lambda b, lo, hi: (0, 0)),
        ],
        [
            pl.BlockSpec((QUERY_TILE, width), lambda b, lo, hi: (b, 0)),
            pl.BlockSpec((count, QUERY_TILE, 1), lambda b, lo, hi: (0, b, 0)),
        ],
        [shape((tokens, width), BF), shape((count, tokens, 1), F32)],
        prefetch=2,
        name="attend",
    )(low, high, heads, heads, heads, segment[:, None], segment[None, :])


def head_back(grad, raw, gain, cosine, sine):
    turned = grad * cosine - pltpu.roll(grad, HS // 2, 1) * sine
    factor = lax.rsqrt(jnp.mean(raw * raw, axis=1, keepdims=True) + EPSILON)
    unit = raw * factor
    gain_part = jnp.sum(turned * unit, axis=0, keepdims=True)
    pulled = turned * gain
    inner = jnp.mean(pulled * unit, axis=1, keepdims=True)
    return (pulled - unit * inner) * factor, gain_part


def attend_back_body(
    low, high, q_ref, k_ref, v_ref, g_ref, o_ref, s_ref, qs_ref, ks_ref, qr_ref, kr_ref,
    cos_ref, sin_ref, hg_ref, grad_ref, gain_ref, along_ref, keys_ref, values_ref,
    inner_ref,
):
    block = pl.program_id(0)
    count = q_ref.shape[1] // HS

    @pl.when(block == 0)
    def _():
        keys_ref[...] = jnp.zeros_like(keys_ref)
        values_ref[...] = jnp.zeros_like(values_ref)
        gain_ref[...] = jnp.zeros_like(gain_ref)

    for h in range(count):
        inner_ref[h] = jnp.sum(
            head(g_ref, h).astype(F32) * head(o_ref, h).astype(F32), axis=1, keepdims=True
        )

    def step(index, state):
        rows = key_rows(index)
        allowed = qs_ref[...] == ks_ref[:, rows]
        scores = [dot(head(q_ref, h), head(k_ref, h, rows), 1, 1) for h in range(count)]
        grads = [dot(head(g_ref, h), head(v_ref, h, rows), 1, 1) for h in range(count)]
        new = []
        for h in range(count):
            columns = slice(h * HS, (h + 1) * HS)
            weights = jnp.where(
                allowed, jnp.exp2(scores[h] * EXP2_SCALE) * (1.0 / s_ref[h]), 0.0
            )
            grad_scores = (weights * (grads[h] - inner_ref[h])).astype(BF)
            values_ref[rows, columns] += dot(weights.astype(BF), head(g_ref, h), 0, 0)
            keys_ref[rows, columns] += dot(grad_scores, head(q_ref, h), 0, 0)
            new.append(state[h] + dot(grad_scores, head(k_ref, h, rows)))
        return tuple(new)

    grad_queries = lax.fori_loop(
        low[block], high[block], step, (jnp.zeros((QUERY_TILE, HS), F32),) * count
    )
    rows = pl.ds(pl.multiple_of(block * QUERY_TILE, QUERY_TILE), QUERY_TILE)
    along = jnp.zeros((QUERY_TILE, 1), F32)
    for h, grad_query in enumerate(grad_queries):
        back, part = head_back(
            grad_query * SCALE, head(qr_ref, h), hg_ref[0:1, :], cos_ref[rows, :], sin_ref[rows, :]
        )
        grad_ref[rows, h * HS : (h + 1) * HS] = back.astype(BF)
        gain_ref[0:1, :] += part
        along += jnp.sum(back * head(qr_ref, h), axis=1, keepdims=True)
    along_ref[rows, :] = along

    @pl.when(block == pl.num_programs(0) - 1)
    def _():
        along_ref[...] += jnp.sum(values_ref[...] * v_ref[...].astype(F32), axis=1, keepdims=True)
        for h in range(count):
            back, part = head_back(
                head(keys_ref, h) * SCALE, head(kr_ref, h), hg_ref[1:2, :], cos_ref[...],
                sin_ref[...],
            )
            grad_ref[:, (count + h) * HS : (count + h + 1) * HS] = back.astype(BF)
            gain_ref[1:2, :] += part
            along_ref[...] += jnp.sum(back * head(kr_ref, h), axis=1, keepdims=True)
        grad_ref[:, 2 * count * HS :] = values_ref[...].astype(BF)


def attend_back(
    heads, grad_mixed, mixed, sums, segment, low, high, raw, cosine, sine, gains, deps=()
):
    tokens, columns = heads.shape
    width = columns // 3
    count = width // HS
    whole = lambda b, lo, hi: (0, 0)
    tile = lambda b, lo, hi: (b, 0)
    return call(
        attend_back_body,
        (tokens // QUERY_TILE,),
        [
            pl.BlockSpec((QUERY_TILE, width), tile),
            pl.BlockSpec((tokens, width), lambda b, lo, hi: (0, 1)),
            pl.BlockSpec((tokens, width), lambda b, lo, hi: (0, 2)),
            pl.BlockSpec((QUERY_TILE, width), tile),
            pl.BlockSpec((QUERY_TILE, width), tile),
            pl.BlockSpec((count, QUERY_TILE, 1), lambda b, lo, hi: (0, b, 0)),
            pl.BlockSpec((QUERY_TILE, 1), tile),
            pl.BlockSpec((1, tokens), whole),
            pl.BlockSpec((QUERY_TILE, width), tile),
            pl.BlockSpec((tokens, width), lambda b, lo, hi: (0, 1)),
            pl.BlockSpec((tokens, HS), whole),
            pl.BlockSpec((tokens, HS), whole),
            pl.BlockSpec((2, HS), whole),
        ],
        [
            pl.BlockSpec((tokens, columns), whole),
            pl.BlockSpec((2, HS), whole),
            pl.BlockSpec((tokens, 1), whole),
        ],
        [shape((tokens, columns), BF), shape((2, HS), F32), shape((tokens, 1), F32)],
        scratch=[
            pltpu.VMEM((tokens, width), F32),
            pltpu.VMEM((tokens, width), F32),
            pltpu.VMEM((count, QUERY_TILE, 1), F32),
        ],
        prefetch=2,
        name="attend_back",
        deps=deps,
    )(
        low, high, heads, heads, heads, grad_mixed, mixed, sums, segment[:, None],
        segment[None, :], raw, raw, cosine, sine, gains,
    )


def dispatch_body(slot_ref, x_ref, out_ref):
    local, capacity = out_ref.shape[1], out_ref.shape[3]
    tokens = x_ref.shape[1]
    rows = x_ref[0]
    order = lax.broadcasted_iota(jnp.int32, (capacity, tokens), 0)
    for index in range(local):
        hot = jnp.where(order == slot_ref[0, 0, index : index + 1, :], 1.0, 0.0).astype(BF)
        out_ref[0, index, 0] = dot(hot, rows).astype(BF)


def dispatch(slots, rows, capacity, deps=()):
    groups, targets, local, tokens = slots.shape
    features = rows.shape[2]
    return call(
        dispatch_body,
        (groups, targets),
        [
            pl.BlockSpec((1, 1, local, tokens), lambda g, d: (g, d, 0, 0)),
            pl.BlockSpec((1, tokens, features), lambda g, d: (g, 0, 0)),
        ],
        pl.BlockSpec((1, local, 1, capacity, features), lambda g, d: (d, 0, g, 0, 0)),
        shape((targets, local, groups, capacity, features), BF),
        name="dispatch",
        deps=deps,
    )(slots, rows)


def combine_body(*refs):
    slot_ref, rows_refs, out_ref = refs[0], refs[1:-1], refs[-1]
    targets, local, _, capacity, features = rows_refs[0].shape
    total_local = local * len(rows_refs)
    tile = out_ref.shape[1]
    order = lax.broadcasted_iota(jnp.int32, (tile, capacity), 1)
    slots = slot_ref[0]
    total = jnp.zeros((tile, features), F32)
    for target in range(targets):
        for part, rows_ref in enumerate(rows_refs):
            first = target * total_local + part * local
            hot = jnp.concatenate(
                [
                    jnp.where(order == slots[:, first + i : first + i + 1], 1.0, 0.0).astype(BF)
                    for i in range(local)
                ],
                axis=1,
            )
            total = total + dot(hot, rows_ref[target].reshape(local * capacity, features))
    out_ref[0] = total.astype(BF)


def combine(slots_by_token, parts, chunk, features, deps=()):
    groups, tokens, experts = slots_by_token.shape
    targets, local, _, capacity, _ = parts[0].shape
    tile = 512
    return call(
        combine_body,
        (groups, tokens // tile),
        [pl.BlockSpec((1, tile, experts), lambda g, t: (g, t, 0))]
        + [
            pl.BlockSpec(
                (targets, local, 1, capacity, features), lambda g, t: (0, 0, g, 0, chunk)
            )
        ]
        * len(parts),
        pl.BlockSpec((1, tile, features), lambda g, t: (g, t, 0)),
        shape((groups, tokens, features), BF),
        name="combine",
        flops=2 * groups * experts * capacity * tokens * features,
        deps=deps,
    )(slots_by_token, *parts)


def block_rows(ref, row=0):
    _, cores, _, groups, capacity, features = ref.shape
    return ref[row].reshape(cores * groups * capacity, features)


def expert_body(*refs):
    x_ref, c_refs = refs[0], refs[1 : 1 + CHUNKS]
    gate_w, up_w, down_w, prob_ref, act_ref, gate_out, up_out = refs[1 + CHUNKS :]
    rows, width = x_ref.shape[0], x_ref.shape[-1]
    prob = prob_ref[0]
    gate = up = grad = None
    for row in range(rows):
        features = pl.ds(row * width, width)
        x = block_rows(x_ref, row)
        gate_part = dot(x, gate_w[0, features, :])
        up_part = dot(x, up_w[0, features, :])
        grad_part = None
        for chunk, c_ref in enumerate(c_refs):
            c = (block_rows(c_ref, row).astype(F32) * prob).astype(BF)
            part_width = width // CHUNKS
            part = dot(c, down_w[0, pl.ds(row * width + chunk * part_width, part_width), :])
            grad_part = part if grad_part is None else grad_part + part
        gate = gate_part if gate is None else gate + gate_part
        up = up_part if up is None else up + up_part
        grad = grad_part if grad is None else grad + grad_part
    squashed = 1.0 / (1.0 + jnp.exp(-gate))
    act_ref[...] = (gate * squashed * up).astype(BF)
    gate_out[...] = (grad * up * squashed * (1.0 + gate * (1.0 - squashed))).astype(BF)
    up_out[...] = (grad * gate * squashed).astype(BF)


def expert(index, rows, cots, gate_weight, up_weight, down_weight, prob):
    row_count, cores, _, groups, capacity, width = rows.shape
    _, features, hidden = gate_weight.shape
    slots = groups * capacity
    tile = min(512, hidden, 512 * 1024 // slots)
    row_spec = pl.BlockSpec(
        (row_count, 1, 1, groups, capacity, width), lambda n, k: (0, k, 0, 0, 0, 0)
    )
    cot_spec = pl.BlockSpec(
        (row_count, 1, 1, groups, capacity, width // CHUNKS), lambda n, k: (0, k, index, 0, 0, 0)
    )
    w_spec = pl.BlockSpec((1, features, tile), lambda n, k: (index, 0, n))
    out_spec = pl.BlockSpec((slots, tile), lambda n, k: (k, n))
    return call(
        expert_body,
        (hidden // tile, cores),
        [row_spec] + [cot_spec] * CHUNKS + [w_spec, w_spec, w_spec]
        + [pl.BlockSpec((1, slots, 1), lambda n, k: (index, k, 0))],
        [out_spec] * 3,
        [shape((cores * slots, hidden), BF)] * 3,
        name="expert",
    )(rows, *cots, gate_weight, up_weight, down_weight, prob)


def produce_body(act_ref, w_ref, prob_ref, *refs):
    c_refs, out_refs, inner_ref = refs[:CHUNKS], refs[-CHUNKS - 1 : -1], refs[-1]
    width = out_refs[0].shape[-1]

    @pl.when(pl.program_id(1) == 0)
    def _():
        inner_ref[...] = jnp.zeros_like(inner_ref)

    made = dot(act_ref[...], w_ref[0], 1, 1)
    weighted = (made * prob_ref[0]).astype(BF)
    for chunk, out_ref in enumerate(out_refs):
        columns = slice(chunk * width, (chunk + 1) * width)
        inner_ref[...] += jnp.sum(
            made[:, columns] * block_rows(c_refs[chunk]).astype(F32), axis=1, keepdims=True
        )
        out_ref[...] = weighted[:, columns].reshape(out_ref.shape)


def produce(index, activated, down_weight, prob, cots, dims, buffers):
    rows, cores, local, groups, capacity, width = dims
    hidden = activated.shape[1]
    slots = groups * capacity
    given = () if buffers is None else tuple(buffers)
    outs = pl.pallas_call(
        produce_body,
        out_shape=[shape(dims, BF)] * CHUNKS + [shape((cores * slots, 1), F32)],
        grid=(cores, rows),
        in_specs=[
            pl.BlockSpec((slots, hidden), lambda k, r: (k, 0)),
            pl.BlockSpec((1, width * CHUNKS, hidden), lambda k, r: (index, r, 0)),
            pl.BlockSpec((1, slots, 1), lambda k, r: (index, k, 0)),
        ]
        + [
            pl.BlockSpec((1, 1, 1, groups, capacity, width), lambda k, r: (r, k, index, 0, 0, 0))
        ]
        * CHUNKS
        + [pl.BlockSpec(memory_space=pl.ANY)] * len(given),
        out_specs=[
            pl.BlockSpec(
                (1, 1, 1, groups, capacity, width), lambda k, r: (r, k, index, 0, 0, 0)
            )
        ]
        * CHUNKS
        + [pl.BlockSpec((slots, 1), lambda k, r: (k, 0))],
        input_output_aliases={3 + CHUNKS + chunk: chunk for chunk in range(len(given))},
        compiler_params=pltpu.CompilerParams(
            dimension_semantics=("arbitrary",) * 2, vmem_limit_bytes=VMEM_BYTES
        ),
        cost_estimate=pl.CostEstimate(
            flops=2 * cores * slots * D * hidden,
            bytes_accessed=2 * D * hidden + 8 * cores * slots * D,
            transcendentals=0,
        ),
        name="produce",
    )(activated, down_weight, prob, *cots, *given)
    return outs[:CHUNKS], outs[CHUNKS]


def held_while(expert_index, last):
    return lambda i, r: jnp.where(i == expert_index, r, jnp.where(i < expert_index, 0, last))


def down_grad_body(*refs):
    prob_ref, c_refs, act_refs, out_ref = (
        refs[0], refs[1 : 1 + CHUNKS], refs[1 + CHUNKS : -1], refs[-1]
    )
    width = c_refs[0].shape[-1]
    for index, act_ref in enumerate(act_refs):

        @pl.when(pl.program_id(0) == index)
        def _():
            for chunk, c_ref in enumerate(c_refs):
                c = (block_rows(c_ref).astype(F32) * prob_ref[0]).astype(BF)
                out_ref[0, pl.ds(chunk * width, width), :] = dot(c, act_ref[...], 0, 0)


def row_specs(local, shape_of):
    rows, cores, _, groups, capacity, width = shape_of

    def spec(index):
        where = held_while(index, rows - 1)
        return pl.BlockSpec(
            (1, cores, 1, groups, capacity, width), lambda i, r: (where(i, r), 0, 0, 0, 0, 0)
        )

    return [spec(index) for index in range(local)]


def down_grad(cots, prob, activated, deps=()):
    rows, cores, local, groups, capacity, width = cots[0].shape
    slots, hidden = activated[0].shape
    return call(
        down_grad_body,
        (local, rows),
        [pl.BlockSpec((1, slots, 1), lambda i, r: (i, 0, 0))]
        + [pl.BlockSpec((1, cores, 1, groups, capacity, width), lambda i, r: (r, 0, i, 0, 0, 0))]
        * CHUNKS
        + [pl.BlockSpec((slots, hidden), lambda i, r: (0, 0))] * local,
        pl.BlockSpec((1, width * CHUNKS, hidden), lambda i, r: (i, r, 0)),
        shape((local, rows * width * CHUNKS, hidden), F32),
        name="down_grad",
        flops=2 * local * slots * D * hidden,
        deps=deps,
    )(prob, *cots, *activated)


def gate_grad_body(*refs):
    local = (len(refs) - 2) // 3
    x_refs, gate_refs, up_refs = refs[:local], refs[local : 2 * local], refs[2 * local : -2]
    gate_out, up_out = refs[-2:]
    for index in range(local):

        @pl.when(pl.program_id(0) == index)
        def _():
            x = block_rows(x_refs[index])
            gate_out[0] = dot(x, gate_refs[index][...], 0, 0)
            up_out[0] = dot(x, up_refs[index][...], 0, 0)


def gate_grad(parts, grad_gate_pre, grad_up_pre, deps=()):
    rows, cores, _, groups, capacity, width = parts[0].shape
    slots, hidden = grad_gate_pre[0].shape
    local = len(parts)
    wide = pl.BlockSpec((slots, hidden), lambda i, r: (0, 0))
    out = pl.BlockSpec((1, width, hidden), lambda i, r: (i, r, 0))
    return call(
        gate_grad_body,
        (local, rows),
        row_specs(local, parts[0].shape) + [wide] * (2 * local),
        [out, out],
        [shape((local, rows * width, hidden), F32)] * 2,
        name="gate_grad",
        deps=deps,
    )(*parts, *grad_gate_pre, *grad_up_pre)


def rows_back_body(gate_ref, up_ref, gate_w, up_w, *refs):
    out_ref = refs[-1]
    made = dot(gate_ref[...], gate_w[0], 1, 1) + dot(up_ref[...], up_w[0], 1, 1)
    out_ref[...] = made.astype(BF).reshape(out_ref.shape)


def rows_back(
    index, grad_gate_pre, grad_up_pre, gate_weight, up_weight, chunk, dims, buffer, deps=()
):
    rows, cores, local, groups, capacity, width = dims
    hidden = gate_weight.shape[2]
    slots = groups * capacity
    pre = pl.BlockSpec((slots, hidden), lambda k, r: (k, 0))
    weight = pl.BlockSpec((1, width, hidden), lambda k, r: (index, r * CHUNKS + chunk, 0))
    given = () if buffer is None else (buffer,)
    return pl.pallas_call(
        rows_back_body,
        out_shape=shape(dims, BF),
        grid=(cores, rows),
        in_specs=[pre, pre, weight, weight]
        + [pl.BlockSpec(memory_space=pl.ANY)] * len(given + tuple(deps)),
        out_specs=pl.BlockSpec(
            (1, 1, 1, groups, capacity, width), lambda k, r: (r, k, index, 0, 0, 0)
        ),
        input_output_aliases={4: 0} if given else {},
        compiler_params=pltpu.CompilerParams(
            dimension_semantics=("arbitrary",) * 2, vmem_limit_bytes=VMEM_BYTES
        ),
        cost_estimate=pl.CostEstimate(
            flops=4 * cores * slots * width * rows * hidden,
            bytes_accessed=4 * rows * width * hidden + 6 * cores * slots * width * rows,
            transcendentals=0,
        ),
        name="rows_back",
    )(grad_gate_pre, grad_up_pre, gate_weight, up_weight, *given, *deps)


def swap(rows):
    return lax.all_to_all(rows, SWAP_AXES, split_axis=0, concat_axis=0, tiled=True)


def slot_positions(routes, ranks, capacity):
    experts = jnp.arange(E, dtype=jnp.int32)
    member = jnp.any(routes.T[:, None, :] == experts[None, :, None], axis=0)
    earlier = (ranks[:, None] < ranks[None, :]).astype(BF)
    position = jnp.dot(member.astype(BF), earlier, preferred_element_type=F32)
    return jnp.where(member & (position < capacity), position, -1.0)


def per_device(
    hidden_in,
    attention_gain,
    query_weight,
    key_weight,
    value_weight,
    projection,
    query_gain,
    key_gain,
    feedforward_gain,
    router_weight,
    gate_weight,
    up_weight,
    down_weight,
    segments,
    routes,
    priority,
    cotangent,
):
    tokens, width_here = hidden_in.shape
    row_count = lax.axis_size("row")
    z_count = lax.axis_size("z")
    core_count = lax.axis_size("core")
    local = gate_weight.shape[0]
    piece_count = row_count * z_count * core_count * local
    pieces = max(1, piece_count // E)
    capacity = tokens * TOPK // E
    width = width_here // CHUNKS
    row_index = lax.axis_index("row")
    z_index = lax.axis_index("z")
    core_index = lax.axis_index("core")
    head_columns = query_weight.shape[1]
    experts_here = E // row_count
    head_count = head_columns // HS

    hidden_pieces, hidden_starts = row_gather(
        jnp.concatenate(
            [hidden_in, jnp.broadcast_to(attention_gain[None, :], (GAIN_ROWS, width_here))], axis=0
        )
    )
    qkv_full = lax.all_gather(
        jnp.concatenate([query_weight, key_weight, value_weight], axis=1),
        TOKENS_AXES,
        axis=0,
        tiled=True,
    )
    with_router = lax.all_gather(
        jnp.concatenate([projection, router_weight], axis=1),
        TOKENS_AXES,
        axis=0,
        tiled=True,
    )
    projection_full = with_router[:, :head_columns]
    router_rows = with_router[:, head_columns:].reshape(row_count, width_here, -1)
    router_here = jnp.swapaxes(small_row_swap(router_rows), 1, 2).reshape(E, width_here)

    position = slot_positions(routes, priority[0], capacity)
    by_piece = jnp.repeat(position.astype(BF), pieces, axis=0).reshape(
        row_count, z_count, core_count * local, tokens
    )
    mine = lax.all_to_all(jnp.swapaxes(by_piece, 0, 1), "z", 0, 0, tiled=True).astype(jnp.int32)
    slots = mine.reshape(z_count, row_count * core_count, local, tokens)
    slots_by_token = jnp.swapaxes(
        mine.reshape(z_count, row_count * core_count * local, tokens), 1, 2
    )
    dims = (row_count, core_count, local, z_count, capacity, width)

    expert_dims = (row_count, core_count, 1, z_count, capacity, width_here)
    def scatter_back(summed):
        return lax.psum_scatter(summed, "z", scatter_dimension=0, tiled=True).reshape(
            tokens, width
        )

    spread_cots = [
        lax.all_gather(
            after(cotangent[:, chunk * width : (chunk + 1) * width], *hidden_pieces[2:6]),
            "z",
            axis=0,
        )
        for chunk in range(CHUNKS)
    ]
    first_picked = dispatch(slots, spread_cots[0], capacity)

    cosine, sine = rotary_tables()
    first_gain = attention_gain.astype(F32)
    second_gain = feedforward_gain.astype(F32)
    head_gains = jnp.stack([query_gain, key_gain]).astype(F32)
    residual = hidden_in.astype(F32)
    normed_one, heads, raw, first_factor = project(
        hidden_starts,
        hidden_pieces,
        qkv_full,
        cosine,
        sine,
        jnp.repeat(head_gains, head_count, axis=0).reshape(1, -1),
        (mine, router_here),
    )
    segment = segments[0]
    low, high = key_ranges(segment)
    mixed, sums = attend(heads, segment, low, high)
    middle = residual + row_scatter(
        mixed, row_scatter_order(projection_full), first_picked
    )[0]
    second_factor = lax.rsqrt(lax.psum(jnp.sum(middle * middle, axis=1), "row") / D + EPSILON)[
        :, None
    ]
    normed_two = (middle * second_factor * second_gain).astype(BF)

    later_picked = [dispatch(slots, spread, capacity, [normed_two]) for spread in spread_cots[1:]]
    logits = row_sum(after(dot(router_here, normed_two, 1, 1), *later_picked))
    raised = jnp.exp(logits)
    router_probs = raised / jnp.sum(raised, axis=0, keepdims=True)

    cots = [swap(after(first_picked, normed_two)).reshape(dims)]
    for picked in later_picked:
        cots.append(swap(after(picked, cots[-1], logits)).reshape(dims))
    spread_rows = lax.all_gather(normed_two, "z", axis=0)
    rows = []
    for index in range(local):
        picked = dispatch(slots[:, :, index : index + 1], spread_rows, capacity, cots[:1])
        rows.append(swap(after(picked, cots[-1], *rows[-1:])).reshape(expert_dims))
    own_slots = lax.dynamic_slice_in_dim(position, row_index * experts_here, experts_here, 0)
    own_probs = lax.dynamic_slice_in_dim(router_probs, row_index * experts_here, experts_here, 0)
    order = jnp.arange(capacity, dtype=jnp.int32).astype(F32)
    slot_prob = jnp.sum(
        jnp.where(own_slots[:, None, :] == order[None, :, None], own_probs[:, None, :], 0.0), axis=2
    )
    prob_groups = jnp.repeat(
        lax.all_gather(slot_prob, TOKENS_AXES, axis=0), pieces, axis=1
    ).reshape(z_count, core_count, z_count, core_count, local, capacity)
    prob_here = lax.dynamic_index_in_dim(
        lax.dynamic_index_in_dim(prob_groups, z_index, 2, keepdims=False),
        core_index,
        2,
        keepdims=False,
    )
    prob = jnp.transpose(prob_here, (2, 1, 0, 3)).reshape(
        local, core_count * z_count * capacity, 1
    )
    swapped_dims = (row_count * core_count,) + dims[2:]
    activated, grad_gate_pre, grad_up_pre = [], [], []
    buffers = [None] * CHUNKS
    for index in range(local):
        rows_here = rows[index]
        act, gate_pre, up_pre = expert(
            index, rows_here, cots, gate_weight, up_weight, down_weight, prob
        )
        activated.append(act)
        grad_gate_pre.append(gate_pre)
        grad_up_pre.append(up_pre)
        for chunk in range(CHUNKS):
            buffers[chunk] = rows_back(
                index, gate_pre, up_pre, gate_weight, up_weight, chunk, dims, buffers[chunk],
                buffers[:chunk] if index == local - 1 else (),
            )
    inners, made_buffers = [], None
    for index in range(local):
        made_buffers, inner = produce(
            index, activated[index], down_weight, prob, cots, dims, made_buffers
        )
        inners.append(inner)

    inner = jnp.stack(inners).reshape(local, core_count, z_count, capacity)
    to_groups = jnp.transpose(inner, (2, 1, 0, 3)).reshape(
        z_count * core_count, local * capacity
    )
    back_rows = [swap(buffers[0].reshape(swapped_dims))]
    ready = after(buffers[1], *inners)
    back_rows.append(swap(ready.reshape(swapped_dims)))
    of_group = lax.all_to_all(
        after(to_groups, *back_rows), TOKENS_AXES, 0, 0, tiled=True
    ).reshape(-1, capacity)
    slot_grads = jnp.sum(small_row_gather(of_group).reshape(E, pieces, capacity), axis=1)
    grad_prob = jnp.sum(
        jnp.where(position[:, None, :] == order[None, :, None], slot_grads[:, :, None], 0.0), axis=1
    )
    grad_logits = (
        router_probs * (grad_prob - jnp.sum(router_probs * grad_prob, axis=0, keepdims=True))
    ).astype(BF)
    from_router = dot(grad_logits, router_here, 0, 0)
    first_sum = combine(slots_by_token, [back_rows[0]], 0, width, [ready])
    grad_gate, grad_up = gate_grad(rows, grad_gate_pre, grad_up_pre, [first_sum])
    first_sum = scatter_back(first_sum)
    second_sum = combine(slots_by_token, [back_rows[1]], 0, width, [grad_gate, first_sum])
    grad_down = down_grad(cots, prob, activated, [second_sum, slot_grads])
    second_sum = scatter_back(second_sum)
    grad_normed_two = after(from_router, grad_down) + jnp.concatenate(
        [first_sum, second_sum], axis=1
    ).astype(F32)
    router_part = dot(grad_logits, normed_two)
    router_swapped = lax.all_to_all(
        router_part.reshape(row_count, experts_here, width_here), "row", 0, 0, tiled=True
    )
    grad_router = lax.psum_scatter(
        jnp.swapaxes(router_swapped, 0, 1).reshape(experts_here, D),
        TOKENS_AXES,
        scatter_dimension=1,
        tiled=True,
    )

    scaled_two = grad_normed_two * second_gain
    second_inner = lax.psum(jnp.sum(scaled_two * middle, axis=1), "row")[:, None]
    grad_middle = (
        cotangent.astype(F32)
        + scaled_two * second_factor
        - middle * second_factor**3 * second_inner / D
    )
    grad_feedforward_gain = jnp.sum(grad_normed_two * middle * second_factor, axis=0)

    grad_branch = grad_middle.astype(BF)
    made_rows = [swap(after(made_buffers[0], back_rows[1], slot_grads).reshape(swapped_dims))]
    branch_pieces, branch_starts = row_gather(after(grad_branch, made_rows[0], router_swapped))
    made_rows.append(swap(after(made_buffers[1], *branch_pieces).reshape(swapped_dims)))
    made_sums = [combine(slots_by_token, [made_rows[0]], 0, width, branch_pieces[2:4])]
    grad_projection = projection_grad(branch_starts, branch_pieces, mixed, made_sums)
    grad_mixed = mix_back(
        branch_starts, branch_pieces, projection_full, [grad_projection, router_swapped]
    )
    projection_sum = core_sum(grad_projection)
    grad_raw, head_gain_grads, along = attend_back(
        heads, grad_mixed, mixed, sums, segment, low, high, raw, cosine, sine, head_gains,
        [projection_sum],
    )
    made_sums.append(combine(slots_by_token, [made_rows[1]], 0, width, [grad_raw]))
    from_experts = [scatter_back(each) for each in made_sums]
    grad_raw = after(grad_raw, made_sums[1], from_experts[0], grad_router)
    grad_first, sent, received = row_scatter(grad_raw, row_scatter_order(qkv_full))
    small = jnp.concatenate([along.reshape(-1, HS), head_gain_grads], axis=0)
    small = jnp.sum(small_row_gather(small), axis=0)
    first_inner = small[:-2].reshape(-1, 1) / first_factor
    head_gain_grads = small[-2:]
    grad_qkv = dot(after(normed_one, *received), grad_raw, 0, 0).astype(BF)
    scaled_one = grad_first * first_gain
    grad_input = (
        grad_middle + scaled_one * first_factor - residual * first_factor**3 * first_inner / D
    )
    grad_attention_gain = jnp.sum(grad_first * residual * first_factor, axis=0)

    grad_attention_gain, grad_feedforward_gain, head_gain_grads = lax.psum(
        (grad_attention_gain, grad_feedforward_gain, head_gain_grads), TOKENS_AXES
    )
    grad_projection = z_scatter(projection_sum).astype(F32)
    grad_qkv = z_scatter(core_sum(grad_qkv)).astype(F32)
    from_experts = jnp.concatenate(from_experts, axis=1).astype(F32)
    output = (after(middle, grad_first) + from_experts).astype(BF)
    return (
        output,
        grad_input,
        grad_attention_gain,
        grad_qkv[:, :head_columns],
        grad_qkv[:, head_columns : 2 * head_columns],
        grad_qkv[:, 2 * head_columns :],
        grad_projection,
        head_gain_grads[0],
        head_gain_grads[1],
        grad_feedforward_gain,
        grad_router.T,
        grad_gate,
        grad_up,
        grad_down,
    )


def solution(mesh):
    rows, columns = mesh.shape["row"], mesh.shape["col"]
    split_mesh = Mesh(
        mesh.devices.reshape(rows, columns // 2, 2), ("row", "z", "core")
    )
    both = P(TOKENS_AXES, "row")
    expert = P(ALL_AXES, None, None)
    grouped = P(TOKENS_AXES, None)
    return jax.shard_map(
        per_device,
        mesh=split_mesh,
        in_specs=(
            both, P("row"), both, both, both, both, P(), P(), P("row"), both,
            expert, expert, expert, grouped, grouped, grouped, both,
        ),
        out_specs=(
            both, both, P("row"), both, both, both, both, P(), P(), P("row"), both,
            expert, expert, expert,
        ),
        check_vma=False,
    )
```
